32 devices in a mesh: occ: 4 (over z), vir: 4 (over y, x), ka: 2 (over core).
Axes of the slice: x: 2, y: 2, z: 4, core: 2. Of those that a mesh axis runs over, the one named last changes fastest.
Arguments:
- lambda_amps: bfloat16 [2, 16, 1024, 1024], P(None, 'occ', 'vir', 'ka'), may hold values from -0.25 to 0.25
- screened_ints: bfloat16 [16, 1024, 1024], P(('occ', 'vir'), 'ka'), may hold values from -6 to 6
- half_ints: bfloat16 [16, 1024, 128], P(('occ', 'vir'), 'ka'), may hold values from -0.5 to 0.5
- singles: bfloat16 [128, 1024], P(None, 'vir'), may hold values from -6 to 6
- block_mask: int32 [16, 8, 8], P('occ', 'ka'), may hold values from 0 to 1, as said below
Outputs:
- residual_part: bfloat16 [2, 16, 1024, 1024], P('ka', 'occ', 'vir')
The draws below stay inside these ranges and needn't reach their ends.
Inputs may be any that keep to these rules, and one draw needn't show every extreme that they name: `block_mask`: for each j and each of the 2 equal ranges of e blocks, between 1 and 16 of its 32 blocks are 1; some (j, range) has exactly 16.
All inputs are finite; a program needn't handle non-finite values.
Results may differ from the reference program's by a relative error of at most 0.0058.
Values may be sent and summed in bfloat16 or wider, within the bound.
A program may use at most 128 MiB of HBM per device.

```python
import jax
import jax.numpy as jnp
from jax import lax

O = 128
V = 1024
TILE = 128
CAP = 16
IW = 2
NB = 8
HALVES = 2
HT = 32
J = 16


def draw_block_mask(key, part):
    first_key, second_key, third_key = jax.random.split(key, 3)
    groups = J * HALVES
    base_draw = jax.random.randint(first_key, (groups,), 1, 6)
    counts = jnp.minimum(base_draw * base_draw, CAP)
    forced = jax.random.randint(second_key, (), 0, groups)
    counts = jnp.where(jnp.arange(groups) == forced, CAP, counts)
    scores = jax.random.randint(third_key, (groups, HT), 0, 1 << 20) * HT + jnp.arange(HT)[None, :]
    ordering = jnp.argsort(scores, axis=1, stable=True)
    ranking = jnp.argsort(ordering, axis=1, stable=True)
    live_tiles = (ranking < counts[:, None]).astype(jnp.int32)
    return live_tiles.reshape(J, NB, NB)


def levels(stream_key, shape, cuts, smallest, largest):
    def one(dim, shards_of):
        heights = jax.random.uniform(jax.random.fold_in(jax.random.fold_in(stream_key, 6), dim), (shards_of,), jnp.float32, smallest / len(cuts), largest / len(cuts))
        return jnp.repeat(jnp.exp(heights), shape[dim] // shards_of).reshape((-1,) + (1,) * (len(shape) - dim - 1))

    factor_of = one(*cuts[0])
    for cut in cuts[1:]:
        factor_of = factor_of * one(*cut)
    return factor_of


def gaussian(own_key, shape, deviation, bound, shards=(), dtype=jnp.bfloat16):
    loudness = levels(own_key, shape, shards, -0.22, 0.18) if shards else 1.0
    values = jax.random.normal(own_key, shape, jnp.float32) * deviation * loudness
    return jnp.minimum(jnp.maximum(values, -bound), bound).astype(dtype)


def setup_inputs(seed: int = 0) -> dict:
    key_list = jax.random.split(jax.random.key(seed), 6)
    return {
        "lambda_amps": gaussian(key_list[0], (IW, J, V, V), (V // 2) ** -0.5, 0.25, ((1, 4), (2, 4), (3, 2))),
        "screened_ints": gaussian(key_list[1], (J, V, V), 1.0, 6.0, ((0, 16), (1, 2))),
        "half_ints": gaussian(key_list[2], (J, V, O), O ** -0.5, 0.5, ((0, 16), (1, 2))),
        "singles": gaussian(key_list[3], (O, V), 1.0, 6.0, ((1, 4),)),
        "block_mask": draw_block_mask(jax.random.fold_in(key_list[5], 71), 0),
    }


def reference(lambda_amps, screened_ints, half_ints, singles, block_mask):
    def per_item(item):
        dressed = screened_ints[item].astype(jnp.float32) - jnp.dot(half_ints[item], singles, preferred_element_type=jnp.float32)
        block_gate = jnp.repeat(jnp.repeat(block_mask[item].astype(jnp.float32), TILE, axis=0), TILE, axis=1)
        blocks = (block_gate * dressed).astype(jnp.bfloat16)
        amp_rows = lambda_amps[:, item].reshape(IW * V, V)
        result = jnp.dot(amp_rows, blocks, preferred_element_type=jnp.float32).astype(jnp.bfloat16)
        return result.reshape(IW, V, V)

    stacked = lax.map(per_item, jnp.arange(J).astype(jnp.int32))
    return jnp.transpose(stacked, (1, 0, 2, 3))
```

```python
import functools

import jax
import jax.numpy as jnp
from jax import lax
from jax.experimental import pallas as pl
from jax.experimental.pallas import tpu as pltpu
from jax.sharding import PartitionSpec as P

TILE = 128
CAP = 16
PER = 2
CHUNKS = CAP // PER


def peers_of(v, n, grid):
    if grid:
        y, x = v // 2, v % 2
        ids = [v, y * 2 + (1 - x), (1 - y) * 2 + x, (1 - y) * 2 + (1 - x)]
        return ids, ids
    return [(v + k) % n for k in range(n)], [(v + n - k) % n for k in range(n)]


def kernel(n, lam, x, y, t, mask, mask_any, out, lam_m, lam_t, x_v, y_v, dressed, dense_m, dense_t, acc, other,
           in_sem, t_send, t_recv, td_send, td_recv, b_send, b_recv, f_send, d_send, d_recv, l_send, l_recv, *bufs):
    t_v, mine, theirs = bufs[:n], bufs[n:2 * n], bufs[2 * n:]
    grid = n == 4
    v, c = lax.axis_index("vir"), lax.axis_index("ka")
    dst, src = peers_of(v, n, grid)
    partner = 1 - c
    half = x_v.shape[0]
    inner, width = t_v[0].shape
    cols = width // TILE
    row_blocks = half // TILE
    col_blocks = x_v.shape[1] // TILE
    part = inner // 2

    loads = [
        pltpu.make_async_copy(t, t_v[0], in_sem.at[0]),
        pltpu.make_async_copy(y.at[0], y_v, in_sem.at[1]),
        pltpu.make_async_copy(x.at[0], x_v, in_sem.at[2]),
        pltpu.make_async_copy(lam.at[c], lam_m, in_sem.at[3]),
    ]
    for load in loads:
        load.start()

    barrier = pltpu.get_barrier_semaphore()
    for k in range(1, n):
        pl.semaphore_signal(barrier, inc=1, device_id={"vir": dst[k]}, device_id_type=pl.DeviceIdType.MESH)
    pl.semaphore_signal(barrier, inc=1, device_id={"ka": partner}, device_id_type=pl.DeviceIdType.MESH)
    loads[0].wait()
    pl.semaphore_wait(barrier, n)

    def remote(source, target, send, recv, where):
        return pltpu.make_async_remote_copy(
            src_ref=source, dst_ref=target, send_sem=send, recv_sem=recv,
            device_id=where, device_id_type=pl.DeviceIdType.MESH)

    def rows_of(ref):
        return ref.at[pl.ds(pl.multiple_of(c * part, part), part)]

    t_copies = [None] + [
        remote(rows_of(t_v[0]), rows_of(t_v[k]), t_send.at[k], t_recv.at[k], {"vir": dst[k]})
        for k in range(1, n)]
    t_swaps = [None] + [
        remote(rows_of(t_v[k]), rows_of(t_v[k]), td_send.at[k], td_recv.at[k], {"ka": partner})
        for k in range(1, n)]
    for copy in reversed(t_copies[1:]):
        copy.start()
    mask_swap = remote(mask_any, other, l_send.at[0], l_recv.at[0], {"ka": partner})
    mask_swap.start()

    zero = jnp.zeros((TILE, TILE), jnp.bfloat16)
    for k in range(n):
        mine[k][CAP] = zero
        theirs[k][CAP] = zero

    blocks = row_blocks * col_blocks
    order = [jnp.int32(0)] * CAP
    count = jnp.int32(0)
    for p in range(blocks):
        live = mask[v, p // col_blocks, p % col_blocks]
        order = [jnp.where((live != 0) & (count == s), p, order[s]) for s in range(CAP)]
        count = count + live

    loads[1].wait()
    loads[2].wait()

    def dress(k):
        start = src[k] * width
        term = jnp.dot(y_v[...], t_v[k][...], preferred_element_type=jnp.float32)
        value = (x_v[:, pl.ds(pl.multiple_of(start, TILE), width)].astype(jnp.float32) - term).astype(jnp.bfloat16)
        for e in range(row_blocks):
            for b in range(cols):
                dressed[e * col_blocks + src[k] * cols + b] = value[e * TILE:(e + 1) * TILE, b * TILE:(b + 1) * TILE]

    dress(0)
    for k in range(1, n):
        t_copies[k].wait_recv()
        t_swaps[k].start()
    for k in range(1, n):
        t_swaps[k].wait_recv()
        dress(k)

    def chunk(ref, q):
        return ref.at[pl.ds(q * PER, PER)]

    def own_copy(k, q):
        return remote(chunk(mine[0], q), chunk(mine[k], q), b_send.at[k, q], b_recv.at[k, q], {"vir": dst[k]})

    def relay_copy(k, q):
        return remote(chunk(mine[k], q), chunk(mine[3], q), f_send.at[q], b_recv.at[3, q], {"vir": dst[3 - k]})

    def swap(k, q):
        return remote(chunk(mine[k], q), chunk(theirs[k], q), d_send.at[k, q], d_recv.at[k, q], {"ka": partner})

    low, high = list(range(CHUNKS // 2)), list(range(CHUNKS // 2, CHUNKS))
    direct = (1, 2) if grid else tuple(range(1, n))
    paths = {k: (high + low if grid and k == 2 else low + high) for k in range(1, n)}
    relays = [(1, q) for q in low] + [(2, q) for q in high] if grid else []

    for pair in zip(low, high):
        for q in pair:
            for s in range(q * PER, (q + 1) * PER):
                mine[0][s] = dressed[order[s]]
            if not grid:
                for k in direct:
                    own_copy(k, q).start()
        if grid:
            own_copy(1, pair[0]).start()
            own_copy(2, pair[1]).start()
    if grid:
        for pair in zip(low, high):
            own_copy(1, pair[1]).start()
            own_copy(2, pair[0]).start()
    for q in range(CHUNKS):
        swap(0, q).start()
    lam_swap = remote(lam.at[partner], lam_t, l_send.at[1], l_recv.at[1], {"ka": partner})
    lam_swap.start()
    mask_swap.wait_recv()

    def fill(dense, gathered, live_of, j):
        count = jnp.int32(0)
        for e in range(row_blocks):
            for b in range(col_blocks):
                live = live_of[j, e, b]
                dense[e * TILE:(e + 1) * TILE, b * TILE:(b + 1) * TILE] = gathered[jnp.where(live != 0, count, CAP)]
                count = count + live

    def first(k):
        fill(dense_m, mine[k], mask, src[k])
        acc[...] = jnp.dot(lam_m[src[k]], dense_m[...], preferred_element_type=jnp.float32)

    def second(k):
        for q in range(CHUNKS):
            swap(k, q).wait_recv()
        fill(dense_t, theirs[k], other, src[k])
        out[0, src[k]] = (acc[...] + jnp.dot(
            lam_t[src[k]], dense_t[...], preferred_element_type=jnp.float32)).astype(jnp.bfloat16)

    def arrive(k, q):
        own_copy(k, q).wait_recv()
        if (k, q) in relays:
            relay_copy(k, q).start()
        swap(k, q).start()

    loads[3].wait()
    first(0)
    lam_swap.wait_recv()
    second(0)
    if grid:
        for i in range(CHUNKS):
            for k in direct:
                arrive(k, paths[k][i])
        first(1)
        second(1)
        arrive(3, low[0])
        arrive(3, high[0])
        first(2)
        second(2)
        for pair in zip(low[1:], high[1:]):
            arrive(3, pair[0])
            arrive(3, pair[1])
        first(3)
        second(3)
    else:
        for k in direct:
            for q in range(CHUNKS):
                arrive(k, q)
            first(k)
            second(k)

    for k in range(1, n):
        t_copies[k].wait_send()
        t_swaps[k].wait_send()
    mask_swap.wait_send()
    lam_swap.wait_send()
    for k in direct:
        for q in range(CHUNKS):
            own_copy(k, q).wait_send()
    for k, q in relays:
        relay_copy(k, q).wait_send()
    for k in range(n):
        for q in range(CHUNKS):
            swap(k, q).wait_send()


def body(n, lambda_amps, screened_ints, half_ints, singles, block_mask):
    wide, pairs, rows, half = lambda_amps.shape
    full = screened_ints.shape[2]
    inner, width = singles.shape
    blocks = (half // TILE) * (full // TILE)
    bf16, f32 = jnp.bfloat16, jnp.float32
    dma = pltpu.SemaphoreType.DMA
    anywhere = pl.BlockSpec(memory_space=pl.ANY)
    return pl.pallas_call(
        functools.partial(kernel, n),
        out_shape=pltpu.VMEM((1, pairs, rows, full), bf16),
        in_specs=[anywhere] * 4 + [pl.BlockSpec(memory_space=pltpu.SMEM), anywhere],
        out_specs=pl.BlockSpec(memory_space=pltpu.VMEM),
        scratch_shapes=[
            pltpu.VMEM((pairs, rows, half), bf16),
            pltpu.VMEM((pairs, rows, half), bf16),
            pltpu.VMEM((half, full), bf16),
            pltpu.VMEM((half, inner), bf16),
            pltpu.VMEM((blocks, TILE, TILE), bf16),
            pltpu.VMEM((half, full), bf16),
            pltpu.VMEM((half, full), bf16),
            pltpu.VMEM((rows, full), f32),
            pltpu.SMEM(block_mask.shape, jnp.int32),
            dma((4,)), dma((n,)), dma((n,)), dma((n,)), dma((n,)), dma((n, CHUNKS)), dma((n, CHUNKS)),
            dma((CHUNKS,)), dma((n, CHUNKS)), dma((n, CHUNKS)), dma((2,)), dma((2,)),
        ] + [pltpu.VMEM((inner, width), bf16)] * n + [pltpu.VMEM((CAP + 1, TILE, TILE), bf16)] * (2 * n),
        compiler_params=pltpu.CompilerParams(
            collective_id=0, has_side_effects=True, vmem_limit_bytes=56 * 1024 * 1024),
    )(lambda_amps, screened_ints, half_ints, singles, block_mask, block_mask)


def solution(mesh):
    return jax.shard_map(
        functools.partial(body, mesh.shape["vir"]),
        mesh=mesh,
        in_specs=(
            P(None, "occ", "vir", "ka"),
            P(("occ", "vir"), "ka", None),
            P(("occ", "vir"), "ka", None),
            P(None, "vir"),
            P("occ", "ka", None),
        ),
        out_specs=P("ka", "occ", "vir", None),
        check_vma=False,
    )
```

```python
import functools

import jax
import jax.numpy as jnp
from jax import lax
from jax.experimental import pallas as pl
from jax.experimental.pallas import tpu as pltpu
from jax.sharding import PartitionSpec as P

TILE = 128
CAP = 16
MESH = pl.DeviceIdType.MESH


def remote(source, target, send, recv, where):
    return pltpu.make_async_remote_copy(
        src_ref=source, dst_ref=target, send_sem=send, recv_sem=recv, device_id=where, device_id_type=MESH)


def enter(places):
    barrier = pltpu.get_barrier_semaphore()
    for place in places:
        pl.semaphore_signal(barrier, inc=1, device_id=place, device_id_type=MESH)
    return barrier


def top_row(live_of, j, row_blocks, col_blocks):
    best, most = jnp.int32(0), jnp.int32(-1)
    for e in range(row_blocks):
        total = live_of[j, e, 0]
        for b in range(1, col_blocks):
            total = total + live_of[j, e, b]
        best = jnp.where(total > most, e, best)
        most = jnp.maximum(total, most)
    return best


def raw_columns(live_of, j, row, raw, col_blocks):
    found = [jnp.int32(0)] * raw
    rank = jnp.int32(0)
    for b in range(col_blocks):
        live = live_of[j, row, b]
        found = [jnp.where((live != 0) & (rank == s), b, found[s]) for s in range(raw)]
        rank = rank + live
    return found


def slots_of(live_of, j, row, raw, late, row_blocks, col_blocks, cols):
    early_next, late_next = jnp.int32(raw), jnp.int32(CAP - 1)
    is_late = [late == g for g in range(col_blocks // cols)]
    slots = []
    for e in range(row_blocks):
        room = jnp.where(row == e, raw, 0)
        rank = jnp.int32(0)
        for b in range(col_blocks):
            live = live_of[j, e, b]
            is_raw = rank < room
            behind = is_late[b // cols]
            slot = jnp.where(is_raw, rank, jnp.where(behind, late_next, early_next))
            slots.append(jnp.where(live != 0, slot, CAP))
            step = jnp.where(is_raw, 0, live)
            late_next = late_next - jnp.where(behind, step, 0)
            early_next = early_next + jnp.where(behind, 0, step)
            rank = rank + live
    return slots


def grid_kernel(lam, x, y, t, mask_any, out, lam_m, lam_t, x_v, y_v, t_v, dressed, dense_m, dense_t, acc, mask, other,
                in_sem, x_sem, t_send, t_recv, td_send, td_recv, b_send, b_recv, f_send, d_send, d_recv, l_send, l_recv,
                *bufs):
    n = 4
    mine, theirs, raw_m, raw_t = bufs[:n], bufs[n:2 * n], bufs[2 * n:3 * n], bufs[3 * n:]
    v, c = lax.axis_index("vir"), lax.axis_index("ka")
    row, col = v // 2, v % 2
    ids = [v, row * 2 + (1 - col), (1 - row) * 2 + col, (1 - row) * 2 + (1 - col)]
    partner = 1 - c
    row_blocks, col_blocks = y_v.shape[0], t_v.shape[0]
    inner = t_v.shape[1]
    cols = col_blocks // n
    part = inner // 2
    raw = CAP // row_blocks
    late = row_blocks * cols
    first = CAP - raw - late
    f32, bf16 = jnp.float32, jnp.bfloat16

    def block(e, b):
        return x.at[0, pl.ds(e * TILE, TILE), pl.ds(b * TILE, TILE)]

    mask_load = pltpu.make_async_copy(mask_any, mask, in_sem.at[0])
    t_loads = [pltpu.make_async_copy(
        t.at[:, pl.ds(i * TILE, TILE)], t_v.at[v * cols + i], in_sem.at[1 + i]) for i in range(cols)]
    y_loads = [pltpu.make_async_copy(
        y.at[0, pl.ds(e * TILE, TILE)], y_v.at[e], in_sem.at[1 + cols + e]) for e in range(row_blocks)]
    x_loads = [pltpu.make_async_copy(
        block(p // col_blocks, p % col_blocks), x_v.at[p], x_sem.at[p]) for p in range(row_blocks * col_blocks)]
    lam_load = pltpu.make_async_copy(lam.at[c], lam_m, in_sem.at[1 + cols + row_blocks])
    mask_load.start()
    for load in t_loads + y_loads + x_loads:
        load.start()
    lam_load.start()
    to_x, to_y, to_core = {"vir": ids[1]}, {"vir": ids[2]}, {"ka": partner}
    near = [None, to_x, to_y]
    barrier = enter([to_x, to_y, to_core])

    zero = jnp.zeros((TILE, TILE), bf16)
    for k in range(n):
        mine[k][CAP] = zero
        theirs[k][CAP] = zero

    mask_load.wait()
    lead = top_row(mask, v, row_blocks, col_blocks)
    lead_columns = raw_columns(mask, v, lead, raw, col_blocks)
    for load in t_loads:
        load.wait()
    pl.semaphore_wait(barrier, 3)

    def t_part(k):
        return t_v.at[pl.ds(ids[k] * cols, cols), pl.ds(pl.multiple_of(c * part, part), part)]

    t_copies = [None] + [remote(t_part(0), t_part(0), t_send.at[k], t_recv.at[k], near[k]) for k in (1, 2)]
    t_relay = remote(t_part(1), t_part(1), t_send.at[3], t_recv.at[3], to_y)
    t_swaps = [None] + [remote(t_part(k), t_part(k), td_send.at[k], td_recv.at[k], to_core) for k in (1, 2, 3)]
    for k in (1, 2):
        t_copies[k].start()
    mask_swap = remote(mask_any, other, l_send.at[0], l_recv.at[0], to_core)
    mask_swap.start()

    for load in y_loads + x_loads:
        load.wait()
    for s in range(raw):
        raw_m[0][s] = x_v[lead * col_blocks + lead_columns[s]]
    raw_m[0][raw] = y_v[lead]

    spans = [(0, raw // 2), (raw // 2, raw + 1)]
    at = raw
    for size in [first // 2] * 2 + [late // 4] * 4:
        spans.append((at, at + size))
        at += size
    chunks = len(spans)
    low, high = (0, 2, 4, 5), (1, 3, 6, 7)
    paths = [None, (0, 1, 2, 3, 4, 5, 6, 7), (1, 0, 3, 2, 6, 7, 4, 5)]

    def chunk(raws, gathered, k, q):
        start, stop = spans[q]
        return (raws if q < 2 else gathered)[k].at[pl.ds(start, stop - start)]

    def here(k, q):
        return chunk(raw_m, mine, k, q)

    def own_copy(k, q):
        return remote(here(0, q), here(k, q), b_send.at[k, q], b_recv.at[k, q], near[k])

    def relay_copy(k, q):
        return remote(here(k, q), here(3, q), f_send.at[q], b_recv.at[3, q], near[3 - k])

    def swap(k, q):
        if k == 0 and q == 0:
            return remote(mine[0].at[pl.ds(0, raw)], theirs[0].at[pl.ds(0, raw)], d_send.at[0, 0], d_recv.at[0, 0], to_core)
        return remote(here(k, q), chunk(raw_t, theirs, k, q), d_send.at[k, q], d_recv.at[k, q], to_core)

    relays = [(1, q) for q in low] + [(2, q) for q in high]

    own_copy(1, 0).start()
    own_copy(2, 1).start()
    own_copy(1, 1).start()

    def dress(k):
        for i in range(cols):
            b = ids[k] * cols + i
            columns = t_v[b]
            for e in range(row_blocks):
                term = jnp.dot(y_v[e], columns, preferred_element_type=f32)
                dressed[e * col_blocks + b] = (x_v[e * col_blocks + b].astype(f32) - term).astype(bf16)

    slots = slots_of(mask, v, lead, raw, n - 1 - v, row_blocks, col_blocks, cols)
    order = []
    for s in range(raw, CAP):
        place = jnp.int32(0)
        for p, slot in enumerate(slots):
            place = jnp.where(slot == s, p, place)
        order.append(place)

    dress(0)
    t_copies[1].wait_recv()
    t_relay.start()
    own_copy(2, 0).start()
    t_swaps[1].start()
    t_copies[2].wait_recv()
    t_swaps[2].start()
    for k in (1, 2):
        t_swaps[k].wait_recv()
        dress(k)

    def pack(q):
        for s in range(*spans[q]):
            mine[0][s] = dressed[order[s - raw]]

    pack(2)
    pack(3)
    for i in (2, 3):
        for k in (1, 2):
            own_copy(k, paths[k][i]).start()
    t_relay.wait_recv()
    t_swaps[3].start()
    t_swaps[3].wait_recv()
    dress(3)
    for i in range(4, chunks):
        if i < 6:
            for k in (1, 2):
                pack(paths[k][i])
        for k in (1, 2):
            own_copy(k, paths[k][i]).start()
    for s in range(raw):
        mine[0][s] = dressed[lead * col_blocks + lead_columns[s]]
    swaps_of = [[0] + list(range(2, chunks))] + [list(range(chunks))] * 3
    for q in swaps_of[0]:
        swap(0, q).start()
    lam_swap = remote(lam.at[partner], lam_t, l_send.at[1], l_recv.at[1], to_core)
    lam_swap.start()
    mask_swap.wait_recv()

    def mend(k, raws, gathered, live_of):
        best = top_row(live_of, ids[k], row_blocks, col_blocks)
        places = raw_columns(live_of, ids[k], best, raw, col_blocks)
        rows = raws[k][raw]
        for s in range(raw):
            term = jnp.dot(rows, t_v[places[s]], preferred_element_type=f32)
            gathered[k][s] = (raws[k][s].astype(f32) - term).astype(bf16)

    def fill(dense, gathered, live_of, k):
        j = ids[k]
        best = top_row(live_of, j, row_blocks, col_blocks)
        slots = slots_of(live_of, j, best, raw, n - 1 - j, row_blocks, col_blocks, cols)
        for p, slot in enumerate(slots):
            e, b = p // col_blocks, p % col_blocks
            dense[e * TILE:(e + 1) * TILE, b * TILE:(b + 1) * TILE] = gathered[k][slot]

    def own_half(k):
        fill(dense_m, mine, mask, k)
        acc[...] = jnp.dot(lam_m[ids[k]], dense_m[...], preferred_element_type=f32)

    def other_half(k):
        for q in swaps_of[k]:
            if k == 0 or q >= 2:
                swap(k, q).wait_recv()
        fill(dense_t, theirs, other, k)
        out[0, ids[k]] = (acc[...] + jnp.dot(
            lam_t[ids[k]], dense_t[...], preferred_element_type=f32)).astype(bf16)

    def arrive(k, q):
        own_copy(1, q).wait_recv() if k == 1 else own_copy(2, q).wait_recv() if k == 2 else relay_copy(1, q).wait_recv()
        if (k, q) in relays:
            relay_copy(k, q).start()
        swap(k, q).start()

    def mend_both(k):
        mend(k, raw_m, mine, mask)
        for q in (0, 1):
            swap(k, q).wait_recv()
        mend(k, raw_t, theirs, other)

    for i in (0, 1):
        for k in (1, 2):
            arrive(k, paths[k][i])
    mend_both(1)
    mend_both(2)
    for i in (2, 3):
        for k in (1, 2):
            arrive(k, paths[k][i])
    lam_load.wait()
    lam_swap.wait_recv()
    own_half(0)
    other_half(0)
    for i in range(4, chunks):
        for k in (1, 2):
            arrive(k, paths[k][i])
    own_half(1)
    other_half(1)
    arrive(3, 0)
    arrive(3, 1)
    mend_both(3)
    own_half(2)
    other_half(2)
    for pair in zip(low[1:], high[1:]):
        for q in pair:
            arrive(3, q)
    own_half(3)
    other_half(3)

    for k in (1, 2):
        t_copies[k].wait_send()
        for q in range(chunks):
            own_copy(k, q).wait_send()
    t_relay.wait_send()
    for k in (1, 2, 3):
        t_swaps[k].wait_send()
    mask_swap.wait_send()
    lam_swap.wait_send()
    for k, q in relays:
        relay_copy(k, q).wait_send()
    for k in range(n):
        for q in swaps_of[k]:
            swap(k, q).wait_send()


def ring_kernel(n, lam, x, y, t, mask_any, out, lam_m, lam_t, x_v, y_v, t_v, dressed, dense_m, dense_t, acc, mask, other,
                in_sem, t_send, t_recv, b_send, b_recv, d_send, d_recv, l_send, l_recv, *bufs):
    mine, theirs = bufs[:n], bufs[n:]
    v, c = lax.axis_index("vir"), lax.axis_index("ka")
    dst, src = [(v + k) % n for k in range(n)], [(v + n - k) % n for k in range(n)]
    half, full = x_v.shape
    width = t_v.shape[2]
    row_blocks, col_blocks = half // TILE, full // TILE
    f32, bf16 = jnp.float32, jnp.bfloat16
    loads = [pltpu.make_async_copy(source, target, in_sem.at[i]) for i, (source, target) in enumerate(
        [(mask_any, mask), (t, t_v.at[v]), (y.at[0], y_v), (x.at[0], x_v), (lam.at[c], lam_m)])]
    for load in loads:
        load.start()
    to_core = {"ka": 1 - c}
    barrier = enter([{"vir": dst[k]} for k in range(1, n)] + [to_core])
    for load in loads:
        load.wait()
    pl.semaphore_wait(barrier, n)

    t_copies = [remote(t_v.at[v], t_v.at[v], t_send.at[k], t_recv.at[k], {"vir": dst[k]}) for k in range(1, n)]
    arrivals = [remote(t_v.at[v], t_v.at[src[k]], t_send.at[k], t_recv.at[k], {"vir": dst[k]}) for k in range(1, n)]
    for copy in t_copies:
        copy.start()
    mask_swap = remote(mask_any, other, l_send.at[0], l_recv.at[0], to_core)
    lam_swap = remote(lam.at[1 - c], lam_t, l_send.at[1], l_recv.at[1], to_core)
    mask_swap.start()
    lam_swap.start()

    zero = jnp.zeros((TILE, TILE), bf16)
    for k in range(n):
        mine[k][CAP] = zero
        theirs[k][CAP] = zero
    order = [jnp.int32(0)] * CAP
    count = jnp.int32(0)
    for p in range(row_blocks * col_blocks):
        live = mask[v, p // col_blocks, p % col_blocks]
        order = [jnp.where((live != 0) & (count == s), p, order[s]) for s in range(CAP)]
        count = count + live

    for copy in arrivals:
        copy.wait_recv()
    for b in range(col_blocks):
        if width >= TILE:
            owner, offset = b * TILE // width, b * TILE % width
            columns = t_v[owner][:, offset:offset + TILE]
        else:
            group = TILE // width
            columns = jnp.concatenate([t_v[b * group + i] for i in range(group)], axis=1)
        term = jnp.dot(y_v[...], columns, preferred_element_type=f32)
        value = (x_v[:, b * TILE:(b + 1) * TILE].astype(f32) - term).astype(bf16)
        for e in range(row_blocks):
            dressed[e * col_blocks + b] = value[e * TILE:(e + 1) * TILE]
    for s in range(CAP):
        mine[0][s] = dressed[order[s]]

    def live_part(ref):
        return ref.at[pl.ds(0, CAP)]

    copies = [None] + [
        remote(live_part(mine[0]), live_part(mine[k]), b_send.at[k], b_recv.at[k], {"vir": dst[k]}) for k in range(1, n)]
    swaps = [remote(live_part(mine[k]), live_part(theirs[k]), d_send.at[k], d_recv.at[k], to_core) for k in range(n)]
    for copy in copies[1:]:
        copy.start()

    def fill(dense, gathered, live_of, j):
        count = jnp.int32(0)
        for e in range(row_blocks):
            for b in range(col_blocks):
                live = live_of[j, e, b]
                dense[e * TILE:(e + 1) * TILE, b * TILE:(b + 1) * TILE] = gathered[jnp.where(live != 0, count, CAP)]
                count = count + live

    mask_swap.wait_recv()
    lam_swap.wait_recv()
    for k in range(n):
        if k:
            copies[k].wait_recv()
        swaps[k].start()
        fill(dense_m, mine[k], mask, src[k])
        acc[...] = jnp.dot(lam_m[src[k]], dense_m[...], preferred_element_type=f32)
        swaps[k].wait_recv()
        fill(dense_t, theirs[k], other, src[k])
        out[0, src[k]] = (acc[...] + jnp.dot(
            lam_t[src[k]], dense_t[...], preferred_element_type=f32)).astype(bf16)

    for copy in t_copies + copies[1:] + swaps + [mask_swap, lam_swap]:
        copy.wait_send()


def body(n, lambda_amps, screened_ints, half_ints, singles, block_mask):
    wide, pairs, rows, half = lambda_amps.shape
    full = screened_ints.shape[2]
    inner, width = singles.shape
    row_blocks, col_blocks = half // TILE, full // TILE
    blocks = row_blocks * col_blocks
    bf16, f32 = jnp.bfloat16, jnp.float32
    dma = pltpu.SemaphoreType.DMA
    grid = n == 4
    tile = (TILE, TILE)
    lams = [pltpu.VMEM((pairs, rows, half), bf16)] * 2
    work = [pltpu.VMEM((half, full), bf16)] * 2 + [pltpu.VMEM((rows, full), f32)] + [
        pltpu.SMEM(block_mask.shape, jnp.int32)] * 2
    held = [pltpu.VMEM((CAP + 1,) + tile, bf16)] * (2 * n)
    if grid:
        raw = CAP // row_blocks
        chunks = 8
        scratch = lams + [
            pltpu.VMEM((blocks,) + tile, bf16), pltpu.VMEM((row_blocks, TILE, inner), bf16),
            pltpu.VMEM((col_blocks, inner, TILE), bf16), pltpu.VMEM((blocks,) + tile, bf16),
        ] + work + [
            dma((2 + width // TILE + row_blocks,)), dma((blocks,)), dma((n,)), dma((n,)), dma((n,)), dma((n,)),
            dma((n, chunks)), dma((n, chunks)), dma((chunks,)), dma((n, chunks)), dma((n, chunks)), dma((2,)), dma((2,)),
        ] + held + [pltpu.VMEM((raw + 1,) + tile, bf16)] * (2 * n)
    else:
        scratch = lams + [
            pltpu.VMEM((half, full), bf16), pltpu.VMEM((half, inner), bf16), pltpu.VMEM((n, inner, width), bf16),
            pltpu.VMEM((blocks,) + tile, bf16),
        ] + work + [dma((5,)), dma((n,)), dma((n,)), dma((n,)), dma((n,)), dma((n,)), dma((n,)), dma((2,)), dma((2,))] + held
    return pl.pallas_call(
        grid_kernel if grid else functools.partial(ring_kernel, n),
        out_shape=pltpu.VMEM((1, pairs, rows, full), bf16),
        in_specs=[pl.BlockSpec(memory_space=pl.ANY)] * 5,
        out_specs=pl.BlockSpec(memory_space=pltpu.VMEM),
        scratch_shapes=scratch,
        compiler_params=pltpu.CompilerParams(
            collective_id=0, has_side_effects=True, vmem_limit_bytes=56 * 1024 * 1024),
    )(lambda_amps, screened_ints, half_ints, singles, block_mask)


def solution(mesh):
    return jax.shard_map(
        functools.partial(body, mesh.shape["vir"]),
        mesh=mesh,
        in_specs=(
            P(None, "occ", "vir", "ka"),
            P(("occ", "vir"), "ka", None),
            P(("occ", "vir"), "ka", None),
            P(None, "vir"),
            P("occ", "ka", None),
        ),
        out_specs=P("ka", "occ", "vir", None),
        check_vma=False,
    )
```

```python
import functools

import jax
import jax.numpy as jnp
from jax import lax
from jax.experimental import pallas as pl
from jax.experimental.pallas import tpu as pltpu
from jax.sharding import PartitionSpec as P

TILE = 128
CAP = 16
MESH = pl.DeviceIdType.MESH


def remote(source, target, send, recv, where):
    return pltpu.make_async_remote_copy(
        src_ref=source, dst_ref=target, send_sem=send, recv_sem=recv, device_id=where, device_id_type=MESH)


def enter(places):
    barrier = pltpu.get_barrier_semaphore()
    for place in places:
        pl.semaphore_signal(barrier, inc=1, device_id=place, device_id_type=MESH)
    return barrier


def top_row(live_of, j, row_blocks, col_blocks):
    best, most = jnp.int32(0), jnp.int32(-1)
    for e in range(row_blocks):
        total = live_of[j, e, 0]
        for b in range(1, col_blocks):
            total = total + live_of[j, e, b]
        best = jnp.where(total > most, e, best)
        most = jnp.maximum(total, most)
    return best


def raw_columns(live_of, j, row, raw, col_blocks):
    found = [jnp.int32(0)] * raw
    rank = jnp.int32(0)
    for b in range(col_blocks):
        live = live_of[j, row, b]
        found = [jnp.where((live != 0) & (rank == s), b, found[s]) for s in range(raw)]
        rank = rank + live
    return found


def slots_of(live_of, j, row, raw, late, row_blocks, col_blocks, cols):
    early_next, late_next = jnp.int32(raw), jnp.int32(CAP - 1)
    is_late = [late == g for g in range(col_blocks // cols)]
    slots = []
    for e in range(row_blocks):
        room = jnp.where(row == e, raw, 0)
        rank = jnp.int32(0)
        for b in range(col_blocks):
            live = live_of[j, e, b]
            is_raw = rank < room
            behind = is_late[b // cols]
            slot = jnp.where(is_raw, rank, jnp.where(behind, late_next, early_next))
            slots.append(jnp.where(live != 0, slot, CAP))
            step = jnp.where(is_raw, 0, live)
            late_next = late_next - jnp.where(behind, step, 0)
            early_next = early_next + jnp.where(behind, 0, step)
            rank = rank + live
    return slots


def grid_kernel(lam, x, y, t, mask_any, out, lam_m, lam_t, x_v, y_v, t_v, dressed, dense_m, dense_t, acc, mask, other,
                in_sem, t_send, t_recv, td_send, td_recv, b_send, b_recv, f_send, d_send, d_recv, r_recv, l_send, l_recv,
                *bufs):
    n = 4
    mine, theirs, raw_m, raw_t = bufs[:n], bufs[n:2 * n], bufs[2 * n:3 * n], bufs[3 * n:]
    v, c = lax.axis_index("vir"), lax.axis_index("ka")
    row, col = v // 2, v % 2
    ids = [v, row * 2 + (1 - col), (1 - row) * 2 + col, (1 - row) * 2 + (1 - col)]
    partner = 1 - c
    row_blocks, col_blocks = y_v.shape[0], t_v.shape[0]
    inner = t_v.shape[1]
    cols = col_blocks // n
    part = inner // 2
    raw = CAP // row_blocks
    late = row_blocks * cols
    first = CAP - raw - late
    f32, bf16 = jnp.float32, jnp.bfloat16

    def block(e, b):
        return x.at[0, pl.ds(e * TILE, TILE), pl.ds(b * TILE, TILE)]

    mask_load = pltpu.make_async_copy(mask_any, mask, in_sem.at[0])
    t_own = t_v.at[pl.ds(v * cols, cols)]
    t_loads = [pltpu.make_async_copy(
        t.at[:, pl.ds(i * TILE, TILE)], t_v.at[v * cols + i], in_sem.at[1]) for i in range(cols)]
    y_loads = [pltpu.make_async_copy(
        y.at[0, pl.ds(e * TILE, TILE)], y_v.at[e], in_sem.at[2]) for e in range(row_blocks)]
    x_loads = [pltpu.make_async_copy(
        block(p // col_blocks, p % col_blocks), x_v.at[p], in_sem.at[3]) for p in range(row_blocks * col_blocks)]
    lam_load = pltpu.make_async_copy(lam.at[c], lam_m, in_sem.at[4])
    mask_load.start()
    for load in t_loads + y_loads + x_loads:
        load.start()
    lam_load.start()
    to_x, to_y, to_core = {"vir": ids[1]}, {"vir": ids[2]}, {"ka": partner}
    near = [None, to_x, to_y]
    barrier = enter([to_x, to_y, to_core])

    zero = jnp.zeros((TILE, TILE), bf16)
    for k in range(n):
        mine[k][CAP] = zero
        theirs[k][CAP] = zero

    mask_load.wait()
    lead = top_row(mask, v, row_blocks, col_blocks)
    lead_columns = raw_columns(mask, v, lead, raw, col_blocks)
    pltpu.make_async_copy(t_own, t_own, in_sem.at[1]).wait()
    pl.semaphore_wait(barrier, 3)

    def t_part(k):
        return t_v.at[pl.ds(ids[k] * cols, cols)]

    t_copies = [None] + [remote(t_part(0), t_part(0), t_send.at[0], t_recv.at[k], near[k]) for k in (1, 2)]
    t_relay = remote(t_part(1), t_part(1), t_send.at[0], t_recv.at[0], to_y)
    t_swaps = [None] + [remote(t_part(k), t_part(k), td_send.at[0], td_recv.at[k - 1], to_core) for k in (1, 2, 3)]

    @pl.when(c == 1)
    def _():
        for k in (1, 2):
            t_copies[k].start()

    mask_swap = remote(mask_any, other, l_send.at[0], l_recv.at[0], to_core)
    mask_swap.start()

    pltpu.make_async_copy(y_v, y_v, in_sem.at[2]).wait()
    pltpu.make_async_copy(x_v, x_v, in_sem.at[3]).wait()
    for s in range(raw):
        raw_m[0][s] = x_v[lead * col_blocks + lead_columns[s]]
    raw_m[0][raw] = y_v[lead]

    spans = [(0, raw // 2), (raw // 2, raw + 1)]
    at = raw
    for size in [first // 2] * 2 + [late // 4] * 4:
        spans.append((at, at + size))
        at += size
    low, high = (0, 2, 4, 5), (1, 3, 6, 7)
    groups = [(0, 0), (1, 1), (2, 2), (3, 3), (4, 5), (6, 7)]
    paths = [None, (0, 1, 2, 3, 4, 5), (1, 0, 3, 2, 5, 4)]

    def chunk(raws, gathered, k, q, r):
        start, stop = spans[q][0], spans[r][1]
        return (raws if q < 2 else gathered)[k].at[pl.ds(start, stop - start)]

    def own_copy(k, g):
        q, r = groups[g]
        return remote(chunk(raw_m, mine, 0, q, r), chunk(raw_m, mine, k, q, r), b_send.at[k - 1], b_recv.at[k - 1, q], near[k])

    def relay_copy(k, q):
        return remote(chunk(raw_m, mine, k, q, q), chunk(raw_m, mine, 3, q, q), f_send.at[0], b_recv.at[2, q], near[3 - k])

    def swap(k, q, r):
        return remote(chunk(raw_m, mine, k, q, r), chunk(raw_t, theirs, k, q, r), d_send.at[k],
                      r_recv.at[k - 1] if q < 2 else d_recv.at[k], to_core)

    own_swap = remote(mine[0].at[pl.ds(0, CAP)], theirs[0].at[pl.ds(0, CAP)], d_send.at[0], d_recv.at[0], to_core)
    lam_swap = remote(lam.at[partner], lam_t, l_send.at[1], l_recv.at[1], to_core)

    own_copy(1, 0).start()
    own_copy(2, 1).start()
    own_copy(1, 1).start()

    @pl.when(c == 0)
    def _():
        own_copy(2, 0).start()
        lam_swap.start()

    def dress(k):
        for i in range(cols):
            b = ids[k] * cols + i
            columns = t_v[b]
            for e in range(row_blocks):
                term = jnp.dot(y_v[e], columns, preferred_element_type=f32)
                dressed[e * col_blocks + b] = (x_v[e * col_blocks + b].astype(f32) - term).astype(bf16)

    slots = slots_of(mask, v, lead, raw, n - 1 - v, row_blocks, col_blocks, cols)
    order = []
    for s in range(raw, CAP):
        place = jnp.int32(0)
        for p, slot in enumerate(slots):
            place = jnp.where(slot == s, p, place)
        order.append(place)

    dress(0)
    @pl.when(c == 1)
    def _():
        t_copies[1].wait_recv()
        t_relay.start()
        own_copy(2, 0).start()
        t_swaps[1].start()
        t_copies[2].wait_recv()
        t_swaps[2].start()

    @pl.when(c == 0)
    def _():
        t_swaps[1].wait_recv()
        t_swaps[2].wait_recv()

    dress(1)
    dress(2)

    def pack(q):
        for s in range(*spans[q]):
            mine[0][s] = dressed[order[s - raw]]

    pack(2)
    pack(3)
    for i in (2, 3):
        for k in (1, 2):
            own_copy(k, paths[k][i]).start()
    @pl.when(c == 1)
    def _():
        t_relay.wait_recv()
        t_swaps[3].start()
        lam_swap.start()

    @pl.when(c == 0)
    def _():
        t_swaps[3].wait_recv()

    dress(3)
    for i in (4, 5):
        for q in groups[i]:
            pack(q)
    for i in (4, 5):
        for k in (1, 2):
            own_copy(k, paths[k][i]).start()
    for s in range(raw):
        mine[0][s] = dressed[lead * col_blocks + lead_columns[s]]
    own_swap.start()
    mask_swap.wait_recv()

    def mend(k, raws, gathered, live_of):
        best = top_row(live_of, ids[k], row_blocks, col_blocks)
        places = raw_columns(live_of, ids[k], best, raw, col_blocks)
        rows = raws[k][raw]
        for s in range(raw):
            term = jnp.dot(rows, t_v[places[s]], preferred_element_type=f32)
            gathered[k][s] = (raws[k][s].astype(f32) - term).astype(bf16)

    def places(live_of, k):
        j = ids[k]
        best = top_row(live_of, j, row_blocks, col_blocks)
        return slots_of(live_of, j, best, raw, n - 1 - j, row_blocks, col_blocks, cols)

    def fill(dense, gathered, slots):
        for p, slot in enumerate(slots):
            e, b = p // col_blocks, p % col_blocks
            dense[e * TILE:(e + 1) * TILE, b * TILE:(b + 1) * TILE] = gathered[slot]

    def own_half(k, slots):
        fill(dense_m, mine[k], slots)
        acc[...] = jnp.dot(lam_m[ids[k]], dense_m[...], preferred_element_type=f32)

    def other_half(k, slots):
        if k == 0:
            own_swap.wait_recv()
        else:
            swap(k, 2, 7).wait_recv()
        fill(dense_t, theirs[k], slots)
        out[0, ids[k]] = (acc[...] + jnp.dot(
            lam_t[ids[k]], dense_t[...], preferred_element_type=f32)).astype(bf16)

    def both(k):
        own_half(k, places(mask, k))
        other_half(k, places(other, k))

    def arrive(k, g):
        own_copy(k, g).wait_recv()
        q, r = groups[g]
        for piece in range(q, r + 1):
            if piece in (low if k == 1 else high):
                relay_copy(k, piece).start()
        swap(k, q, r).start()

    def arrive_relayed(q):
        relay_copy(1, q).wait_recv()
        swap(3, q, q).start()

    def mend_both(k):
        mend(k, raw_m, mine, mask)
        swap(k, 0, 1).wait_recv()
        mend(k, raw_t, theirs, other)

    for i in (0, 1):
        for k in (1, 2):
            arrive(k, paths[k][i])
    for i in (2, 3):
        for k in (1, 2):
            arrive(k, paths[k][i])
    mend_both(1)
    mend_both(2)
    lam_load.wait()
    lam_swap.wait_recv()
    both(0)
    for i in (4, 5):
        for k in (1, 2):
            arrive(k, paths[k][i])
    both(1)
    arrive_relayed(0)
    arrive_relayed(1)
    mend_both(3)
    both(2)
    here, there = places(mask, 3), places(other, 3)
    for pair in zip(low[1:], high[1:]):
        for q in pair:
            arrive_relayed(q)
    own_half(3, here)
    other_half(3, there)

    @pl.when(c == 1)
    def _():
        sent = remote(t_v.at[pl.ds(0, 3 * cols)], t_v.at[pl.ds(0, 3 * cols)], t_send.at[0], t_recv.at[0], to_x)
        sent.wait_send()
        passed = remote(t_v.at[pl.ds(0, 3 * cols)], t_v.at[pl.ds(0, 3 * cols)], td_send.at[0], td_recv.at[0], to_core)
        passed.wait_send()

    mask_swap.wait_send()
    lam_swap.wait_send()
    for k in (1, 2):
        remote(mine[0], mine[k], b_send.at[k - 1], b_recv.at[0, 0], near[k]).wait_send()
    remote(mine[1], mine[3], f_send.at[0], b_recv.at[2, 0], to_y).wait_send()
    own_swap.wait_send()
    for k in (1, 2, 3):
        remote(mine[k], theirs[k], d_send.at[k], d_recv.at[k], to_core).wait_send()


def ring_kernel(n, lam, x, y, t, mask_any, out, lam_m, lam_t, x_v, y_v, t_v, dressed, dense_m, dense_t, acc, mask, other,
                in_sem, t_send, t_recv, b_send, b_recv, d_send, d_recv, l_send, l_recv, *bufs):
    mine, theirs = bufs[:n], bufs[n:]
    v, c = lax.axis_index("vir"), lax.axis_index("ka")
    dst, src = [(v + k) % n for k in range(n)], [(v + n - k) % n for k in range(n)]
    half, full = x_v.shape
    width = t_v.shape[2]
    row_blocks, col_blocks = half // TILE, full // TILE
    f32, bf16 = jnp.float32, jnp.bfloat16
    loads = [pltpu.make_async_copy(source, target, in_sem.at[i]) for i, (source, target) in enumerate(
        [(mask_any, mask), (t, t_v.at[v]), (y.at[0], y_v), (x.at[0], x_v), (lam.at[c], lam_m)])]
    for load in loads:
        load.start()
    to_core = {"ka": 1 - c}
    barrier = enter([{"vir": dst[k]} for k in range(1, n)] + [to_core])
    for load in loads:
        load.wait()
    pl.semaphore_wait(barrier, n)

    t_copies = [remote(t_v.at[v], t_v.at[v], t_send.at[k], t_recv.at[k], {"vir": dst[k]}) for k in range(1, n)]
    arrivals = [remote(t_v.at[v], t_v.at[src[k]], t_send.at[k], t_recv.at[k], {"vir": dst[k]}) for k in range(1, n)]
    for copy in t_copies:
        copy.start()
    mask_swap = remote(mask_any, other, l_send.at[0], l_recv.at[0], to_core)
    lam_swap = remote(lam.at[1 - c], lam_t, l_send.at[1], l_recv.at[1], to_core)
    mask_swap.start()
    lam_swap.start()

    zero = jnp.zeros((TILE, TILE), bf16)
    for k in range(n):
        mine[k][CAP] = zero
        theirs[k][CAP] = zero
    order = [jnp.int32(0)] * CAP
    count = jnp.int32(0)
    for p in range(row_blocks * col_blocks):
        live = mask[v, p // col_blocks, p % col_blocks]
        order = [jnp.where((live != 0) & (count == s), p, order[s]) for s in range(CAP)]
        count = count + live

    for copy in arrivals:
        copy.wait_recv()
    for b in range(col_blocks):
        if width >= TILE:
            owner, offset = b * TILE // width, b * TILE % width
            columns = t_v[owner][:, offset:offset + TILE]
        else:
            group = TILE // width
            columns = jnp.concatenate([t_v[b * group + i] for i in range(group)], axis=1)
        term = jnp.dot(y_v[...], columns, preferred_element_type=f32)
        value = (x_v[:, b * TILE:(b + 1) * TILE].astype(f32) - term).astype(bf16)
        for e in range(row_blocks):
            dressed[e * col_blocks + b] = value[e * TILE:(e + 1) * TILE]
    for s in range(CAP):
        mine[0][s] = dressed[order[s]]

    def live_part(ref):
        return ref.at[pl.ds(0, CAP)]

    copies = [None] + [
        remote(live_part(mine[0]), live_part(mine[k]), b_send.at[k], b_recv.at[k], {"vir": dst[k]}) for k in range(1, n)]
    swaps = [remote(live_part(mine[k]), live_part(theirs[k]), d_send.at[k], d_recv.at[k], to_core) for k in range(n)]
    for copy in copies[1:]:
        copy.start()

    def fill(dense, gathered, live_of, j):
        count = jnp.int32(0)
        for e in range(row_blocks):
            for b in range(col_blocks):
                live = live_of[j, e, b]
                dense[e * TILE:(e + 1) * TILE, b * TILE:(b + 1) * TILE] = gathered[jnp.where(live != 0, count, CAP)]
                count = count + live

    mask_swap.wait_recv()
    lam_swap.wait_recv()
    for k in range(n):
        if k:
            copies[k].wait_recv()
        swaps[k].start()
        fill(dense_m, mine[k], mask, src[k])
        acc[...] = jnp.dot(lam_m[src[k]], dense_m[...], preferred_element_type=f32)
        swaps[k].wait_recv()
        fill(dense_t, theirs[k], other, src[k])
        out[0, src[k]] = (acc[...] + jnp.dot(
            lam_t[src[k]], dense_t[...], preferred_element_type=f32)).astype(bf16)

    for copy in t_copies + copies[1:] + swaps + [mask_swap, lam_swap]:
        copy.wait_send()


def body(n, lambda_amps, screened_ints, half_ints, singles, block_mask):
    wide, pairs, rows, half = lambda_amps.shape
    full = screened_ints.shape[2]
    inner, width = singles.shape
    row_blocks, col_blocks = half // TILE, full // TILE
    blocks = row_blocks * col_blocks
    bf16, f32 = jnp.bfloat16, jnp.float32
    dma = pltpu.SemaphoreType.DMA
    grid = n == 4
    tile = (TILE, TILE)
    lams = [pltpu.VMEM((pairs, rows, half), bf16)] * 2
    work = [pltpu.VMEM((half, full), bf16)] * 2 + [pltpu.VMEM((rows, full), f32)] + [
        pltpu.SMEM(block_mask.shape, jnp.int32)] * 2
    held = [pltpu.VMEM((CAP + 1,) + tile, bf16)] * (2 * n)
    if grid:
        raw = CAP // row_blocks
        chunks = 8
        scratch = lams + [
            pltpu.VMEM((blocks,) + tile, bf16), pltpu.VMEM((row_blocks, TILE, inner), bf16),
            pltpu.VMEM((col_blocks, inner, TILE), bf16), pltpu.VMEM((blocks,) + tile, bf16),
        ] + work + [
            dma((5,)), dma((1,)), dma((3,)), dma((1,)), dma((3,)), dma((2,)), dma((3, chunks)), dma((1,)), dma((n,)), dma((n,)),
            dma((3,)), dma((2,)), dma((2,)),
        ] + held + [pltpu.VMEM((raw + 1,) + tile, bf16)] * (2 * n)
    else:
        scratch = lams + [
            pltpu.VMEM((half, full), bf16), pltpu.VMEM((half, inner), bf16), pltpu.VMEM((n, inner, width), bf16),
            pltpu.VMEM((blocks,) + tile, bf16),
        ] + work + [dma((5,)), dma((n,)), dma((n,)), dma((n,)), dma((n,)), dma((n,)), dma((n,)), dma((2,)), dma((2,))] + held
    return pl.pallas_call(
        grid_kernel if grid else functools.partial(ring_kernel, n),
        out_shape=pltpu.VMEM((1, pairs, rows, full), bf16),
        in_specs=[pl.BlockSpec(memory_space=pl.ANY)] * 5,
        out_specs=pl.BlockSpec(memory_space=pltpu.VMEM),
        scratch_shapes=scratch,
        compiler_params=pltpu.CompilerParams(
            collective_id=0, has_side_effects=True, vmem_limit_bytes=56 * 1024 * 1024),
    )(lambda_amps, screened_ints, half_ints, singles, block_mask)


def solution(mesh):
    return jax.shard_map(
        functools.partial(body, mesh.shape["vir"]),
        mesh=mesh,
        in_specs=(
            P(None, "occ", "vir", "ka"),
            P(("occ", "vir"), "ka", None),
            P(("occ", "vir"), "ka", None),
            P(None, "vir"),
            P("occ", "ka", None),
        ),
        out_specs=P("ka", "occ", "vir", None),
        check_vma=False,
    )
```

```python
import functools

import jax
import jax.numpy as jnp
from jax import lax
from jax.experimental import pallas as pl
from jax.experimental.pallas import tpu as pltpu
from jax.sharding import PartitionSpec as P

TILE = 128
CAP = 16
MESH = pl.DeviceIdType.MESH


def remote(source, target, send, recv, where):
    return pltpu.make_async_remote_copy(
        src_ref=source, dst_ref=target, send_sem=send, recv_sem=recv, device_id=where, device_id_type=MESH)


def enter(places):
    barrier = pltpu.get_barrier_semaphore()
    for place in places:
        pl.semaphore_signal(barrier, inc=1, device_id=place, device_id_type=MESH)
    return barrier


def top_row(live_of, j, row_blocks, col_blocks):
    best, most = jnp.int32(0), jnp.int32(-1)
    for e in range(row_blocks):
        total = live_of[j, e, 0]
        for b in range(1, col_blocks):
            total = total + live_of[j, e, b]
        best = jnp.where(total > most, e, best)
        most = jnp.maximum(total, most)
    return best


def raw_columns(live_of, j, row, raw, col_blocks):
    found = [jnp.int32(0)] * raw
    rank = jnp.int32(0)
    for b in range(col_blocks):
        live = live_of[j, row, b]
        found = [jnp.where((live != 0) & (rank == s), b, found[s]) for s in range(raw)]
        rank = rank + live
    return found


def slots_of(live_of, j, row, raw, late, row_blocks, col_blocks, cols):
    early_next, late_next = jnp.int32(raw), jnp.int32(CAP - 1)
    is_late = [late == g for g in range(col_blocks // cols)]
    slots = []
    for e in range(row_blocks):
        room = jnp.where(row == e, raw, 0)
        rank = jnp.int32(0)
        for b in range(col_blocks):
            live = live_of[j, e, b]
            is_raw = rank < room
            behind = is_late[b // cols]
            slot = jnp.where(is_raw, rank, jnp.where(behind, late_next, early_next))
            slots.append(jnp.where(live != 0, slot, CAP))
            step = jnp.where(is_raw, 0, live)
            late_next = late_next - jnp.where(behind, step, 0)
            early_next = early_next + jnp.where(behind, 0, step)
            rank = rank + live
    return slots


def grid_kernel(lam, x, y, t, mask_any, stage, dense_t, lam_last, acc, lam_m, lam_t, x_v, y_v, t_v, dressed, dense_m, mask, other,
                spare, in_sem, s_sem, t_recv, b_recv, d_recv, *bufs):
    n = 4
    mine, theirs, raw_m, raw_t = bufs[:n], bufs[n:2 * n], bufs[2 * n:3 * n], bufs[3 * n:]
    v, c = lax.axis_index("vir"), lax.axis_index("ka")
    row, col = v // 2, v % 2
    ids = [v, row * 2 + (1 - col), (1 - row) * 2 + col, (1 - row) * 2 + (1 - col)]
    partner = 1 - c
    row_blocks, col_blocks = y_v.shape[0], t_v.shape[0]
    inner = t_v.shape[1]
    cols = col_blocks // n
    part = inner // 2
    raw = CAP // row_blocks
    late = row_blocks * cols
    first = CAP - raw - late
    lam_blocks = lam_m.shape[0] * lam_m.shape[1] * lam_m.shape[2] // (TILE * TILE)
    f32, bf16 = jnp.float32, jnp.bfloat16

    def block(e, b):
        return x.at[0, pl.ds(e * TILE, TILE), pl.ds(b * TILE, TILE)]

    def drain(sem, count):
        pltpu.make_async_copy(spare.at[pl.ds(0, count)], spare.at[pl.ds(0, count)], sem).wait()

    mask_load = pltpu.make_async_copy(mask_any, mask, in_sem.at[0])
    t_loads = [pltpu.make_async_copy(
        t.at[:, pl.ds(i * TILE, TILE)], t_v.at[v * cols + i], in_sem.at[1]) for i in range(cols)]
    y_loads = [pltpu.make_async_copy(
        y.at[0, pl.ds(e * TILE, TILE)], y_v.at[e], in_sem.at[2]) for e in range(row_blocks)]
    x_loads = [pltpu.make_async_copy(
        block(p // col_blocks, p % col_blocks), x_v.at[p], in_sem.at[2]) for p in range(row_blocks * col_blocks)]
    lam_load = pltpu.make_async_copy(lam.at[c], lam_m, in_sem.at[3])
    mask_load.start()
    for load in t_loads + y_loads + x_loads:
        load.start()
    lam_load.start()
    to_x, to_y, to_core = {"vir": ids[1]}, {"vir": ids[2]}, {"ka": partner}
    near = [None, to_x, to_y]
    barrier = enter([to_x, to_y, to_core])

    zero = jnp.zeros((TILE, TILE), bf16)
    for k in range(n):
        mine[k][CAP] = zero
        theirs[k][CAP] = zero

    mask_load.wait()
    lead = top_row(mask, v, row_blocks, col_blocks)
    lead_columns = raw_columns(mask, v, lead, raw, col_blocks)
    drain(in_sem.at[1], cols)
    pl.semaphore_wait(barrier, 3)

    def t_part(k):
        return t_v.at[pl.ds(ids[k] * cols, cols)]

    t_copies = [None] + [remote(t_part(0), t_part(0), s_sem.at[1], t_recv.at[k], near[k]) for k in (1, 2)]
    t_relay = remote(t_part(1), t_part(1), s_sem.at[1], t_recv.at[0], to_y)
    t_swaps = [None] + [remote(t_part(k), t_part(k), s_sem.at[1], d_recv.at[k // 3], to_core) for k in (1, 2, 3)]

    @pl.when(c == 1)
    def _():
        for k in (1, 2):
            t_copies[k].start()

    mask_swap = remote(mask_any, other, s_sem.at[2], d_recv.at[2], to_core)
    mask_swap.start()

    drain(in_sem.at[2], row_blocks + row_blocks * col_blocks)
    for s in range(raw):
        raw_m[0][s] = x_v[lead * col_blocks + lead_columns[s]]
    raw_m[0][raw] = y_v[lead]

    spans = [(0, raw // 2), (raw // 2, raw + 1)]
    at = raw
    for size in [first // 2] * 2 + [late // 4] * 4:
        spans.append((at, at + size))
        at += size
    low, high = (0, 2, 4, 5), (1, 3, 6, 7)
    groups = [(0, 0), (1, 1), (2, 2), (3, 3), (4, 5), (6, 7)]
    paths = [None, (0, 1, 2, 3, 4, 5), (1, 0, 3, 2, 5, 4)]

    def chunk(raws, gathered, k, q, r):
        start, stop = spans[q][0], spans[r][1]
        return (raws if q < 2 else gathered)[k].at[pl.ds(start, stop - start)]

    stages = (0, 0, 1, 1, 2, 2)
    last_stages = (0, 0, 1, 1, 2, 3, 2, 3)
    sizes = [raw + 1, first, late, late // 2]

    def own_copy(k, g):
        q, r = groups[g]
        return remote(chunk(raw_m, mine, 0, q, r), chunk(raw_m, mine, k, q, r), s_sem.at[0], b_recv.at[k - 1, stages[g]], near[k])

    def relay_copy(k, q):
        return remote(chunk(raw_m, mine, k, q, q), chunk(raw_m, mine, 3, q, q), s_sem.at[0],
                      b_recv.at[2, last_stages[q]], near[3 - k])

    def swap(k, q, r):
        return remote(chunk(raw_m, mine, k, q, r), chunk(raw_t, theirs, k, q, r), s_sem.at[0],
                      d_recv.at[3 + k // 3] if q < 2 else d_recv.at[5 + k], to_core)

    own_swap = remote(mine[0].at[pl.ds(0, CAP)], theirs[0].at[pl.ds(0, CAP)], s_sem.at[0], d_recv.at[5], to_core)
    lam_swap = remote(lam.at[partner], lam_t, s_sem.at[0], d_recv.at[5], to_core)

    own_copy(1, 0).start()
    own_copy(2, 1).start()
    own_copy(1, 1).start()

    @pl.when(c == 0)
    def _():
        own_copy(2, 0).start()
        lam_swap.start()

    def dress(k):
        for i in range(cols):
            b = ids[k] * cols + i
            columns = t_v[b]
            for e in range(row_blocks):
                term = jnp.dot(y_v[e], columns, preferred_element_type=f32)
                dressed[e * col_blocks + b] = (x_v[e * col_blocks + b].astype(f32) - term).astype(bf16)

    slots = slots_of(mask, v, lead, raw, n - 1 - v, row_blocks, col_blocks, cols)
    order = []
    for s in range(raw, CAP):
        place = jnp.int32(0)
        for p, slot in enumerate(slots):
            place = jnp.where(slot == s, p, place)
        order.append(place)

    dress(0)
    @pl.when(c == 1)
    def _():
        t_copies[1].wait_recv()
        t_relay.start()
        own_copy(2, 0).start()
        t_swaps[1].start()
        t_copies[2].wait_recv()
        t_swaps[2].start()

    @pl.when(c == 0)
    def _():
        drain(d_recv.at[0], 2 * cols)

    dress(1)
    dress(2)

    def pack(q):
        for s in range(*spans[q]):
            mine[0][s] = dressed[order[s - raw]]

    pack(2)
    pack(3)
    for i in (2, 3):
        for k in (1, 2):
            own_copy(k, paths[k][i]).start()
    @pl.when(c == 1)
    def _():
        t_relay.wait_recv()
        t_swaps[3].start()
        lam_swap.start()

    @pl.when(c == 0)
    def _():
        t_swaps[3].wait_recv()

    dress(3)
    for i in (4, 5):
        for q in groups[i]:
            pack(q)
    for i in (4, 5):
        for k in (1, 2):
            own_copy(k, paths[k][i]).start()
    for s in range(raw):
        mine[0][s] = dressed[lead * col_blocks + lead_columns[s]]
    own_swap.start()
    mask_swap.wait_recv()

    def mend(k, raws, gathered, live_of):
        best = top_row(live_of, ids[k], row_blocks, col_blocks)
        places = raw_columns(live_of, ids[k], best, raw, col_blocks)
        rows = raws[k][raw]
        for s in range(raw):
            term = jnp.dot(rows, t_v[places[s]], preferred_element_type=f32)
            gathered[k][s] = (raws[k][s].astype(f32) - term).astype(bf16)

    def places(live_of, k):
        j = ids[k]
        best = top_row(live_of, j, row_blocks, col_blocks)
        return slots_of(live_of, j, best, raw, n - 1 - j, row_blocks, col_blocks, cols)

    def fill(dense, gathered, slots):
        for p, slot in enumerate(slots):
            e, b = p // col_blocks, p % col_blocks
            dense[e * TILE:(e + 1) * TILE, b * TILE:(b + 1) * TILE] = gathered[slot]

    def own_half(k, slots):
        fill(dense_m, mine[k], slots)
        acc[...] = jnp.dot(lam_m[ids[k]], dense_m[...], preferred_element_type=f32)

    def other_half(k, slots):
        if k:
            drain(d_recv.at[5 + k], CAP - raw)
        fill(dense_t, theirs[k], slots)
        if k < n - 1:
            stage[k] = (acc[...] + jnp.dot(
                lam_t[ids[k]], dense_t[...], preferred_element_type=f32)).astype(bf16)

    def both(k):
        own_half(k, places(mask, k))
        other_half(k, places(other, k))

    def arrive(k, level):
        drain(b_recv.at[k - 1, level], sizes[level])
        for q in (low if k == 1 else high):
            if min(last_stages[q], 2) == level:
                relay_copy(k, q).start()
        swap(k, *((0, 1), (2, 3), (4, 7))[level]).start()

    arrive(1, 0)
    arrive(2, 0)
    arrive(1, 1)
    arrive(2, 1)
    mend(1, raw_m, mine, mask)
    mend(2, raw_m, mine, mask)
    drain(d_recv.at[3], 2 * (raw + 1))
    mend(1, raw_t, theirs, other)
    mend(2, raw_t, theirs, other)
    lam_load.wait()
    drain(d_recv.at[5], CAP + lam_blocks)
    both(0)
    arrive(1, 2)
    arrive(2, 2)
    both(1)
    drain(b_recv.at[2, 0], raw + 1)
    swap(3, 0, 1).start()
    mend(3, raw_m, mine, mask)
    drain(d_recv.at[4], raw + 1)
    mend(3, raw_t, theirs, other)
    both(2)
    lam_last[...] = lam_t[ids[3]]
    here, there = places(mask, 3), places(other, 3)
    drain(b_recv.at[2, 1], first)
    swap(3, 2, 3).start()
    for level in (2, 3):
        drain(b_recv.at[2, level], late // 2)
        for q in (2 + level, 4 + level):
            swap(3, q, q).start()
    own_half(3, here)
    other_half(3, there)

    @pl.when(c == 1)
    def _():
        drain(s_sem.at[1], 6 * cols)

    mask_swap.wait_send()
    drain(s_sem.at[0], 3 * (CAP + 1) + CAP + 3 * (CAP + 1) + lam_blocks)


def last_kernel(done, dense_t, lam_last, acc, out, stage, sems):
    v = lax.axis_index("vir")
    row, col = v // 2, v % 2
    ids = [v, row * 2 + (1 - col), (1 - row) * 2 + col, 3 - v]
    count = done.shape[0]
    pieces, rows, width = stage.shape
    copies = [pltpu.make_async_copy(done.at[k], out.at[0, ids[k]], sems.at[pieces + k]) for k in range(count)]
    for copy in copies:
        copy.start()
    for i in range(pieces):
        columns = slice(i * width, (i + 1) * width)
        stage[i] = (acc[:, columns] + jnp.dot(
            lam_last[...], dense_t[:, columns], preferred_element_type=jnp.float32)).astype(jnp.bfloat16)
        copy = pltpu.make_async_copy(stage.at[i], out.at[0, ids[3], :, pl.ds(i * width, width)], sems.at[i])
        copy.start()
        copies.append(copy)
    for copy in copies:
        copy.wait()


def ring_kernel(n, lam, x, y, t, mask_any, out, lam_m, lam_t, x_v, y_v, t_v, dressed, dense_m, dense_t, acc, mask, other,
                in_sem, t_send, t_recv, b_send, b_recv, d_send, d_recv, l_send, l_recv, *bufs):
    mine, theirs = bufs[:n], bufs[n:]
    v, c = lax.axis_index("vir"), lax.axis_index("ka")
    dst, src = [(v + k) % n for k in range(n)], [(v + n - k) % n for k in range(n)]
    half, full = x_v.shape
    width = t_v.shape[2]
    row_blocks, col_blocks = half // TILE, full // TILE
    f32, bf16 = jnp.float32, jnp.bfloat16
    loads = [pltpu.make_async_copy(source, target, in_sem.at[i]) for i, (source, target) in enumerate(
        [(mask_any, mask), (t, t_v.at[v]), (y.at[0], y_v), (x.at[0], x_v), (lam.at[c], lam_m)])]
    for load in loads:
        load.start()
    to_core = {"ka": 1 - c}
    barrier = enter([{"vir": dst[k]} for k in range(1, n)] + [to_core])
    for load in loads:
        load.wait()
    pl.semaphore_wait(barrier, n)

    t_copies = [remote(t_v.at[v], t_v.at[v], t_send.at[k], t_recv.at[k], {"vir": dst[k]}) for k in range(1, n)]
    arrivals = [remote(t_v.at[v], t_v.at[src[k]], t_send.at[k], t_recv.at[k], {"vir": dst[k]}) for k in range(1, n)]
    for copy in t_copies:
        copy.start()
    mask_swap = remote(mask_any, other, l_send.at[0], l_recv.at[0], to_core)
    lam_swap = remote(lam.at[1 - c], lam_t, l_send.at[1], l_recv.at[1], to_core)
    mask_swap.start()
    lam_swap.start()

    zero = jnp.zeros((TILE, TILE), bf16)
    for k in range(n):
        mine[k][CAP] = zero
        theirs[k][CAP] = zero
    order = [jnp.int32(0)] * CAP
    count = jnp.int32(0)
    for p in range(row_blocks * col_blocks):
        live = mask[v, p // col_blocks, p % col_blocks]
        order = [jnp.where((live != 0) & (count == s), p, order[s]) for s in range(CAP)]
        count = count + live

    for copy in arrivals:
        copy.wait_recv()
    for b in range(col_blocks):
        if width >= TILE:
            owner, offset = b * TILE // width, b * TILE % width
            columns = t_v[owner][:, offset:offset + TILE]
        else:
            group = TILE // width
            columns = jnp.concatenate([t_v[b * group + i] for i in range(group)], axis=1)
        term = jnp.dot(y_v[...], columns, preferred_element_type=f32)
        value = (x_v[:, b * TILE:(b + 1) * TILE].astype(f32) - term).astype(bf16)
        for e in range(row_blocks):
            dressed[e * col_blocks + b] = value[e * TILE:(e + 1) * TILE]
    for s in range(CAP):
        mine[0][s] = dressed[order[s]]

    def live_part(ref):
        return ref.at[pl.ds(0, CAP)]

    copies = [None] + [
        remote(live_part(mine[0]), live_part(mine[k]), b_send.at[k], b_recv.at[k], {"vir": dst[k]}) for k in range(1, n)]
    swaps = [remote(live_part(mine[k]), live_part(theirs[k]), d_send.at[k], d_recv.at[k], to_core) for k in range(n)]
    for copy in copies[1:]:
        copy.start()

    def fill(dense, gathered, live_of, j):
        count = jnp.int32(0)
        for e in range(row_blocks):
            for b in range(col_blocks):
                live = live_of[j, e, b]
                dense[e * TILE:(e + 1) * TILE, b * TILE:(b + 1) * TILE] = gathered[jnp.where(live != 0, count, CAP)]
                count = count + live

    mask_swap.wait_recv()
    lam_swap.wait_recv()
    for k in range(n):
        if k:
            copies[k].wait_recv()
        swaps[k].start()
        fill(dense_m, mine[k], mask, src[k])
        acc[...] = jnp.dot(lam_m[src[k]], dense_m[...], preferred_element_type=f32)
        swaps[k].wait_recv()
        fill(dense_t, theirs[k], other, src[k])
        out[0, src[k]] = (acc[...] + jnp.dot(
            lam_t[src[k]], dense_t[...], preferred_element_type=f32)).astype(bf16)

    for copy in t_copies + copies[1:] + swaps + [mask_swap, lam_swap]:
        copy.wait_send()


def body(n, lambda_amps, screened_ints, half_ints, singles, block_mask):
    wide, pairs, rows, half = lambda_amps.shape
    full = screened_ints.shape[2]
    inner, width = singles.shape
    row_blocks, col_blocks = half // TILE, full // TILE
    blocks = row_blocks * col_blocks
    bf16, f32 = jnp.bfloat16, jnp.float32
    dma = pltpu.SemaphoreType.DMA
    tile = (TILE, TILE)
    anywhere, vmem = pl.BlockSpec(memory_space=pl.ANY), pl.BlockSpec(memory_space=pltpu.VMEM)
    lams = [pltpu.VMEM((pairs, rows, half), bf16)] * 2
    dense, total = pltpu.VMEM((half, full), bf16), pltpu.VMEM((rows, full), f32)
    masks = [pltpu.SMEM(block_mask.shape, jnp.int32)] * 2
    held = [pltpu.VMEM((CAP + 1,) + tile, bf16)] * (2 * n)
    args = (lambda_amps, screened_ints, half_ints, singles, block_mask)
    params = pltpu.CompilerParams(collective_id=0, has_side_effects=True, vmem_limit_bytes=56 * 1024 * 1024)
    if n != 4:
        return pl.pallas_call(
            functools.partial(ring_kernel, n),
            out_shape=pltpu.VMEM((1, pairs, rows, full), bf16),
            in_specs=[anywhere] * 5,
            out_specs=vmem,
            scratch_shapes=lams + [
                pltpu.VMEM((half, full), bf16), pltpu.VMEM((half, inner), bf16), pltpu.VMEM((n, inner, width), bf16),
                pltpu.VMEM((blocks,) + tile, bf16), dense, dense, total,
            ] + masks + [dma((5,)), dma((n,)), dma((n,)), dma((n,)), dma((n,)), dma((n,)), dma((n,)), dma((2,)), dma((2,))] + held,
            compiler_params=params,
        )(*args)
    raw = CAP // row_blocks
    held_over = (pltpu.VMEM((n - 1, rows, full), bf16), dense, pltpu.VMEM((rows, half), bf16), total)
    handed = pl.pallas_call(
        grid_kernel,
        out_shape=held_over,
        in_specs=[anywhere] * 5,
        out_specs=(vmem,) * 4,
        scratch_shapes=lams + [
            pltpu.VMEM((blocks,) + tile, bf16), pltpu.VMEM((row_blocks, TILE, inner), bf16),
            pltpu.VMEM((col_blocks, inner, TILE), bf16), pltpu.VMEM((blocks,) + tile, bf16), dense,
        ] + masks + [
            pltpu.VMEM((7 * (CAP + 1) + pairs * rows * half // (TILE * TILE),) + tile, bf16),
            dma((4,)), dma((3,)), dma((3,)), dma((3, 4)), dma((9,)),
        ] + held + [pltpu.VMEM((raw + 1,) + tile, bf16)] * (2 * n),
        compiler_params=params,
    )(*args)
    pieces = 2
    return pl.pallas_call(
        last_kernel,
        out_shape=jax.ShapeDtypeStruct((1, pairs, rows, full), bf16),
        in_specs=[vmem] * 4,
        out_specs=anywhere,
        scratch_shapes=[pltpu.VMEM((pieces, rows, full // pieces), bf16), dma((pieces + n - 1,))],
        compiler_params=pltpu.CompilerParams(vmem_limit_bytes=8 * 1024 * 1024),
    )(*handed)


def solution(mesh):
    return jax.shard_map(
        functools.partial(body, mesh.shape["vir"]),
        mesh=mesh,
        in_specs=(
            P(None, "occ", "vir", "ka"),
            P(("occ", "vir"), "ka", None),
            P(("occ", "vir"), "ka", None),
            P(None, "vir"),
            P("occ", "ka", None),
        ),
        out_specs=P("ka", "occ", "vir", None),
        check_vma=False,
    )
```

```python
import functools

import jax
import jax.numpy as jnp
from jax import lax
from jax.experimental import pallas as pl
from jax.experimental.pallas import tpu as pltpu
from jax.sharding import PartitionSpec as P

TILE = 128
CAP = 16
MESH = pl.DeviceIdType.MESH


def remote(source, target, send, recv, where):
    return pltpu.make_async_remote_copy(
        src_ref=source, dst_ref=target, send_sem=send, recv_sem=recv, device_id=where, device_id_type=MESH)


def enter(places):
    barrier = pltpu.get_barrier_semaphore()
    for place in places:
        pl.semaphore_signal(barrier, inc=1, device_id=place, device_id_type=MESH)
    return barrier


def top_row(live_of, j, row_blocks, col_blocks):
    best, most = jnp.int32(0), jnp.int32(-1)
    for e in range(row_blocks):
        total = live_of[j, e, 0]
        for b in range(1, col_blocks):
            total = total + live_of[j, e, b]
        best = jnp.where(total > most, e, best)
        most = jnp.maximum(total, most)
    return best


def raw_columns(live_of, j, row, raw, col_blocks):
    found = [jnp.int32(0)] * raw
    rank = jnp.int32(0)
    for b in range(col_blocks):
        live = live_of[j, row, b]
        found = [jnp.where((live != 0) & (rank == s), b, found[s]) for s in range(raw)]
        rank = rank + live
    return found


def slots_of(live_of, j, row, raw, late, row_blocks, col_blocks, cols):
    early_next, late_next = jnp.int32(raw), jnp.int32(CAP - 1)
    is_late = [late == g for g in range(col_blocks // cols)]
    slots = []
    for e in range(row_blocks):
        room = jnp.where(row == e, raw, 0)
        rank = jnp.int32(0)
        for b in range(col_blocks):
            live = live_of[j, e, b]
            is_raw = rank < room
            behind = is_late[b // cols]
            slot = jnp.where(is_raw, rank, jnp.where(behind, late_next, early_next))
            slots.append(jnp.where(live != 0, slot, CAP))
            step = jnp.where(is_raw, 0, live)
            late_next = late_next - jnp.where(behind, step, 0)
            early_next = early_next + jnp.where(behind, 0, step)
            rank = rank + live
    return slots


def grid_kernel(lam, x, y, t, mask_any, stage, dense_t, lam_last, acc, lam_m, lam_t, x_v, y_v, t_v, dressed, mask, other,
                tail, spare, in_sem, s_sem, t_recv, b_recv, d_recv, ready, *bufs):
    n = 4
    mine, theirs, raw_m, raw_t = bufs[:n], bufs[n:2 * n], bufs[2 * n:3 * n], bufs[3 * n:]
    v, c = lax.axis_index("vir"), lax.axis_index("ka")
    row, col = v // 2, v % 2
    ids = [v, row * 2 + (1 - col), (1 - row) * 2 + col, (1 - row) * 2 + (1 - col)]
    partner = 1 - c
    row_blocks, col_blocks = y_v.shape[0], t_v.shape[0]
    inner = t_v.shape[1]
    cols = col_blocks // n
    part = inner // 2
    raw = CAP // row_blocks
    late = row_blocks * cols
    first = CAP - raw - late
    lam_blocks = lam_m.shape[0] * lam_m.shape[1] * lam_m.shape[2] // (TILE * TILE)
    f32, bf16 = jnp.float32, jnp.bfloat16

    to_x, to_y, to_core = {"vir": ids[1]}, {"vir": ids[2]}, {"ka": partner}
    near = [None, to_x, to_y]
    last = [None, col == 1, row == 1]
    barrier = enter([to_core])
    for k in (1, 2):
        @pl.when(jnp.logical_not(last[k]))
        def _():
            pl.semaphore_signal(barrier, inc=1, device_id=near[k], device_id_type=MESH)

    def block(e, b):
        return x.at[0, pl.ds(e * TILE, TILE), pl.ds(b * TILE, TILE)]

    def drain(sem, count):
        pltpu.make_async_copy(spare.at[pl.ds(0, count)], spare.at[pl.ds(0, count)], sem).wait()

    mask_load = pltpu.make_async_copy(mask_any, mask, in_sem.at[0])
    t_loads = [pltpu.make_async_copy(
        t.at[:, pl.ds(i * TILE, TILE)], t_v.at[v * cols + i], in_sem.at[1]) for i in range(cols)]
    y_loads = [pltpu.make_async_copy(
        y.at[0, pl.ds(e * TILE, TILE)], y_v.at[e], in_sem.at[2]) for e in range(row_blocks)]
    x_loads = [pltpu.make_async_copy(
        block(p // col_blocks, p % col_blocks), x_v.at[p], in_sem.at[2]) for p in range(row_blocks * col_blocks)]
    lam_load = pltpu.make_async_copy(lam.at[c], lam_m, d_recv.at[5])
    mask_load.start()
    for load in t_loads + y_loads + x_loads:
        load.start()

    zero = jnp.zeros((TILE, TILE), bf16)
    for k in range(n):
        mine[k][CAP] = zero
        theirs[k][CAP] = zero
    tail[2] = zero

    pl.semaphore_wait(barrier, 1 + row + col)
    for k in (1, 2):
        @pl.when(last[k])
        def _():
            pl.semaphore_signal(ready.at[k - 1], inc=1, device_id=near[k], device_id_type=MESH)

    mask_load.wait()
    lead = top_row(mask, v, row_blocks, col_blocks)
    lead_columns = raw_columns(mask, v, lead, raw, col_blocks)
    drain(in_sem.at[1], cols)
    def t_part(k):
        return t_v.at[pl.ds(ids[k] * cols, cols)]

    t_copies = [None] + [remote(t_part(0), t_part(0), s_sem.at[1], t_recv.at[1], near[k]) for k in (1, 2)]
    t_relay = remote(t_part(1), t_part(1), s_sem.at[1], t_recv.at[0], to_y)
    t_swaps = [None] + [remote(t_part(k), t_part(k), s_sem.at[1], d_recv.at[k // 3], to_core) for k in (1, 2, 3)]

    for k in (1, 2):
        @pl.when((c == 1) & last[k])
        def _():
            t_copies[k].start()

    mask_swap = remote(mask_any, other, s_sem.at[2], d_recv.at[2], to_core)
    mask_swap.start()

    drain(in_sem.at[2], row_blocks + row_blocks * col_blocks)
    lam_load.start()
    for s in range(raw):
        raw_m[0][s] = x_v[lead * col_blocks + lead_columns[s]]
    raw_m[0][raw] = y_v[lead]

    spans = [(0, raw // 2), (raw // 2, raw + 1)]
    at = raw
    for size in [first // 2] * 2 + [late // 2 - 1, 1] * 2:
        spans.append((at, at + size))
        at += size
    low, high = (0, 2, 4, 5), (1, 3, 6, 7)
    groups = [(0, 0), (1, 1), (2, 2), (3, 3), (4, 5), (6, 7)]
    paths = [None, (0, 1, 2, 3, 4, 5), (1, 0, 3, 2, 5, 4)]

    def chunk(raws, gathered, k, q, r):
        start, stop = spans[q][0], spans[r][1]
        return (raws if q < 2 else gathered)[k].at[pl.ds(start, stop - start)]

    stages = (0, 0, 1, 1, 2, 2)
    last_stages = (0, 0, 1, 1, 2, 3, 2, 3)
    sizes = [raw + 1, first, late]

    def own_copy(k, g):
        q, r = groups[g]
        return remote(chunk(raw_m, mine, 0, q, r), chunk(raw_m, mine, k, q, r), s_sem.at[0], b_recv.at[stages[g]], near[k])

    def relay_copy(k, q):
        return remote(chunk(raw_m, mine, k, q, q), chunk(raw_m, mine, 3, q, q), s_sem.at[0],
                      b_recv.at[3 + last_stages[q]], near[3 - k])

    def swap(k, q, r):
        sem = 3 + k // 3 if q < 2 else 6 if k < 3 else 8 if q in (5, 7) else 7
        target = tail.at[pl.ds(q // 7, 1)] if k == 3 and q in (5, 7) else chunk(raw_t, theirs, k, q, r)
        return remote(chunk(raw_m, mine, k, q, r), target, s_sem.at[0], d_recv.at[sem], to_core)

    own_swap = remote(mine[0].at[pl.ds(0, CAP)], theirs[0].at[pl.ds(0, CAP)], s_sem.at[0], d_recv.at[5], to_core)
    lam_swap = remote(lam.at[partner], lam_t, s_sem.at[0], d_recv.at[5], to_core)

    def raw_start(k):
        own_copy(k, paths[k][0]).start()

        @pl.when((c == 0) | (k == 1))
        def _():
            own_copy(k, paths[k][1]).start()

    for k in (1, 2):
        @pl.when(last[k])
        def _():
            raw_start(k)

    for k in (1, 2):
        @pl.when(jnp.logical_not(last[k]))
        def _():
            pl.semaphore_wait(ready.at[k - 1], 1)

            @pl.when(c == 1)
            def _():
                t_copies[k].start()

            raw_start(k)

    @pl.when(c == 0)
    def _():
        lam_swap.start()

    def dress(k):
        for i in range(cols):
            b = ids[k] * cols + i
            columns = t_v[b]
            for e in range(row_blocks):
                term = jnp.dot(y_v[e], columns, preferred_element_type=f32)
                dressed[e * col_blocks + b] = (x_v[e * col_blocks + b].astype(f32) - term).astype(bf16)

    slots = slots_of(mask, v, lead, raw, n - 1 - v, row_blocks, col_blocks, cols)
    order = []
    for s in range(raw, CAP):
        place = jnp.int32(0)
        for p, slot in enumerate(slots):
            place = jnp.where(slot == s, p, place)
        order.append(place)

    dress(0)
    @pl.when(c == 1)
    def _():
        drain(t_recv.at[1], 2 * cols)
        t_relay.start()
        own_copy(2, 0).start()
        t_swaps[1].start()
        t_swaps[2].start()

    @pl.when(c == 0)
    def _():
        drain(d_recv.at[0], 2 * cols)

    dress(1)
    dress(2)

    def pack(q):
        for s in range(*spans[q]):
            mine[0][s] = dressed[order[s - raw]]

    pack(2)
    pack(3)
    for i in (2, 3):
        for k in (1, 2):
            own_copy(k, paths[k][i]).start()
    @pl.when(c == 1)
    def _():
        t_relay.wait_recv()
        t_swaps[3].start()
        lam_swap.start()

    @pl.when(c == 0)
    def _():
        t_swaps[3].wait_recv()

    dress(3)
    for i in (4, 5):
        for q in groups[i]:
            pack(q)
    for i in (4, 5):
        for k in (1, 2):
            own_copy(k, paths[k][i]).start()
    for s in range(raw):
        mine[0][s] = dressed[lead * col_blocks + lead_columns[s]]
    own_swap.start()
    mask_swap.wait_recv()

    def mend(k, raws, gathered, live_of):
        best = top_row(live_of, ids[k], row_blocks, col_blocks)
        places = raw_columns(live_of, ids[k], best, raw, col_blocks)
        rows = raws[k][raw]
        for s in range(raw):
            term = jnp.dot(rows, t_v[places[s]], preferred_element_type=f32)
            gathered[k][s] = (raws[k][s].astype(f32) - term).astype(bf16)

    def places(live_of, k):
        j = ids[k]
        best = top_row(live_of, j, row_blocks, col_blocks)
        return slots_of(live_of, j, best, raw, n - 1 - j, row_blocks, col_blocks, cols)

    def tile(gathered, slots, e, b):
        rows = [jnp.concatenate([gathered[slots[p * col_blocks + q]] for q in (b, b + 1)], axis=1) for p in (e, e + 1)]
        return jnp.concatenate(rows, axis=0)

    def product(pairs, b):
        return sum(
            jnp.dot(rows[:, e * TILE:(e + 2) * TILE], tile(gathered, slots, e, b), preferred_element_type=f32)
            for rows, gathered, slots in pairs for e in range(0, row_blocks, 2))

    def both(k):
        mine_k = (lam_m[ids[k]], mine[k], places(mask, k))
        theirs_k = (lam_t[ids[k]], theirs[k], places(other, k))
        for b in range(0, col_blocks, 2):
            stage[k, :, b * TILE:(b + 2) * TILE] = product([mine_k, theirs_k], b).astype(bf16)

    def arrive(level):
        drain(b_recv.at[level], 2 * sizes[level])
        for k in (1, 2):
            for q in (low if k == 1 else high):
                if min(last_stages[q], 2) == level:
                    relay_copy(k, q).start()
        for k in (1, 2):
            swap(k, *((0, 1), (2, 3), (4, 7))[level]).start()

    arrive(0)
    arrive(1)
    mend(1, raw_m, mine, mask)
    mend(2, raw_m, mine, mask)
    drain(d_recv.at[3], 2 * (raw + 1))
    mend(1, raw_t, theirs, other)
    mend(2, raw_t, theirs, other)
    drain(d_recv.at[5], CAP + 2 * lam_blocks)
    both(0)
    arrive(2)
    here, there = places(mask, 3), places(other, 3)
    ends = [spans[5][0], spans[7][0]]
    for end in ends:
        theirs[3][end] = zero
    seats = []
    for end in ends:
        seat = jnp.int32(-1)
        for p, slot in enumerate(there):
            seat = jnp.where(slot == end, p, seat)
        seats.append(seat)
    lam_rows = lam_t[ids[3]]
    for i, seat in enumerate(seats):
        rows = lam_rows[:, :TILE]
        for e in range(1, row_blocks):
            rows = jnp.where(seat >= e * col_blocks, lam_rows[:, e * TILE:(e + 1) * TILE], rows)
        lam_last[:, i * TILE:(i + 1) * TILE] = rows
    there = [jnp.where((slot == ends[0]) | (slot == ends[1]), CAP, slot) for slot in there]
    picks = []
    for i, seat in enumerate(seats):
        for b in range(col_blocks):
            hit = seat == b
            for e in range(1, row_blocks):
                hit = hit | (seat == e * col_blocks + b)
            picks.append(jnp.where(hit, i, 2))
    drain(b_recv.at[3], raw + 1)
    swap(3, 0, 1).start()
    drain(d_recv.at[6], 2 * (CAP - raw))
    both(1)
    drain(b_recv.at[4], first)
    swap(3, 2, 3).start()
    mend(3, raw_m, mine, mask)
    drain(d_recv.at[4], raw + 1)
    mend(3, raw_t, theirs, other)
    both(2)
    drain(b_recv.at[5], late - 2)
    for q in (4, 6):
        swap(3, q, q).start()
    drain(b_recv.at[6], 2)
    for q in (5, 7):
        swap(3, q, q).start()
    for b in range(0, col_blocks, 2):
        acc[:, b * TILE:(b + 2) * TILE] = product([(lam_m[ids[3]], mine[3], here)], b)
    drain(d_recv.at[7], CAP - raw - 2)
    for b in range(0, col_blocks, 2):
        acc[:, b * TILE:(b + 2) * TILE] += product([(lam_t[ids[3]], theirs[3], there)], b)
    drain(d_recv.at[8], 2)
    for i, pick in enumerate(picks):
        e, b = i // col_blocks, i % col_blocks
        dense_t[e * TILE:(e + 1) * TILE, b * TILE:(b + 1) * TILE] = tail[pick]

    @pl.when(c == 1)
    def _():
        drain(s_sem.at[1], 6 * cols)

    mask_swap.wait_send()
    drain(s_sem.at[0], 3 * (CAP + 1) + CAP + 3 * (CAP + 1) + lam_blocks)


def last_kernel(done, dense_t, lam_last, acc, out, stage, sems):
    v = lax.axis_index("vir")
    row, col = v // 2, v % 2
    ids = [v, row * 2 + (1 - col), (1 - row) * 2 + col, 3 - v]
    count = done.shape[0]
    pieces, rows, width = stage.shape
    copies = [pltpu.make_async_copy(done.at[k], out.at[0, ids[k]], sems.at[pieces + k]) for k in range(count)]
    for copy in copies:
        copy.start()
    for i in range(pieces):
        columns = slice(i * width, (i + 1) * width)
        stage[i] = (acc[:, columns] + jnp.dot(
            lam_last[...], dense_t[:, columns], preferred_element_type=jnp.float32)).astype(jnp.bfloat16)
        copy = pltpu.make_async_copy(stage.at[i], out.at[0, ids[3], :, pl.ds(i * width, width)], sems.at[i])
        copy.start()
        copies.append(copy)
    for copy in copies:
        copy.wait()


def ring_kernel(n, lam, x, y, t, mask_any, out, lam_m, lam_t, x_v, y_v, t_v, dressed, dense_m, dense_t, acc, mask, other,
                in_sem, t_send, t_recv, b_send, b_recv, d_send, d_recv, l_send, l_recv, *bufs):
    mine, theirs = bufs[:n], bufs[n:]
    v, c = lax.axis_index("vir"), lax.axis_index("ka")
    dst, src = [(v + k) % n for k in range(n)], [(v + n - k) % n for k in range(n)]
    half, full = x_v.shape
    width = t_v.shape[2]
    row_blocks, col_blocks = half // TILE, full // TILE
    f32, bf16 = jnp.float32, jnp.bfloat16
    loads = [pltpu.make_async_copy(source, target, in_sem.at[i]) for i, (source, target) in enumerate(
        [(mask_any, mask), (t, t_v.at[v]), (y.at[0], y_v), (x.at[0], x_v), (lam.at[c], lam_m)])]
    for load in loads:
        load.start()
    to_core = {"ka": 1 - c}
    barrier = enter([{"vir": dst[k]} for k in range(1, n)] + [to_core])
    for load in loads:
        load.wait()
    pl.semaphore_wait(barrier, n)

    t_copies = [remote(t_v.at[v], t_v.at[v], t_send.at[k], t_recv.at[k], {"vir": dst[k]}) for k in range(1, n)]
    arrivals = [remote(t_v.at[v], t_v.at[src[k]], t_send.at[k], t_recv.at[k], {"vir": dst[k]}) for k in range(1, n)]
    for copy in t_copies:
        copy.start()
    mask_swap = remote(mask_any, other, l_send.at[0], l_recv.at[0], to_core)
    lam_swap = remote(lam.at[1 - c], lam_t, l_send.at[1], l_recv.at[1], to_core)
    mask_swap.start()
    lam_swap.start()

    zero = jnp.zeros((TILE, TILE), bf16)
    for k in range(n):
        mine[k][CAP] = zero
        theirs[k][CAP] = zero
    order = [jnp.int32(0)] * CAP
    count = jnp.int32(0)
    for p in range(row_blocks * col_blocks):
        live = mask[v, p // col_blocks, p % col_blocks]
        order = [jnp.where((live != 0) & (count == s), p, order[s]) for s in range(CAP)]
        count = count + live

    for copy in arrivals:
        copy.wait_recv()
    for b in range(col_blocks):
        if width >= TILE:
            owner, offset = b * TILE // width, b * TILE % width
            columns = t_v[owner][:, offset:offset + TILE]
        else:
            group = TILE // width
            columns = jnp.concatenate([t_v[b * group + i] for i in range(group)], axis=1)
        term = jnp.dot(y_v[...], columns, preferred_element_type=f32)
        value = (x_v[:, b * TILE:(b + 1) * TILE].astype(f32) - term).astype(bf16)
        for e in range(row_blocks):
            dressed[e * col_blocks + b] = value[e * TILE:(e + 1) * TILE]
    for s in range(CAP):
        mine[0][s] = dressed[order[s]]

    def live_part(ref):
        return ref.at[pl.ds(0, CAP)]

    copies = [None] + [
        remote(live_part(mine[0]), live_part(mine[k]), b_send.at[k], b_recv.at[k], {"vir": dst[k]}) for k in range(1, n)]
    swaps = [remote(live_part(mine[k]), live_part(theirs[k]), d_send.at[k], d_recv.at[k], to_core) for k in range(n)]
    for copy in copies[1:]:
        copy.start()

    def fill(dense, gathered, live_of, j):
        count = jnp.int32(0)
        for e in range(row_blocks):
            for b in range(col_blocks):
                live = live_of[j, e, b]
                dense[e * TILE:(e + 1) * TILE, b * TILE:(b + 1) * TILE] = gathered[jnp.where(live != 0, count, CAP)]
                count = count + live

    mask_swap.wait_recv()
    lam_swap.wait_recv()
    for k in range(n):
        if k:
            copies[k].wait_recv()
        swaps[k].start()
        fill(dense_m, mine[k], mask, src[k])
        acc[...] = jnp.dot(lam_m[src[k]], dense_m[...], preferred_element_type=f32)
        swaps[k].wait_recv()
        fill(dense_t, theirs[k], other, src[k])
        out[0, src[k]] = (acc[...] + jnp.dot(
            lam_t[src[k]], dense_t[...], preferred_element_type=f32)).astype(bf16)

    for copy in t_copies + copies[1:] + swaps + [mask_swap, lam_swap]:
        copy.wait_send()


def body(n, lambda_amps, screened_ints, half_ints, singles, block_mask):
    wide, pairs, rows, half = lambda_amps.shape
    full = screened_ints.shape[2]
    inner, width = singles.shape
    row_blocks, col_blocks = half // TILE, full // TILE
    blocks = row_blocks * col_blocks
    bf16, f32 = jnp.bfloat16, jnp.float32
    dma = pltpu.SemaphoreType.DMA
    tile = (TILE, TILE)
    anywhere, vmem = pl.BlockSpec(memory_space=pl.ANY), pl.BlockSpec(memory_space=pltpu.VMEM)
    lams = [pltpu.VMEM((pairs, rows, half), bf16)] * 2
    dense, total = pltpu.VMEM((half, full), bf16), pltpu.VMEM((rows, full), f32)
    masks = [pltpu.SMEM(block_mask.shape, jnp.int32)] * 2
    held = [pltpu.VMEM((CAP + 1,) + tile, bf16)] * (2 * n)
    args = (lambda_amps, screened_ints, half_ints, singles, block_mask)
    params = pltpu.CompilerParams(collective_id=0, has_side_effects=True, vmem_limit_bytes=56 * 1024 * 1024)
    if n != 4:
        return pl.pallas_call(
            functools.partial(ring_kernel, n),
            out_shape=pltpu.VMEM((1, pairs, rows, full), bf16),
            in_specs=[anywhere] * 5,
            out_specs=vmem,
            scratch_shapes=lams + [
                pltpu.VMEM((half, full), bf16), pltpu.VMEM((half, inner), bf16), pltpu.VMEM((n, inner, width), bf16),
                pltpu.VMEM((blocks,) + tile, bf16), dense, dense, total,
            ] + masks + [dma((5,)), dma((n,)), dma((n,)), dma((n,)), dma((n,)), dma((n,)), dma((n,)), dma((2,)), dma((2,))] + held,
            compiler_params=params,
        )(*args)
    raw = CAP // row_blocks
    held_over = (pltpu.VMEM((n - 1, rows, full), bf16), pltpu.VMEM((2 * TILE, full), bf16), pltpu.VMEM((rows, 2 * TILE), bf16), total)
    handed = pl.pallas_call(
        grid_kernel,
        out_shape=held_over,
        in_specs=[anywhere] * 5,
        out_specs=(vmem,) * 4,
        scratch_shapes=lams + [
            pltpu.VMEM((blocks,) + tile, bf16), pltpu.VMEM((row_blocks, TILE, inner), bf16),
            pltpu.VMEM((col_blocks, inner, TILE), bf16), pltpu.VMEM((blocks,) + tile, bf16),
        ] + masks + [
            pltpu.VMEM((3,) + tile, bf16), pltpu.VMEM((7 * (CAP + 1) + pairs * rows * half // (TILE * TILE),) + tile, bf16),
            dma((3,)), dma((3,)), dma((2,)), dma((7,)), dma((9,)), pltpu.SemaphoreType.REGULAR((2,)),
        ] + held + [pltpu.VMEM((raw + 1,) + tile, bf16)] * (2 * n),
        compiler_params=params,
    )(*args)
    pieces = 2
    return pl.pallas_call(
        last_kernel,
        out_shape=jax.ShapeDtypeStruct((1, pairs, rows, full), bf16),
        in_specs=[vmem] * 4,
        out_specs=anywhere,
        scratch_shapes=[pltpu.VMEM((pieces, rows, full // pieces), bf16), dma((pieces + n - 1,))],
        compiler_params=pltpu.CompilerParams(vmem_limit_bytes=8 * 1024 * 1024),
    )(*handed)


def solution(mesh):
    return jax.shard_map(
        functools.partial(body, mesh.shape["vir"]),
        mesh=mesh,
        in_specs=(
            P(None, "occ", "vir", "ka"),
            P(("occ", "vir"), "ka", None),
            P(("occ", "vir"), "ka", None),
            P(None, "vir"),
            P("occ", "ka", None),
        ),
        out_specs=P("ka", "occ", "vir", None),
        check_vma=False,
    )
```

```python
import functools

import jax
import jax.numpy as jnp
from jax import lax
from jax.experimental import pallas as pl
from jax.experimental.pallas import tpu as pltpu
from jax.sharding import PartitionSpec as P

TILE = 128
CAP = 16
MESH = pl.DeviceIdType.MESH


def remote(source, target, send, recv, where):
    return pltpu.make_async_remote_copy(
        src_ref=source, dst_ref=target, send_sem=send, recv_sem=recv, device_id=where, device_id_type=MESH)


def enter(places):
    barrier = pltpu.get_barrier_semaphore()
    for place in places:
        pl.semaphore_signal(barrier, inc=1, device_id=place, device_id_type=MESH)
    return barrier


def top_row(live_of, j, row_blocks, col_blocks):
    best, most = jnp.int32(0), jnp.int32(-1)
    for e in range(row_blocks):
        total = live_of[j, e, 0]
        for b in range(1, col_blocks):
            total = total + live_of[j, e, b]
        best = jnp.where(total > most, e, best)
        most = jnp.maximum(total, most)
    return best


def raw_columns(live_of, j, row, raw, col_blocks):
    found = [jnp.int32(0)] * raw
    rank = jnp.int32(0)
    for b in range(col_blocks):
        live = live_of[j, row, b]
        found = [jnp.where((live != 0) & (rank == s), b, found[s]) for s in range(raw)]
        rank = rank + live
    return found


def slots_of(live_of, j, row, raw, late, row_blocks, col_blocks, cols):
    early_next, late_next = jnp.int32(raw), jnp.int32(CAP - 1)
    is_late = [late == g for g in range(col_blocks // cols)]
    slots = []
    for e in range(row_blocks):
        room = jnp.where(row == e, raw, 0)
        rank = jnp.int32(0)
        for b in range(col_blocks):
            live = live_of[j, e, b]
            is_raw = rank < room
            behind = is_late[b // cols]
            slot = jnp.where(is_raw, rank, jnp.where(behind, late_next, early_next))
            slots.append(jnp.where(live != 0, slot, CAP))
            step = jnp.where(is_raw, 0, live)
            late_next = late_next - jnp.where(behind, step, 0)
            early_next = early_next + jnp.where(behind, 0, step)
            rank = rank + live
    return slots


def grid_kernel(lam, x, y, t, mask_any, stage, dense_t, lam_last, acc, lam_m, lam_t, x_v, y_v, t_v, dressed, mask, other,
                tail, spare, in_sem, s_sem, t_recv, b_recv, d_recv, ready, *bufs):
    n = 4
    mine, theirs, raw_m, raw_t = bufs[:n], bufs[n:2 * n], bufs[2 * n:3 * n], bufs[3 * n:]
    v, c = lax.axis_index("vir"), lax.axis_index("ka")
    row, col = v // 2, v % 2
    ids = [v, row * 2 + (1 - col), (1 - row) * 2 + col, (1 - row) * 2 + (1 - col)]
    partner = 1 - c
    row_blocks, col_blocks = y_v.shape[0], t_v.shape[0]
    inner = t_v.shape[1]
    cols = col_blocks // n
    part = inner // 2
    raw = CAP // row_blocks
    late = row_blocks * cols
    first = CAP - raw - late
    lam_blocks = lam_m.shape[0] * lam_m.shape[1] * lam_m.shape[2] // (TILE * TILE)
    f32, bf16 = jnp.float32, jnp.bfloat16

    to_x, to_y, to_core = {"vir": ids[1]}, {"vir": ids[2]}, {"ka": partner}
    near = [None, to_x, to_y]
    last = [None, col == 1, row == 1]
    barrier = enter([to_core])
    for k in (1, 2):
        @pl.when(jnp.logical_not(last[k]))
        def _():
            pl.semaphore_signal(barrier, inc=1, device_id=near[k], device_id_type=MESH)

    def block(e, b):
        return x.at[0, pl.ds(e * TILE, TILE), pl.ds(b * TILE, TILE)]

    def drain(sem, count):
        pltpu.make_async_copy(spare.at[pl.ds(0, count)], spare.at[pl.ds(0, count)], sem).wait()

    mask_load = pltpu.make_async_copy(mask_any, mask, in_sem.at[0])
    t_loads = [pltpu.make_async_copy(
        t.at[:, pl.ds(i * TILE, TILE)], t_v.at[v * cols + i], in_sem.at[1]) for i in range(cols)]
    y_loads = [pltpu.make_async_copy(
        y.at[0, pl.ds(e * TILE, TILE)], y_v.at[e], in_sem.at[2]) for e in range(row_blocks)]
    x_loads = [pltpu.make_async_copy(
        block(p // col_blocks, p % col_blocks), x_v.at[p], in_sem.at[2]) for p in range(row_blocks * col_blocks)]
    lam_load = pltpu.make_async_copy(lam.at[c], lam_m, d_recv.at[5])
    mask_load.start()
    for load in t_loads + y_loads + x_loads:
        load.start()

    zero = jnp.zeros((TILE, TILE), bf16)
    for k in range(n):
        mine[k][CAP] = zero
        theirs[k][CAP] = zero
    tail[2] = zero

    pl.semaphore_wait(barrier, 1 + row + col)
    for k in (1, 2):
        @pl.when(last[k])
        def _():
            pl.semaphore_signal(ready.at[k - 1], inc=1, device_id=near[k], device_id_type=MESH)

    mask_load.wait()
    lead = top_row(mask, v, row_blocks, col_blocks)
    lead_columns = raw_columns(mask, v, lead, raw, col_blocks)
    drain(in_sem.at[1], cols)
    def t_part(k):
        return t_v.at[pl.ds(ids[k] * cols, cols)]

    t_copies = [None] + [remote(t_part(0), t_part(0), s_sem.at[1], t_recv.at[1], near[k]) for k in (1, 2)]
    t_relay = remote(t_part(1), t_part(1), s_sem.at[1], t_recv.at[0], to_y)
    t_swaps = [None] + [remote(t_part(k), t_part(k), s_sem.at[1], d_recv.at[k // 3], to_core) for k in (1, 2, 3)]

    for k in (1, 2):
        @pl.when((c == 1) & last[k])
        def _():
            t_copies[k].start()

    mask_swap = remote(mask_any, other, s_sem.at[2], d_recv.at[2], to_core)
    mask_swap.start()

    drain(in_sem.at[2], row_blocks + row_blocks * col_blocks)
    lam_load.start()
    for s in range(raw):
        raw_m[0][s] = x_v[lead * col_blocks + lead_columns[s]]
    raw_m[0][raw] = y_v[lead]

    spans = [(0, raw // 2), (raw // 2, raw + 1)]
    at = raw
    for size in [first // 2] * 2 + [late // 2 - 1, 1] * 2:
        spans.append((at, at + size))
        at += size
    low, high = (0, 2, 4, 5), (1, 3, 6, 7)
    groups = [(0, 0), (1, 1), (2, 2), (3, 3), (4, 5), (6, 7)]
    paths = [None, (0, 1, 2, 3, 4, 5), (1, 0, 3, 2, 5, 4)]

    def chunk(raws, gathered, k, q, r):
        start, stop = spans[q][0], spans[r][1]
        return (raws if q < 2 else gathered)[k].at[pl.ds(start, stop - start)]

    stages = [None, (0, 0, 1, 1, 2, 7), (0, 0, 1, 1, 7, 2)]
    last_stages = (0, 0, 1, 1, 2, 3, 2, 3)
    sizes = [raw + 1, first, late]

    def own_copy(k, g):
        q, r = groups[g]
        return remote(chunk(raw_m, mine, 0, q, r), chunk(raw_m, mine, k, q, r), s_sem.at[0], b_recv.at[stages[k][g]], near[k])

    def relay_copy(k, q):
        return remote(chunk(raw_m, mine, k, q, q), chunk(raw_m, mine, 3, q, q), s_sem.at[0],
                      b_recv.at[3 + last_stages[q]], near[3 - k])

    def swap(k, q, r):
        sem = 3 + k // 3 if q < 2 else 6 if k < 3 else 8 if q in (5, 7) else 7
        target = tail.at[pl.ds(q // 7, 1)] if k == 3 and q in (5, 7) else chunk(raw_t, theirs, k, q, r)
        return remote(chunk(raw_m, mine, k, q, r), target, s_sem.at[0], d_recv.at[sem], to_core)

    own_swap = remote(mine[0].at[pl.ds(0, CAP)], theirs[0].at[pl.ds(0, CAP)], s_sem.at[0], d_recv.at[5], to_core)
    lam_swap = remote(lam.at[partner], lam_t, s_sem.at[0], d_recv.at[5], to_core)

    def raw_start(k):
        own_copy(k, paths[k][0]).start()

        @pl.when((c == 0) | (k == 1))
        def _():
            own_copy(k, paths[k][1]).start()

    for k in (1, 2):
        @pl.when(last[k])
        def _():
            raw_start(k)

    for k in (1, 2):
        @pl.when(jnp.logical_not(last[k]))
        def _():
            pl.semaphore_wait(ready.at[k - 1], 1)

            @pl.when(c == 1)
            def _():
                t_copies[k].start()

            raw_start(k)

    @pl.when(c == 0)
    def _():
        lam_swap.start()

    def dress(k):
        for i in range(cols):
            b = ids[k] * cols + i
            columns = t_v[b]
            for e in range(row_blocks):
                term = jnp.dot(y_v[e], columns, preferred_element_type=f32)
                dressed[e * col_blocks + b] = (x_v[e * col_blocks + b].astype(f32) - term).astype(bf16)

    slots = slots_of(mask, v, lead, raw, n - 1 - v, row_blocks, col_blocks, cols)
    order = []
    for s in range(raw, CAP):
        place = jnp.int32(0)
        for p, slot in enumerate(slots):
            place = jnp.where(slot == s, p, place)
        order.append(place)

    dress(0)
    @pl.when(c == 1)
    def _():
        drain(t_recv.at[1], 2 * cols)
        t_relay.start()
        own_copy(2, 0).start()
        t_swaps[1].start()
        t_swaps[2].start()

    @pl.when(c == 0)
    def _():
        drain(d_recv.at[0], 2 * cols)

    dress(1)
    dress(2)

    def pack(q):
        for s in range(*spans[q]):
            mine[0][s] = dressed[order[s - raw]]

    pack(2)
    pack(3)
    for i in (2, 3):
        for k in (1, 2):
            own_copy(k, paths[k][i]).start()
    @pl.when(c == 1)
    def _():
        t_relay.wait_recv()
        t_swaps[3].start()
        lam_swap.start()

    @pl.when(c == 0)
    def _():
        t_swaps[3].wait_recv()

    dress(3)
    for i in (4, 5):
        for q in groups[i]:
            pack(q)
    for i in (4, 5):
        for k in (1, 2):
            own_copy(k, paths[k][i]).start()
    for s in range(raw):
        mine[0][s] = dressed[lead * col_blocks + lead_columns[s]]
    own_swap.start()
    mask_swap.wait_recv()

    def mend(k, raws, gathered, live_of):
        best = top_row(live_of, ids[k], row_blocks, col_blocks)
        places = raw_columns(live_of, ids[k], best, raw, col_blocks)
        rows = raws[k][raw]
        for s in range(raw):
            term = jnp.dot(rows, t_v[places[s]], preferred_element_type=f32)
            gathered[k][s] = (raws[k][s].astype(f32) - term).astype(bf16)

    def places(live_of, k):
        j = ids[k]
        best = top_row(live_of, j, row_blocks, col_blocks)
        return slots_of(live_of, j, best, raw, n - 1 - j, row_blocks, col_blocks, cols)

    def tile(gathered, slots, e, b):
        rows = [jnp.concatenate([gathered[slots[p * col_blocks + q]] for q in (b, b + 1)], axis=1) for p in (e, e + 1)]
        return jnp.concatenate(rows, axis=0)

    def product(pairs, b):
        return sum(
            jnp.dot(rows[:, e * TILE:(e + 2) * TILE], tile(gathered, slots, e, b), preferred_element_type=f32)
            for rows, gathered, slots in pairs for e in range(0, row_blocks, 2))

    def both(k):
        mine_k = (lam_m[ids[k]], mine[k], places(mask, k))
        theirs_k = (lam_t[ids[k]], theirs[k], places(other, k))
        for b in range(0, col_blocks, 2):
            stage[k, :, b * TILE:(b + 2) * TILE] = product([mine_k, theirs_k], b).astype(bf16)

    def relay(level):
        for q in (0, 1, 2, 3, 4, 6, 5, 7):
            if min(last_stages[q], 2) == level:
                relay_copy(1 if q in low else 2, q).start()

    def arrive(level):
        drain(b_recv.at[level], 2 * sizes[level])
        relay(level)
        for k in (1, 2):
            swap(k, *((0, 1), (2, 3))[level]).start()

    arrive(0)
    arrive(1)
    mend(1, raw_m, mine, mask)
    mend(2, raw_m, mine, mask)
    drain(d_recv.at[3], 2 * (raw + 1))
    mend(1, raw_t, theirs, other)
    mend(2, raw_t, theirs, other)
    drain(d_recv.at[5], CAP + 2 * lam_blocks)
    both(0)
    drain(b_recv.at[2], late)
    @pl.when(c == 0)
    def _():
        relay(2)

    swap(1, 4, 5).start()
    swap(2, 6, 7).start()
    drain(b_recv.at[7], late)
    swap(1, 6, 7).start()
    swap(2, 4, 5).start()
    here, there = places(mask, 3), places(other, 3)
    ends = [spans[5][0], spans[7][0]]
    for end in ends:
        theirs[3][end] = zero
    seats = []
    for end in ends:
        seat = jnp.int32(-1)
        for p, slot in enumerate(there):
            seat = jnp.where(slot == end, p, seat)
        seats.append(seat)
    lam_rows = lam_t[ids[3]]
    for i, seat in enumerate(seats):
        rows = lam_rows[:, :TILE]
        for e in range(1, row_blocks):
            rows = jnp.where(seat >= e * col_blocks, lam_rows[:, e * TILE:(e + 1) * TILE], rows)
        lam_last[:, i * TILE:(i + 1) * TILE] = rows
    there = [jnp.where((slot == ends[0]) | (slot == ends[1]), CAP, slot) for slot in there]
    picks = []
    for i, seat in enumerate(seats):
        for b in range(col_blocks):
            hit = seat == b
            for e in range(1, row_blocks):
                hit = hit | (seat == e * col_blocks + b)
            picks.append(jnp.where(hit, i, 2))
    drain(b_recv.at[3], raw + 1)
    swap(3, 0, 1).start()
    drain(d_recv.at[6], 2 * (CAP - raw))

    @pl.when(c == 1)
    def _():
        relay(2)

    both(1)
    drain(b_recv.at[4], first)
    swap(3, 2, 3).start()
    mend(3, raw_m, mine, mask)
    drain(d_recv.at[4], raw + 1)
    mend(3, raw_t, theirs, other)
    both(2)
    drain(b_recv.at[5], late - 2)
    for q in (4, 6):
        swap(3, q, q).start()
    drain(b_recv.at[6], 2)
    for q in (5, 7):
        swap(3, q, q).start()
    for b in range(0, col_blocks, 2):
        acc[:, b * TILE:(b + 2) * TILE] = product([(lam_m[ids[3]], mine[3], here)], b)
    drain(d_recv.at[7], CAP - raw - 2)
    for b in range(0, col_blocks, 2):
        acc[:, b * TILE:(b + 2) * TILE] += product([(lam_t[ids[3]], theirs[3], there)], b)
    drain(d_recv.at[8], 2)
    for i, pick in enumerate(picks):
        e, b = i // col_blocks, i % col_blocks
        dense_t[e * TILE:(e + 1) * TILE, b * TILE:(b + 1) * TILE] = tail[pick]

    @pl.when(c == 1)
    def _():
        drain(s_sem.at[1], 6 * cols)

    mask_swap.wait_send()
    drain(s_sem.at[0], 3 * (CAP + 1) + CAP + 3 * (CAP + 1) + lam_blocks)


def last_kernel(done, dense_t, lam_last, acc, out, stage, sems):
    v = lax.axis_index("vir")
    row, col = v // 2, v % 2
    ids = [v, row * 2 + (1 - col), (1 - row) * 2 + col, 3 - v]
    count = done.shape[0]
    pieces, rows, width = stage.shape
    copies = [pltpu.make_async_copy(done.at[k], out.at[0, ids[k]], sems.at[pieces + k]) for k in range(count)]
    for copy in copies:
        copy.start()
    for i in range(pieces):
        columns = slice(i * width, (i + 1) * width)
        stage[i] = (acc[:, columns] + jnp.dot(
            lam_last[...], dense_t[:, columns], preferred_element_type=jnp.float32)).astype(jnp.bfloat16)
        copy = pltpu.make_async_copy(stage.at[i], out.at[0, ids[3], :, pl.ds(i * width, width)], sems.at[i])
        copy.start()
        copies.append(copy)
    for copy in copies:
        copy.wait()


def ring_kernel(n, lam, x, y, t, mask_any, out, lam_m, lam_t, x_v, y_v, t_v, dressed, dense_m, dense_t, acc, mask, other,
                in_sem, t_send, t_recv, b_send, b_recv, d_send, d_recv, l_send, l_recv, *bufs):
    mine, theirs = bufs[:n], bufs[n:]
    v, c = lax.axis_index("vir"), lax.axis_index("ka")
    dst, src = [(v + k) % n for k in range(n)], [(v + n - k) % n for k in range(n)]
    half, full = x_v.shape
    width = t_v.shape[2]
    row_blocks, col_blocks = half // TILE, full // TILE
    f32, bf16 = jnp.float32, jnp.bfloat16
    loads = [pltpu.make_async_copy(source, target, in_sem.at[i]) for i, (source, target) in enumerate(
        [(mask_any, mask), (t, t_v.at[v]), (y.at[0], y_v), (x.at[0], x_v), (lam.at[c], lam_m)])]
    for load in loads:
        load.start()
    to_core = {"ka": 1 - c}
    barrier = enter([{"vir": dst[k]} for k in range(1, n)] + [to_core])
    for load in loads:
        load.wait()
    pl.semaphore_wait(barrier, n)

    t_copies = [remote(t_v.at[v], t_v.at[v], t_send.at[k], t_recv.at[k], {"vir": dst[k]}) for k in range(1, n)]
    arrivals = [remote(t_v.at[v], t_v.at[src[k]], t_send.at[k], t_recv.at[k], {"vir": dst[k]}) for k in range(1, n)]
    for copy in t_copies:
        copy.start()
    mask_swap = remote(mask_any, other, l_send.at[0], l_recv.at[0], to_core)
    lam_swap = remote(lam.at[1 - c], lam_t, l_send.at[1], l_recv.at[1], to_core)
    mask_swap.start()
    lam_swap.start()

    zero = jnp.zeros((TILE, TILE), bf16)
    for k in range(n):
        mine[k][CAP] = zero
        theirs[k][CAP] = zero
    order = [jnp.int32(0)] * CAP
    count = jnp.int32(0)
    for p in range(row_blocks * col_blocks):
        live = mask[v, p // col_blocks, p % col_blocks]
        order = [jnp.where((live != 0) & (count == s), p, order[s]) for s in range(CAP)]
        count = count + live

    for copy in arrivals:
        copy.wait_recv()
    for b in range(col_blocks):
        if width >= TILE:
            owner, offset = b * TILE // width, b * TILE % width
            columns = t_v[owner][:, offset:offset + TILE]
        else:
            group = TILE // width
            columns = jnp.concatenate([t_v[b * group + i] for i in range(group)], axis=1)
        term = jnp.dot(y_v[...], columns, preferred_element_type=f32)
        value = (x_v[:, b * TILE:(b + 1) * TILE].astype(f32) - term).astype(bf16)
        for e in range(row_blocks):
            dressed[e * col_blocks + b] = value[e * TILE:(e + 1) * TILE]
    for s in range(CAP):
        mine[0][s] = dressed[order[s]]

    def live_part(ref):
        return ref.at[pl.ds(0, CAP)]

    copies = [None] + [
        remote(live_part(mine[0]), live_part(mine[k]), b_send.at[k], b_recv.at[k], {"vir": dst[k]}) for k in range(1, n)]
    swaps = [remote(live_part(mine[k]), live_part(theirs[k]), d_send.at[k], d_recv.at[k], to_core) for k in range(n)]
    for copy in copies[1:]:
        copy.start()

    def fill(dense, gathered, live_of, j):
        count = jnp.int32(0)
        for e in range(row_blocks):
            for b in range(col_blocks):
                live = live_of[j, e, b]
                dense[e * TILE:(e + 1) * TILE, b * TILE:(b + 1) * TILE] = gathered[jnp.where(live != 0, count, CAP)]
                count = count + live

    mask_swap.wait_recv()
    lam_swap.wait_recv()
    for k in range(n):
        if k:
            copies[k].wait_recv()
        swaps[k].start()
        fill(dense_m, mine[k], mask, src[k])
        acc[...] = jnp.dot(lam_m[src[k]], dense_m[...], preferred_element_type=f32)
        swaps[k].wait_recv()
        fill(dense_t, theirs[k], other, src[k])
        out[0, src[k]] = (acc[...] + jnp.dot(
            lam_t[src[k]], dense_t[...], preferred_element_type=f32)).astype(bf16)

    for copy in t_copies + copies[1:] + swaps + [mask_swap, lam_swap]:
        copy.wait_send()


def body(n, lambda_amps, screened_ints, half_ints, singles, block_mask):
    wide, pairs, rows, half = lambda_amps.shape
    full = screened_ints.shape[2]
    inner, width = singles.shape
    row_blocks, col_blocks = half // TILE, full // TILE
    blocks = row_blocks * col_blocks
    bf16, f32 = jnp.bfloat16, jnp.float32
    dma = pltpu.SemaphoreType.DMA
    tile = (TILE, TILE)
    anywhere, vmem = pl.BlockSpec(memory_space=pl.ANY), pl.BlockSpec(memory_space=pltpu.VMEM)
    lams = [pltpu.VMEM((pairs, rows, half), bf16)] * 2
    dense, total = pltpu.VMEM((half, full), bf16), pltpu.VMEM((rows, full), f32)
    masks = [pltpu.SMEM(block_mask.shape, jnp.int32)] * 2
    held = [pltpu.VMEM((CAP + 1,) + tile, bf16)] * (2 * n)
    args = (lambda_amps, screened_ints, half_ints, singles, block_mask)
    params = pltpu.CompilerParams(collective_id=0, has_side_effects=True, vmem_limit_bytes=56 * 1024 * 1024)
    if n != 4:
        return pl.pallas_call(
            functools.partial(ring_kernel, n),
            out_shape=pltpu.VMEM((1, pairs, rows, full), bf16),
            in_specs=[anywhere] * 5,
            out_specs=vmem,
            scratch_shapes=lams + [
                pltpu.VMEM((half, full), bf16), pltpu.VMEM((half, inner), bf16), pltpu.VMEM((n, inner, width), bf16),
                pltpu.VMEM((blocks,) + tile, bf16), dense, dense, total,
            ] + masks + [dma((5,)), dma((n,)), dma((n,)), dma((n,)), dma((n,)), dma((n,)), dma((n,)), dma((2,)), dma((2,))] + held,
            compiler_params=params,
        )(*args)
    raw = CAP // row_blocks
    held_over = (pltpu.VMEM((n - 1, rows, full), bf16), pltpu.VMEM((2 * TILE, full), bf16), pltpu.VMEM((rows, 2 * TILE), bf16), total)
    handed = pl.pallas_call(
        grid_kernel,
        out_shape=held_over,
        in_specs=[anywhere] * 5,
        out_specs=(vmem,) * 4,
        scratch_shapes=lams + [
            pltpu.VMEM((blocks,) + tile, bf16), pltpu.VMEM((row_blocks, TILE, inner), bf16),
            pltpu.VMEM((col_blocks, inner, TILE), bf16), pltpu.VMEM((blocks,) + tile, bf16),
        ] + masks + [
            pltpu.VMEM((3,) + tile, bf16), pltpu.VMEM((7 * (CAP + 1) + pairs * rows * half // (TILE * TILE),) + tile, bf16),
            dma((3,)), dma((3,)), dma((2,)), dma((8,)), dma((9,)), pltpu.SemaphoreType.REGULAR((2,)),
        ] + held + [pltpu.VMEM((raw + 1,) + tile, bf16)] * (2 * n),
        compiler_params=params,
    )(*args)
    pieces = 2
    return pl.pallas_call(
        last_kernel,
        out_shape=jax.ShapeDtypeStruct((1, pairs, rows, full), bf16),
        in_specs=[vmem] * 4,
        out_specs=anywhere,
        scratch_shapes=[pltpu.VMEM((pieces, rows, full // pieces), bf16), dma((pieces + n - 1,))],
        compiler_params=pltpu.CompilerParams(vmem_limit_bytes=8 * 1024 * 1024),
    )(*handed)


def solution(mesh):
    return jax.shard_map(
        functools.partial(body, mesh.shape["vir"]),
        mesh=mesh,
        in_specs=(
            P(None, "occ", "vir", "ka"),
            P(("occ", "vir"), "ka", None),
            P(("occ", "vir"), "ka", None),
            P(None, "vir"),
            P("occ", "ka", None),
        ),
        out_specs=P("ka", "occ", "vir", None),
        check_vma=False,
    )
```

```python
import functools

import jax
import jax.numpy as jnp
from jax import lax
from jax.experimental import pallas as pl
from jax.experimental.pallas import tpu as pltpu
from jax.sharding import PartitionSpec as P

TILE = 128
CAP = 16
MESH = pl.DeviceIdType.MESH


def remote(source, target, send, recv, where):
    return pltpu.make_async_remote_copy(
        src_ref=source, dst_ref=target, send_sem=send, recv_sem=recv, device_id=where, device_id_type=MESH)


def enter(places):
    barrier = pltpu.get_barrier_semaphore()
    for place in places:
        pl.semaphore_signal(barrier, inc=1, device_id=place, device_id_type=MESH)
    return barrier


def top_row(live_of, j, row_blocks, col_blocks):
    best, most = jnp.int32(0), jnp.int32(-1)
    for e in range(row_blocks):
        total = live_of[j, e, 0]
        for b in range(1, col_blocks):
            total = total + live_of[j, e, b]
        best = jnp.where(total > most, e, best)
        most = jnp.maximum(total, most)
    return best


def raw_columns(live_of, j, row, raw, col_blocks):
    found = [jnp.int32(0)] * raw
    rank = jnp.int32(0)
    for b in range(col_blocks):
        live = live_of[j, row, b]
        found = [jnp.where((live != 0) & (rank == s), b, found[s]) for s in range(raw)]
        rank = rank + live
    return found


def slots_of(live_of, j, row, raw, late, row_blocks, col_blocks, cols):
    early_next, late_next = jnp.int32(raw), jnp.int32(CAP - 1)
    is_late = [late == g for g in range(col_blocks // cols)]
    slots = []
    for e in range(row_blocks):
        room = jnp.where(row == e, raw, 0)
        rank = jnp.int32(0)
        for b in range(col_blocks):
            live = live_of[j, e, b]
            is_raw = rank < room
            behind = is_late[b // cols]
            slot = jnp.where(is_raw, rank, jnp.where(behind, late_next, early_next))
            slots.append(jnp.where(live != 0, slot, CAP))
            step = jnp.where(is_raw, 0, live)
            late_next = late_next - jnp.where(behind, step, 0)
            early_next = early_next + jnp.where(behind, 0, step)
            rank = rank + live
    return slots


def grid_kernel(lam, x, y, t, mask_any, stage, dense_t, lam_last, acc, lam_m, lam_t, x_v, y_v, t_v, dressed, mask, other,
                spare, in_sem, s_sem, t_recv, b_recv, d_recv, ready, *bufs):
    n = 4
    mine, theirs, raw_m, raw_t = bufs[:n], bufs[n:2 * n], bufs[2 * n:3 * n], bufs[3 * n:]
    v, c = lax.axis_index("vir"), lax.axis_index("ka")
    row, col = v // 2, v % 2
    ids = [v, row * 2 + (1 - col), (1 - row) * 2 + col, (1 - row) * 2 + (1 - col)]
    partner = 1 - c
    row_blocks, col_blocks = y_v.shape[0], t_v.shape[0]
    inner = t_v.shape[1]
    cols = col_blocks // n
    part = inner // 2
    raw = CAP // row_blocks
    late = row_blocks * cols
    first = CAP - raw - late
    lam_blocks = lam_m.shape[0] * lam_m.shape[1] * lam_m.shape[2] // (TILE * TILE)
    f32, bf16 = jnp.float32, jnp.bfloat16

    to_x, to_y, to_core = {"vir": ids[1]}, {"vir": ids[2]}, {"ka": partner}
    near = [None, to_x, to_y]
    last = [None, col == 1, row == 1]
    barrier = enter([to_core])
    for k in (1, 2):
        @pl.when(jnp.logical_not(last[k]))
        def _():
            pl.semaphore_signal(barrier, inc=1, device_id=near[k], device_id_type=MESH)

    def block(e, b):
        return x.at[0, pl.ds(e * TILE, TILE), pl.ds(b * TILE, TILE)]

    def drain(sem, count):
        pltpu.make_async_copy(spare.at[pl.ds(0, count)], spare.at[pl.ds(0, count)], sem).wait()

    mask_load = pltpu.make_async_copy(mask_any, mask, in_sem.at[0])
    t_loads = [pltpu.make_async_copy(
        t.at[:, pl.ds(i * TILE, TILE)], t_v.at[v * cols + i], in_sem.at[1]) for i in range(cols)]
    y_loads = [pltpu.make_async_copy(
        y.at[0, pl.ds(e * TILE, TILE)], y_v.at[e], in_sem.at[2]) for e in range(row_blocks)]
    x_loads = [pltpu.make_async_copy(
        block(p // col_blocks, p % col_blocks), x_v.at[p], in_sem.at[2]) for p in range(row_blocks * col_blocks)]
    lam_load = pltpu.make_async_copy(lam.at[c], lam_m, d_recv.at[5])
    mask_load.start()
    for load in t_loads + y_loads + x_loads:
        load.start()

    zero = jnp.zeros((TILE, TILE), bf16)
    for k in range(n):
        mine[k][CAP] = zero
        theirs[k][CAP] = zero

    pl.semaphore_wait(barrier, 1 + row + col)
    for k in (1, 2):
        @pl.when(last[k])
        def _():
            pl.semaphore_signal(ready.at[k - 1], inc=1, device_id=near[k], device_id_type=MESH)

    mask_load.wait()
    lead = top_row(mask, v, row_blocks, col_blocks)
    lead_columns = raw_columns(mask, v, lead, raw, col_blocks)
    drain(in_sem.at[1], cols)
    def t_part(k):
        return t_v.at[pl.ds(ids[k] * cols, cols)]

    t_copies = [None] + [remote(t_part(0), t_part(0), s_sem.at[1], t_recv.at[1], near[k]) for k in (1, 2)]
    t_relay = remote(t_part(1), t_part(1), s_sem.at[1], t_recv.at[0], to_y)
    t_swaps = [None] + [remote(t_part(k), t_part(k), s_sem.at[1], d_recv.at[k // 3], to_core) for k in (1, 2, 3)]

    for k in (1, 2):
        @pl.when((c == 1) & last[k])
        def _():
            t_copies[k].start()

    mask_swap = remote(mask_any, other, s_sem.at[2], d_recv.at[2], to_core)
    mask_swap.start()

    drain(in_sem.at[2], row_blocks + row_blocks * col_blocks)
    lam_load.start()
    for s in range(raw):
        raw_m[0][s] = x_v[lead * col_blocks + lead_columns[s]]
    raw_m[0][raw] = y_v[lead]

    spans = [(0, raw // 2), (raw // 2, raw + 1)]
    at = raw
    for size in [first // 2] * 2 + [late // 2 - 1, 1] * 2:
        spans.append((at, at + size))
        at += size
    low, high = (0, 2, 4, 5), (1, 3, 6, 7)
    groups = [(0, 0), (1, 1), (2, 2), (3, 3), (4, 5), (6, 7)]
    paths = [None, (0, 1, 2, 3, 4, 5), (1, 0, 3, 2, 5, 4)]

    def chunk(raws, gathered, k, q, r):
        start, stop = spans[q][0], spans[r][1]
        return (raws if q < 2 else gathered)[k].at[pl.ds(start, stop - start)]

    stages = [None, (0, 0, 1, 1, 2, 7), (0, 0, 1, 1, 7, 2)]
    last_stages = (0, 0, 1, 1, 2, 3, 2, 3)
    sizes = [raw + 1, first, late]

    def own_copy(k, g):
        q, r = groups[g]
        return remote(chunk(raw_m, mine, 0, q, r), chunk(raw_m, mine, k, q, r), s_sem.at[0], b_recv.at[stages[k][g]], near[k])

    def relay_copy(k, q):
        return remote(chunk(raw_m, mine, k, q, q), chunk(raw_m, mine, 3, q, q), s_sem.at[0],
                      b_recv.at[3 + last_stages[q]], near[3 - k])

    def swap(k, q, r):
        sem = 3 + k // 3 if q < 2 else 6 + k // 3
        return remote(chunk(raw_m, mine, k, q, r), chunk(raw_t, theirs, k, q, r), s_sem.at[0], d_recv.at[sem], to_core)

    own_swap = remote(mine[0].at[pl.ds(0, CAP)], theirs[0].at[pl.ds(0, CAP)], s_sem.at[0], d_recv.at[5], to_core)
    lam_swap = remote(lam.at[partner], lam_t, s_sem.at[0], d_recv.at[5], to_core)

    def raw_start(k):
        own_copy(k, paths[k][0]).start()

        @pl.when((c == 0) | (k == 1))
        def _():
            own_copy(k, paths[k][1]).start()

    for k in (1, 2):
        @pl.when(last[k])
        def _():
            raw_start(k)

    for k in (1, 2):
        @pl.when(jnp.logical_not(last[k]))
        def _():
            pl.semaphore_wait(ready.at[k - 1], 1)

            @pl.when(c == 1)
            def _():
                t_copies[k].start()

            raw_start(k)

    @pl.when(c == 0)
    def _():
        lam_swap.start()

    def dress(k):
        for i in range(cols):
            b = ids[k] * cols + i
            columns = t_v[b]
            for e in range(row_blocks):
                term = jnp.dot(y_v[e], columns, preferred_element_type=f32)
                dressed[e * col_blocks + b] = (x_v[e * col_blocks + b].astype(f32) - term).astype(bf16)

    slots = slots_of(mask, v, lead, raw, n - 1 - v, row_blocks, col_blocks, cols)
    order = []
    for s in range(raw, CAP):
        place = jnp.int32(0)
        for p, slot in enumerate(slots):
            place = jnp.where(slot == s, p, place)
        order.append(place)

    dress(0)
    @pl.when(c == 1)
    def _():
        drain(t_recv.at[1], 2 * cols)
        t_relay.start()
        own_copy(2, 0).start()
        t_swaps[1].start()
        t_swaps[2].start()

    @pl.when(c == 0)
    def _():
        drain(d_recv.at[0], 2 * cols)

    dress(1)
    dress(2)

    def pack(q):
        for s in range(*spans[q]):
            mine[0][s] = dressed[order[s - raw]]

    pack(2)
    pack(3)
    for i in (2, 3):
        for k in (1, 2):
            own_copy(k, paths[k][i]).start()
    @pl.when(c == 1)
    def _():
        t_relay.wait_recv()
        t_swaps[3].start()
        lam_swap.start()

    @pl.when(c == 0)
    def _():
        t_swaps[3].wait_recv()

    dress(3)
    for i in (4, 5):
        for q in groups[i]:
            pack(q)
    for i in (4, 5):
        for k in (1, 2):
            own_copy(k, paths[k][i]).start()
    for s in range(raw):
        mine[0][s] = dressed[lead * col_blocks + lead_columns[s]]
    own_swap.start()
    mask_swap.wait_recv()

    def mend(k, raws, gathered, live_of):
        best = top_row(live_of, ids[k], row_blocks, col_blocks)
        places = raw_columns(live_of, ids[k], best, raw, col_blocks)
        rows = raws[k][raw]
        for s in range(raw):
            term = jnp.dot(rows, t_v[places[s]], preferred_element_type=f32)
            gathered[k][s] = (raws[k][s].astype(f32) - term).astype(bf16)

    def places(live_of, k):
        j = ids[k]
        best = top_row(live_of, j, row_blocks, col_blocks)
        return slots_of(live_of, j, best, raw, n - 1 - j, row_blocks, col_blocks, cols)

    def tile(gathered, slots, e, b):
        rows = [jnp.concatenate([gathered[slots[p * col_blocks + q]] for q in (b, b + 1)], axis=1) for p in (e, e + 1)]
        return jnp.concatenate(rows, axis=0)

    def product(pairs, b):
        return sum(
            jnp.dot(rows[:, e * TILE:(e + 2) * TILE], tile(gathered, slots, e, b), preferred_element_type=f32)
            for rows, gathered, slots in pairs for e in range(0, row_blocks, 2))

    def both(k):
        mine_k = (lam_m[ids[k]], mine[k], places(mask, k))
        theirs_k = (lam_t[ids[k]], theirs[k], places(other, k))
        for b in range(0, col_blocks, 2):
            stage[k, :, b * TILE:(b + 2) * TILE] = product([mine_k, theirs_k], b).astype(bf16)

    def relay(level):
        for q in (0, 1, 2, 3, 4, 6, 5, 7):
            if min(last_stages[q], 2) == level:
                relay_copy(1 if q in low else 2, q).start()

    def arrive(level):
        drain(b_recv.at[level], 2 * sizes[level])
        relay(level)
        for k in (1, 2):
            swap(k, *((0, 1), (2, 3))[level]).start()

    arrive(0)
    arrive(1)
    mend(1, raw_m, mine, mask)
    mend(2, raw_m, mine, mask)
    drain(d_recv.at[3], 2 * (raw + 1))
    mend(1, raw_t, theirs, other)
    mend(2, raw_t, theirs, other)
    drain(d_recv.at[5], CAP + 2 * lam_blocks)
    both(0)
    drain(b_recv.at[2], late)
    @pl.when(c == 0)
    def _():
        relay(2)

    swap(1, 4, 5).start()
    swap(2, 6, 7).start()
    drain(b_recv.at[7], late)
    swap(1, 6, 7).start()
    swap(2, 4, 5).start()
    here, there = places(mask, 3), places(other, 3)
    lam_last[...] = lam_t[ids[3]]
    drain(b_recv.at[3], raw + 1)
    swap(3, 0, 1).start()
    drain(d_recv.at[6], 2 * (CAP - raw))

    @pl.when(c == 1)
    def _():
        relay(2)

    both(1)
    drain(b_recv.at[4], first)
    swap(3, 2, 3).start()
    mend(3, raw_m, mine, mask)
    drain(d_recv.at[4], raw + 1)
    mend(3, raw_t, theirs, other)
    both(2)
    drain(b_recv.at[5], late - 2)
    for q in (4, 6):
        swap(3, q, q).start()
    drain(b_recv.at[6], 2)
    for q in (5, 7):
        swap(3, q, q).start()
    for b in range(0, col_blocks, 2):
        acc[:, b * TILE:(b + 2) * TILE] = product([(lam_m[ids[3]], mine[3], here)], b)
    drain(d_recv.at[7], CAP - raw)
    for p, slot in enumerate(there):
        e, b = p // col_blocks, p % col_blocks
        dense_t[e * TILE:(e + 1) * TILE, b * TILE:(b + 1) * TILE] = theirs[3][slot]

    @pl.when(c == 1)
    def _():
        drain(s_sem.at[1], 6 * cols)

    mask_swap.wait_send()
    drain(s_sem.at[0], 3 * (CAP + 1) + CAP + 3 * (CAP + 1) + lam_blocks)


def last_kernel(done, dense_t, lam_last, acc, out, stage, sem):
    v = lax.axis_index("vir")
    row, col = v // 2, v % 2
    ids = [v, row * 2 + (1 - col), (1 - row) * 2 + col, 3 - v]
    pieces, rows, width = stage.shape
    for k in range(done.shape[0]):
        pltpu.make_async_copy(done.at[k], out.at[0, ids[k]], sem.at[0]).start()
    for i in range(pieces):
        columns = slice(i * width, (i + 1) * width)
        stage[i] = (acc[:, columns] + jnp.dot(
            lam_last[...], dense_t[:, columns], preferred_element_type=jnp.float32)).astype(jnp.bfloat16)
        pltpu.make_async_copy(stage.at[i], out.at[0, ids[3], :, pl.ds(i * width, width)], sem.at[0]).start()
    pltpu.make_async_copy(out, out, sem.at[0]).wait()


def ring_kernel(n, lam, x, y, t, mask_any, out, lam_m, lam_t, x_v, y_v, t_v, dressed, dense_m, dense_t, acc, mask, other,
                in_sem, t_send, t_recv, b_send, b_recv, d_send, d_recv, l_send, l_recv, *bufs):
    mine, theirs = bufs[:n], bufs[n:]
    v, c = lax.axis_index("vir"), lax.axis_index("ka")
    dst, src = [(v + k) % n for k in range(n)], [(v + n - k) % n for k in range(n)]
    half, full = x_v.shape
    width = t_v.shape[2]
    row_blocks, col_blocks = half // TILE, full // TILE
    f32, bf16 = jnp.float32, jnp.bfloat16
    loads = [pltpu.make_async_copy(source, target, in_sem.at[i]) for i, (source, target) in enumerate(
        [(mask_any, mask), (t, t_v.at[v]), (y.at[0], y_v), (x.at[0], x_v), (lam.at[c], lam_m)])]
    for load in loads:
        load.start()
    to_core = {"ka": 1 - c}
    barrier = enter([{"vir": dst[k]} for k in range(1, n)] + [to_core])
    for load in loads:
        load.wait()
    pl.semaphore_wait(barrier, n)

    t_copies = [remote(t_v.at[v], t_v.at[v], t_send.at[k], t_recv.at[k], {"vir": dst[k]}) for k in range(1, n)]
    arrivals = [remote(t_v.at[v], t_v.at[src[k]], t_send.at[k], t_recv.at[k], {"vir": dst[k]}) for k in range(1, n)]
    for copy in t_copies:
        copy.start()
    mask_swap = remote(mask_any, other, l_send.at[0], l_recv.at[0], to_core)
    lam_swap = remote(lam.at[1 - c], lam_t, l_send.at[1], l_recv.at[1], to_core)
    mask_swap.start()
    lam_swap.start()

    zero = jnp.zeros((TILE, TILE), bf16)
    for k in range(n):
        mine[k][CAP] = zero
        theirs[k][CAP] = zero
    order = [jnp.int32(0)] * CAP
    count = jnp.int32(0)
    for p in range(row_blocks * col_blocks):
        live = mask[v, p // col_blocks, p % col_blocks]
        order = [jnp.where((live != 0) & (count == s), p, order[s]) for s in range(CAP)]
        count = count + live

    for copy in arrivals:
        copy.wait_recv()
    for b in range(col_blocks):
        if width >= TILE:
            owner, offset = b * TILE // width, b * TILE % width
            columns = t_v[owner][:, offset:offset + TILE]
        else:
            group = TILE // width
            columns = jnp.concatenate([t_v[b * group + i] for i in range(group)], axis=1)
        term = jnp.dot(y_v[...], columns, preferred_element_type=f32)
        value = (x_v[:, b * TILE:(b + 1) * TILE].astype(f32) - term).astype(bf16)
        for e in range(row_blocks):
            dressed[e * col_blocks + b] = value[e * TILE:(e + 1) * TILE]
    for s in range(CAP):
        mine[0][s] = dressed[order[s]]

    def live_part(ref):
        return ref.at[pl.ds(0, CAP)]

    copies = [None] + [
        remote(live_part(mine[0]), live_part(mine[k]), b_send.at[k], b_recv.at[k], {"vir": dst[k]}) for k in range(1, n)]
    swaps = [remote(live_part(mine[k]), live_part(theirs[k]), d_send.at[k], d_recv.at[k], to_core) for k in range(n)]
    for copy in copies[1:]:
        copy.start()

    def fill(dense, gathered, live_of, j):
        count = jnp.int32(0)
        for e in range(row_blocks):
            for b in range(col_blocks):
                live = live_of[j, e, b]
                dense[e * TILE:(e + 1) * TILE, b * TILE:(b + 1) * TILE] = gathered[jnp.where(live != 0, count, CAP)]
                count = count + live

    mask_swap.wait_recv()
    lam_swap.wait_recv()
    for k in range(n):
        if k:
            copies[k].wait_recv()
        swaps[k].start()
        fill(dense_m, mine[k], mask, src[k])
        acc[...] = jnp.dot(lam_m[src[k]], dense_m[...], preferred_element_type=f32)
        swaps[k].wait_recv()
        fill(dense_t, theirs[k], other, src[k])
        out[0, src[k]] = (acc[...] + jnp.dot(
            lam_t[src[k]], dense_t[...], preferred_element_type=f32)).astype(bf16)

    for copy in t_copies + copies[1:] + swaps + [mask_swap, lam_swap]:
        copy.wait_send()


def body(n, lambda_amps, screened_ints, half_ints, singles, block_mask):
    wide, pairs, rows, half = lambda_amps.shape
    full = screened_ints.shape[2]
    inner, width = singles.shape
    row_blocks, col_blocks = half // TILE, full // TILE
    blocks = row_blocks * col_blocks
    bf16, f32 = jnp.bfloat16, jnp.float32
    dma = pltpu.SemaphoreType.DMA
    tile = (TILE, TILE)
    anywhere, vmem = pl.BlockSpec(memory_space=pl.ANY), pl.BlockSpec(memory_space=pltpu.VMEM)
    lams = [pltpu.VMEM((pairs, rows, half), bf16)] * 2
    dense, total = pltpu.VMEM((half, full), bf16), pltpu.VMEM((rows, full), f32)
    masks = [pltpu.SMEM(block_mask.shape, jnp.int32)] * 2
    held = [pltpu.VMEM((CAP + 1,) + tile, bf16)] * (2 * n)
    args = (lambda_amps, screened_ints, half_ints, singles, block_mask)
    params = pltpu.CompilerParams(collective_id=0, has_side_effects=True, vmem_limit_bytes=56 * 1024 * 1024)
    if n != 4:
        return pl.pallas_call(
            functools.partial(ring_kernel, n),
            out_shape=pltpu.VMEM((1, pairs, rows, full), bf16),
            in_specs=[anywhere] * 5,
            out_specs=vmem,
            scratch_shapes=lams + [
                pltpu.VMEM((half, full), bf16), pltpu.VMEM((half, inner), bf16), pltpu.VMEM((n, inner, width), bf16),
                pltpu.VMEM((blocks,) + tile, bf16), dense, dense, total,
            ] + masks + [dma((5,)), dma((n,)), dma((n,)), dma((n,)), dma((n,)), dma((n,)), dma((n,)), dma((2,)), dma((2,))] + held,
            compiler_params=params,
        )(*args)
    raw = CAP // row_blocks
    held_over = (pltpu.VMEM((n - 1, rows, full), bf16), dense, pltpu.VMEM((rows, half), bf16), total)
    handed = pl.pallas_call(
        grid_kernel,
        out_shape=held_over,
        in_specs=[anywhere] * 5,
        out_specs=(vmem,) * 4,
        scratch_shapes=lams + [
            pltpu.VMEM((blocks,) + tile, bf16), pltpu.VMEM((row_blocks, TILE, inner), bf16),
            pltpu.VMEM((col_blocks, inner, TILE), bf16), pltpu.VMEM((blocks,) + tile, bf16),
        ] + masks + [
            pltpu.VMEM((7 * (CAP + 1) + pairs * rows * half // (TILE * TILE),) + tile, bf16),
            dma((3,)), dma((3,)), dma((2,)), dma((8,)), dma((8,)), pltpu.SemaphoreType.REGULAR((2,)),
        ] + held + [pltpu.VMEM((raw + 1,) + tile, bf16)] * (2 * n),
        compiler_params=params,
    )(*args)
    pieces = 2
    return pl.pallas_call(
        last_kernel,
        out_shape=jax.ShapeDtypeStruct((1, pairs, rows, full), bf16),
        in_specs=[vmem] * 4,
        out_specs=anywhere,
        scratch_shapes=[pltpu.VMEM((pieces, rows, full // pieces), bf16), dma((1,))],
        compiler_params=pltpu.CompilerParams(vmem_limit_bytes=8 * 1024 * 1024),
    )(*handed)


def solution(mesh):
    return jax.shard_map(
        functools.partial(body, mesh.shape["vir"]),
        mesh=mesh,
        in_specs=(
            P(None, "occ", "vir", "ka"),
            P(("occ", "vir"), "ka", None),
            P(("occ", "vir"), "ka", None),
            P(None, "vir"),
            P("occ", "ka", None),
        ),
        out_specs=P("ka", "occ", "vir", None),
        check_vma=False,
    )
```

```python
import functools

import jax
import jax.numpy as jnp
from jax import lax
from jax.experimental import pallas as pl
from jax.experimental.pallas import tpu as pltpu
from jax.sharding import PartitionSpec as P

TILE = 128
CAP = 16
MESH = pl.DeviceIdType.MESH


def remote(source, target, send, recv, where):
    return pltpu.make_async_remote_copy(
        src_ref=source, dst_ref=target, send_sem=send, recv_sem=recv, device_id=where, device_id_type=MESH)


def enter(places):
    barrier = pltpu.get_barrier_semaphore()
    for place in places:
        pl.semaphore_signal(barrier, inc=1, device_id=place, device_id_type=MESH)
    return barrier


def top_row(live_of, j, row_blocks, col_blocks):
    best, most = jnp.int32(0), jnp.int32(-1)
    for e in range(row_blocks):
        total = live_of[j, e, 0]
        for b in range(1, col_blocks):
            total = total + live_of[j, e, b]
        best = jnp.where(total > most, e, best)
        most = jnp.maximum(total, most)
    return best


def raw_columns(live_of, j, row, raw, col_blocks):
    found = [jnp.int32(0)] * raw
    rank = jnp.int32(0)
    for b in range(col_blocks):
        live = live_of[j, row, b]
        found = [jnp.where((live != 0) & (rank == s), b, found[s]) for s in range(raw)]
        rank = rank + live
    return found


def slots_of(live_of, j, row, raw, late, row_blocks, col_blocks, cols):
    early_next, late_next = jnp.int32(raw), jnp.int32(CAP - 1)
    is_late = [late == g for g in range(col_blocks // cols)]
    slots = []
    for e in range(row_blocks):
        room = jnp.where(row == e, raw, 0)
        rank = jnp.int32(0)
        for b in range(col_blocks):
            live = live_of[j, e, b]
            is_raw = rank < room
            behind = is_late[b // cols]
            slot = jnp.where(is_raw, rank, jnp.where(behind, late_next, early_next))
            slots.append(jnp.where(live != 0, slot, CAP))
            step = jnp.where(is_raw, 0, live)
            late_next = late_next - jnp.where(behind, step, 0)
            early_next = early_next + jnp.where(behind, 0, step)
            rank = rank + live
    return slots


def grid_kernel(lam, x, y, t, mask_any, stage, dense_t, lam_last, acc, lam_m, lam_t, x_v, y_v, t_v, dressed, mask, other,
                spare, in_sem, s_sem, t_recv, b_recv, d_recv, ready, *bufs):
    n = 4
    mine, theirs, raw_m, raw_t = bufs[:n], bufs[n:2 * n], bufs[2 * n:3 * n], bufs[3 * n:]
    v, c = lax.axis_index("vir"), lax.axis_index("ka")
    row, col = v // 2, v % 2
    ids = [v, row * 2 + (1 - col), (1 - row) * 2 + col, (1 - row) * 2 + (1 - col)]
    partner = 1 - c
    row_blocks, col_blocks = y_v.shape[0], t_v.shape[0]
    inner = t_v.shape[1]
    cols = col_blocks // n
    part = inner // 2
    raw = CAP // row_blocks
    late = row_blocks * cols
    first = CAP - raw - late
    lam_blocks = lam_m.shape[0] * lam_m.shape[1] * lam_m.shape[2] // (TILE * TILE)
    f32, bf16 = jnp.float32, jnp.bfloat16

    to_x, to_y, to_core = {"vir": ids[1]}, {"vir": ids[2]}, {"ka": partner}
    near = [None, to_x, to_y]
    last = [None, col == 1, row == 1]
    barrier = enter([to_core])
    for k in (1, 2):
        @pl.when(jnp.logical_not(last[k]))
        def _():
            pl.semaphore_signal(barrier, inc=1, device_id=near[k], device_id_type=MESH)

    def block(e, b):
        return x.at[0, pl.ds(e * TILE, TILE), pl.ds(b * TILE, TILE)]

    def drain(sem, count):
        pltpu.make_async_copy(spare.at[pl.ds(0, count)], spare.at[pl.ds(0, count)], sem).wait()

    mask_load = pltpu.make_async_copy(mask_any, mask, in_sem.at[0])
    t_loads = [pltpu.make_async_copy(
        t.at[:, pl.ds(i * TILE, TILE)], t_v.at[v * cols + i], in_sem.at[1]) for i in range(cols)]
    y_loads = [pltpu.make_async_copy(
        y.at[0, pl.ds(e * TILE, TILE)], y_v.at[e], in_sem.at[2]) for e in range(row_blocks)]
    x_loads = [pltpu.make_async_copy(
        block(p // col_blocks, p % col_blocks), x_v.at[p], in_sem.at[2]) for p in range(row_blocks * col_blocks)]
    lam_load = pltpu.make_async_copy(lam.at[c], lam_m, d_recv.at[5])
    mask_load.start()
    for load in t_loads + y_loads + x_loads:
        load.start()

    zero = jnp.zeros((TILE, TILE), bf16)
    for k in range(n):
        mine[k][CAP] = zero
        theirs[k][CAP] = zero

    pl.semaphore_wait(barrier, 1 + row + col)
    for k in (1, 2):
        @pl.when(last[k])
        def _():
            pl.semaphore_signal(ready.at[k - 1], inc=1, device_id=near[k], device_id_type=MESH)

    mask_load.wait()
    lead = top_row(mask, v, row_blocks, col_blocks)
    lead_columns = raw_columns(mask, v, lead, raw, col_blocks)
    drain(in_sem.at[1], cols)
    def t_part(k):
        return t_v.at[pl.ds(ids[k] * cols, cols)]

    t_copies = [None] + [remote(t_part(0), t_part(0), s_sem.at[1], t_recv.at[1], near[k]) for k in (1, 2)]
    t_relay = remote(t_part(1), t_part(1), s_sem.at[1], t_recv.at[0], to_y)
    t_swaps = [None] + [remote(t_part(k), t_part(k), s_sem.at[1], d_recv.at[k // 3], to_core) for k in (1, 2, 3)]

    for k in (1, 2):
        @pl.when((c == 1) & last[k])
        def _():
            t_copies[k].start()

    mask_swap = remote(mask_any, other, s_sem.at[2], d_recv.at[2], to_core)
    mask_swap.start()

    drain(in_sem.at[2], row_blocks + row_blocks * col_blocks)
    lam_load.start()
    for s in range(raw):
        raw_m[0][s] = x_v[lead * col_blocks + lead_columns[s]]
    raw_m[0][raw] = y_v[lead]

    spans = [(0, raw // 2), (raw // 2, raw + 1)]
    at = raw
    for size in [first // 2] * 2 + [late // 2 - 1, 1] * 2:
        spans.append((at, at + size))
        at += size
    low, high = (0, 2, 4, 5), (1, 3, 6, 7)
    groups = [(0, 0), (1, 1), (2, 2), (3, 3), (4, 5), (6, 7)]
    paths = [None, (0, 1, 2, 3, 4, 5), (1, 0, 3, 2, 5, 4)]

    def chunk(raws, gathered, k, q, r):
        start, stop = spans[q][0], spans[r][1]
        return (raws if q < 2 else gathered)[k].at[pl.ds(start, stop - start)]

    stages = [None, (0, 0, 1, 1, 2, 7), (0, 0, 1, 1, 7, 2)]
    last_stages = (0, 0, 1, 1, 2, 3, 2, 3)
    sizes = [raw + 1, first, late]

    def own_copy(k, g):
        q, r = groups[g]
        return remote(chunk(raw_m, mine, 0, q, r), chunk(raw_m, mine, k, q, r), s_sem.at[0], b_recv.at[stages[k][g]], near[k])

    def relay_copy(k, q):
        return remote(chunk(raw_m, mine, k, q, q), chunk(raw_m, mine, 3, q, q), s_sem.at[0],
                      b_recv.at[3 + last_stages[q]], near[3 - k])

    def swap(k, q, r):
        sem = 3 + k // 3 if q < 2 else 6 + k // 3
        return remote(chunk(raw_m, mine, k, q, r), chunk(raw_t, theirs, k, q, r), s_sem.at[0], d_recv.at[sem], to_core)

    own_swap = remote(mine[0].at[pl.ds(0, CAP)], theirs[0].at[pl.ds(0, CAP)], s_sem.at[0], d_recv.at[5], to_core)
    lam_swap = remote(lam.at[partner], lam_t, s_sem.at[0], d_recv.at[5], to_core)

    def raw_start(k):
        own_copy(k, paths[k][0]).start()

        @pl.when((c == 0) | (k == 1))
        def _():
            own_copy(k, paths[k][1]).start()

    for k in (1, 2):
        @pl.when(last[k])
        def _():
            raw_start(k)

    for k in (1, 2):
        @pl.when(jnp.logical_not(last[k]))
        def _():
            pl.semaphore_wait(ready.at[k - 1], 1)

            @pl.when(c == 1)
            def _():
                t_copies[k].start()

            raw_start(k)

    @pl.when(c == 0)
    def _():
        lam_swap.start()

    def dress(k):
        for i in range(cols):
            b = ids[k] * cols + i
            columns = t_v[b]
            for e in range(row_blocks):
                term = jnp.dot(y_v[e], columns, preferred_element_type=f32)
                dressed[e * col_blocks + b] = (x_v[e * col_blocks + b].astype(f32) - term).astype(bf16)

    slots = slots_of(mask, v, lead, raw, n - 1 - v, row_blocks, col_blocks, cols)
    order = []
    for s in range(raw, CAP):
        place = jnp.int32(0)
        for p, slot in enumerate(slots):
            place = jnp.where(slot == s, p, place)
        order.append(place)

    dress(0)
    @pl.when(c == 1)
    def _():
        drain(t_recv.at[1], 2 * cols)
        t_relay.start()
        own_copy(2, 0).start()
        t_swaps[1].start()
        t_swaps[2].start()

    @pl.when(c == 0)
    def _():
        drain(d_recv.at[0], 2 * cols)

    dress(1)
    dress(2)

    def pack(q):
        for s in range(*spans[q]):
            mine[0][s] = dressed[order[s - raw]]

    pack(2)
    pack(3)
    for i in (2, 3):
        for k in (1, 2):
            own_copy(k, paths[k][i]).start()
    @pl.when(c == 1)
    def _():
        t_relay.wait_recv()
        t_swaps[3].start()
        lam_swap.start()

    @pl.when(c == 0)
    def _():
        t_swaps[3].wait_recv()

    dress(3)
    for i in (4, 5):
        for q in groups[i]:
            pack(q)
    for i in (4, 5):
        for k in (1, 2):
            own_copy(k, paths[k][i]).start()
    for s in range(raw):
        mine[0][s] = dressed[lead * col_blocks + lead_columns[s]]
    own_swap.start()
    mask_swap.wait_recv()

    def mend(k, raws, gathered, live_of):
        best = top_row(live_of, ids[k], row_blocks, col_blocks)
        places = raw_columns(live_of, ids[k], best, raw, col_blocks)
        rows = raws[k][raw]
        for s in range(raw):
            term = jnp.dot(rows, t_v[places[s]], preferred_element_type=f32)
            gathered[k][s] = (raws[k][s].astype(f32) - term).astype(bf16)

    def places(live_of, k):
        j = ids[k]
        best = top_row(live_of, j, row_blocks, col_blocks)
        return slots_of(live_of, j, best, raw, n - 1 - j, row_blocks, col_blocks, cols)

    def tile(gathered, slots, e, b):
        rows = [jnp.concatenate([gathered[slots[p * col_blocks + q]] for q in (b, b + 1)], axis=1) for p in (e, e + 1)]
        return jnp.concatenate(rows, axis=0)

    def product(pairs, b):
        return sum(
            jnp.dot(rows[:, e * TILE:(e + 2) * TILE], tile(gathered, slots, e, b), preferred_element_type=f32)
            for rows, gathered, slots in pairs for e in range(0, row_blocks, 2))

    def both(k):
        mine_k = (lam_m[ids[k]], mine[k], places(mask, k))
        theirs_k = (lam_t[ids[k]], theirs[k], places(other, k))
        for b in range(0, col_blocks, 2):
            stage[k, :, b * TILE:(b + 2) * TILE] = product([mine_k, theirs_k], b).astype(bf16)

    def relay(level):
        for q in (0, 1, 2, 3, 4, 6, 5, 7):
            if min(last_stages[q], 2) == level:
                relay_copy(1 if q in low else 2, q).start()

    def arrive(level):
        drain(b_recv.at[level], 2 * sizes[level])
        relay(level)
        for k in (1, 2):
            swap(k, *((0, 1), (2, 3))[level]).start()

    arrive(0)
    arrive(1)
    mend(1, raw_m, mine, mask)
    mend(2, raw_m, mine, mask)
    drain(d_recv.at[3], 2 * (raw + 1))
    mend(1, raw_t, theirs, other)
    mend(2, raw_t, theirs, other)
    drain(d_recv.at[5], CAP + 2 * lam_blocks)
    both(0)
    drain(b_recv.at[2], late)
    @pl.when(c == 0)
    def _():
        relay(2)

    swap(1, 4, 5).start()
    swap(2, 6, 7).start()
    drain(b_recv.at[7], late)
    swap(1, 6, 7).start()
    swap(2, 4, 5).start()
    here, there = places(mask, 3), places(other, 3)
    lam_last[...] = lam_t[ids[3]]
    drain(b_recv.at[3], raw + 1)
    swap(3, 0, 1).start()
    drain(d_recv.at[6], 2 * (CAP - raw))

    @pl.when(c == 1)
    def _():
        relay(2)

    both(1)
    drain(b_recv.at[4], first)
    swap(3, 2, 3).start()
    mend(3, raw_m, mine, mask)
    drain(d_recv.at[4], raw + 1)
    mend(3, raw_t, theirs, other)
    both(2)
    drain(b_recv.at[5], late - 2)
    for q in (4, 6):
        swap(3, q, q).start()
    drain(b_recv.at[6], 2)
    for q in (5, 7):
        swap(3, q, q).start()
    for b in range(0, col_blocks, 2):
        acc[:, b * TILE:(b + 2) * TILE] = product([(lam_m[ids[3]], mine[3], here)], b)
    drain(d_recv.at[7], CAP - raw)
    for b in range(0, col_blocks, 2):
        for e in range(0, row_blocks, 2):
            dense_t[e * TILE:(e + 2) * TILE, b * TILE:(b + 2) * TILE] = tile(theirs[3], there, e, b)

    @pl.when(c == 1)
    def _():
        drain(s_sem.at[1], 6 * cols)

    mask_swap.wait_send()
    drain(s_sem.at[0], 3 * (CAP + 1) + CAP + 3 * (CAP + 1) + lam_blocks)


def last_kernel(done, dense_t, lam_last, acc, out, stage, sem):
    v = lax.axis_index("vir")
    row, col = v // 2, v % 2
    ids = [v, row * 2 + (1 - col), (1 - row) * 2 + col, 3 - v]
    pieces, rows, width = stage.shape
    for k in range(done.shape[0]):
        pltpu.make_async_copy(done.at[k], out.at[0, ids[k]], sem.at[0]).start()
    for i in range(pieces):
        columns = slice(i * width, (i + 1) * width)
        stage[i] = (acc[:, columns] + jnp.dot(
            lam_last[...], dense_t[:, columns], preferred_element_type=jnp.float32)).astype(jnp.bfloat16)
        pltpu.make_async_copy(stage.at[i], out.at[0, ids[3], :, pl.ds(i * width, width)], sem.at[0]).start()
    pltpu.make_async_copy(out, out, sem.at[0]).wait()


def ring_kernel(n, lam, x, y, t, mask_any, out, lam_m, lam_t, x_v, y_v, t_v, dressed, dense_m, dense_t, acc, mask, other,
                in_sem, t_send, t_recv, b_send, b_recv, d_send, d_recv, l_send, l_recv, *bufs):
    mine, theirs = bufs[:n], bufs[n:]
    v, c = lax.axis_index("vir"), lax.axis_index("ka")
    dst, src = [(v + k) % n for k in range(n)], [(v + n - k) % n for k in range(n)]
    half, full = x_v.shape
    width = t_v.shape[2]
    row_blocks, col_blocks = half // TILE, full // TILE
    f32, bf16 = jnp.float32, jnp.bfloat16
    loads = [pltpu.make_async_copy(source, target, in_sem.at[i]) for i, (source, target) in enumerate(
        [(mask_any, mask), (t, t_v.at[v]), (y.at[0], y_v), (x.at[0], x_v), (lam.at[c], lam_m)])]
    for load in loads:
        load.start()
    to_core = {"ka": 1 - c}
    barrier = enter([{"vir": dst[k]} for k in range(1, n)] + [to_core])
    for load in loads:
        load.wait()
    pl.semaphore_wait(barrier, n)

    t_copies = [remote(t_v.at[v], t_v.at[v], t_send.at[k], t_recv.at[k], {"vir": dst[k]}) for k in range(1, n)]
    arrivals = [remote(t_v.at[v], t_v.at[src[k]], t_send.at[k], t_recv.at[k], {"vir": dst[k]}) for k in range(1, n)]
    for copy in t_copies:
        copy.start()
    mask_swap = remote(mask_any, other, l_send.at[0], l_recv.at[0], to_core)
    lam_swap = remote(lam.at[1 - c], lam_t, l_send.at[1], l_recv.at[1], to_core)
    mask_swap.start()
    lam_swap.start()

    zero = jnp.zeros((TILE, TILE), bf16)
    for k in range(n):
        mine[k][CAP] = zero
        theirs[k][CAP] = zero
    order = [jnp.int32(0)] * CAP
    count = jnp.int32(0)
    for p in range(row_blocks * col_blocks):
        live = mask[v, p // col_blocks, p % col_blocks]
        order = [jnp.where((live != 0) & (count == s), p, order[s]) for s in range(CAP)]
        count = count + live

    for copy in arrivals:
        copy.wait_recv()
    for b in range(col_blocks):
        if width >= TILE:
            owner, offset = b * TILE // width, b * TILE % width
            columns = t_v[owner][:, offset:offset + TILE]
        else:
            group = TILE // width
            columns = jnp.concatenate([t_v[b * group + i] for i in range(group)], axis=1)
        term = jnp.dot(y_v[...], columns, preferred_element_type=f32)
        value = (x_v[:, b * TILE:(b + 1) * TILE].astype(f32) - term).astype(bf16)
        for e in range(row_blocks):
            dressed[e * col_blocks + b] = value[e * TILE:(e + 1) * TILE]
    for s in range(CAP):
        mine[0][s] = dressed[order[s]]

    def live_part(ref):
        return ref.at[pl.ds(0, CAP)]

    copies = [None] + [
        remote(live_part(mine[0]), live_part(mine[k]), b_send.at[k], b_recv.at[k], {"vir": dst[k]}) for k in range(1, n)]
    swaps = [remote(live_part(mine[k]), live_part(theirs[k]), d_send.at[k], d_recv.at[k], to_core) for k in range(n)]
    for copy in copies[1:]:
        copy.start()

    def fill(dense, gathered, live_of, j):
        count = jnp.int32(0)
        for e in range(row_blocks):
            for b in range(col_blocks):
                live = live_of[j, e, b]
                dense[e * TILE:(e + 1) * TILE, b * TILE:(b + 1) * TILE] = gathered[jnp.where(live != 0, count, CAP)]
                count = count + live

    mask_swap.wait_recv()
    lam_swap.wait_recv()
    for k in range(n):
        if k:
            copies[k].wait_recv()
        swaps[k].start()
        fill(dense_m, mine[k], mask, src[k])
        acc[...] = jnp.dot(lam_m[src[k]], dense_m[...], preferred_element_type=f32)
        swaps[k].wait_recv()
        fill(dense_t, theirs[k], other, src[k])
        out[0, src[k]] = (acc[...] + jnp.dot(
            lam_t[src[k]], dense_t[...], preferred_element_type=f32)).astype(bf16)

    for copy in t_copies + copies[1:] + swaps + [mask_swap, lam_swap]:
        copy.wait_send()


def body(n, lambda_amps, screened_ints, half_ints, singles, block_mask):
    wide, pairs, rows, half = lambda_amps.shape
    full = screened_ints.shape[2]
    inner, width = singles.shape
    row_blocks, col_blocks = half // TILE, full // TILE
    blocks = row_blocks * col_blocks
    bf16, f32 = jnp.bfloat16, jnp.float32
    dma = pltpu.SemaphoreType.DMA
    tile = (TILE, TILE)
    anywhere, vmem = pl.BlockSpec(memory_space=pl.ANY), pl.BlockSpec(memory_space=pltpu.VMEM)
    lams = [pltpu.VMEM((pairs, rows, half), bf16)] * 2
    dense, total = pltpu.VMEM((half, full), bf16), pltpu.VMEM((rows, full), f32)
    masks = [pltpu.SMEM(block_mask.shape, jnp.int32)] * 2
    held = [pltpu.VMEM((CAP + 1,) + tile, bf16)] * (2 * n)
    args = (lambda_amps, screened_ints, half_ints, singles, block_mask)
    params = pltpu.CompilerParams(collective_id=0, has_side_effects=True, vmem_limit_bytes=56 * 1024 * 1024)
    if n != 4:
        return pl.pallas_call(
            functools.partial(ring_kernel, n),
            out_shape=pltpu.VMEM((1, pairs, rows, full), bf16),
            in_specs=[anywhere] * 5,
            out_specs=vmem,
            scratch_shapes=lams + [
                pltpu.VMEM((half, full), bf16), pltpu.VMEM((half, inner), bf16), pltpu.VMEM((n, inner, width), bf16),
                pltpu.VMEM((blocks,) + tile, bf16), dense, dense, total,
            ] + masks + [dma((5,)), dma((n,)), dma((n,)), dma((n,)), dma((n,)), dma((n,)), dma((n,)), dma((2,)), dma((2,))] + held,
            compiler_params=params,
        )(*args)
    raw = CAP // row_blocks
    held_over = (pltpu.VMEM((n - 1, rows, full), bf16), dense, pltpu.VMEM((rows, half), bf16), total)
    handed = pl.pallas_call(
        grid_kernel,
        out_shape=held_over,
        in_specs=[anywhere] * 5,
        out_specs=(vmem,) * 4,
        scratch_shapes=lams + [
            pltpu.VMEM((blocks,) + tile, bf16), pltpu.VMEM((row_blocks, TILE, inner), bf16),
            pltpu.VMEM((col_blocks, inner, TILE), bf16), pltpu.VMEM((blocks,) + tile, bf16),
        ] + masks + [
            pltpu.VMEM((7 * (CAP + 1) + pairs * rows * half // (TILE * TILE),) + tile, bf16),
            dma((3,)), dma((3,)), dma((2,)), dma((8,)), dma((8,)), pltpu.SemaphoreType.REGULAR((2,)),
        ] + held + [pltpu.VMEM((raw + 1,) + tile, bf16)] * (2 * n),
        compiler_params=params,
    )(*args)
    pieces = 2
    return pl.pallas_call(
        last_kernel,
        out_shape=jax.ShapeDtypeStruct((1, pairs, rows, full), bf16),
        in_specs=[vmem] * 4,
        out_specs=anywhere,
        scratch_shapes=[pltpu.VMEM((pieces, rows, full // pieces), bf16), dma((1,))],
        compiler_params=pltpu.CompilerParams(vmem_limit_bytes=8 * 1024 * 1024),
    )(*handed)


def solution(mesh):
    return jax.shard_map(
        functools.partial(body, mesh.shape["vir"]),
        mesh=mesh,
        in_specs=(
            P(None, "occ", "vir", "ka"),
            P(("occ", "vir"), "ka", None),
            P(("occ", "vir"), "ka", None),
            P(None, "vir"),
            P("occ", "ka", None),
        ),
        out_specs=P("ka", "occ", "vir", None),
        check_vma=False,
    )
```

```python
import functools

import jax
import jax.numpy as jnp
from jax import lax
from jax.experimental import pallas as pl
from jax.experimental.pallas import tpu as pltpu
from jax.sharding import PartitionSpec as P

TILE = 128
CAP = 16
MESH = pl.DeviceIdType.MESH


def remote(source, target, send, recv, where):
    return pltpu.make_async_remote_copy(
        src_ref=source, dst_ref=target, send_sem=send, recv_sem=recv, device_id=where, device_id_type=MESH)


def enter(places):
    barrier = pltpu.get_barrier_semaphore()
    for place in places:
        pl.semaphore_signal(barrier, inc=1, device_id=place, device_id_type=MESH)
    return barrier


def top_row(live_of, j, row_blocks, col_blocks):
    best, most = jnp.int32(0), jnp.int32(-1)
    for e in range(row_blocks):
        total = live_of[j, e, 0]
        for b in range(1, col_blocks):
            total = total + live_of[j, e, b]
        best = jnp.where(total > most, e, best)
        most = jnp.maximum(total, most)
    return best


def raw_columns(live_of, j, row, raw, col_blocks):
    found = [jnp.int32(0)] * raw
    rank = jnp.int32(0)
    for b in range(col_blocks):
        live = live_of[j, row, b]
        found = [jnp.where((live != 0) & (rank == s), b, found[s]) for s in range(raw)]
        rank = rank + live
    return found


def slots_of(live_of, j, row, raw, late, row_blocks, col_blocks, cols):
    early_next, late_next = jnp.int32(raw), jnp.int32(CAP - 1)
    is_late = [late == g for g in range(col_blocks // cols)]
    slots = []
    for e in range(row_blocks):
        room = jnp.where(row == e, raw, 0)
        rank = jnp.int32(0)
        for b in range(col_blocks):
            live = live_of[j, e, b]
            is_raw = rank < room
            behind = is_late[b // cols]
            slot = jnp.where(is_raw, rank, jnp.where(behind, late_next, early_next))
            slots.append(jnp.where(live != 0, slot, CAP))
            step = jnp.where(is_raw, 0, live)
            late_next = late_next - jnp.where(behind, step, 0)
            early_next = early_next + jnp.where(behind, 0, step)
            rank = rank + live
    return slots


def grid_kernel(lam, x, y, t, mask_any, stage, dense_t, lam_last, acc, lam_m, lam_t, x_v, y_v, t_v, dressed, mask, other,
                spare, in_sem, s_sem, t_recv, b_recv, d_recv, ready, *bufs):
    n = 4
    mine, theirs, raw_m, raw_t = bufs[:n], bufs[n:2 * n], bufs[2 * n:3 * n], bufs[3 * n:]
    v, c = lax.axis_index("vir"), lax.axis_index("ka")
    row, col = v // 2, v % 2
    ids = [v, row * 2 + (1 - col), (1 - row) * 2 + col, (1 - row) * 2 + (1 - col)]
    partner = 1 - c
    row_blocks, col_blocks = y_v.shape[0], t_v.shape[0]
    inner = t_v.shape[1]
    cols = col_blocks // n
    part = inner // 2
    raw = CAP // row_blocks
    late = row_blocks * cols
    first = CAP - raw - late
    lam_blocks = lam_m.shape[0] * lam_m.shape[1] * lam_m.shape[2] // (TILE * TILE)
    f32, bf16 = jnp.float32, jnp.bfloat16

    to_x, to_y, to_core = {"vir": ids[1]}, {"vir": ids[2]}, {"ka": partner}
    near = [None, to_x, to_y]
    last = [None, col == 1, row == 1]
    barrier = enter([to_core])
    for k in (1, 2):
        @pl.when(jnp.logical_not(last[k]))
        def _():
            pl.semaphore_signal(barrier, inc=1, device_id=near[k], device_id_type=MESH)

    def block(e, b):
        return x.at[0, pl.ds(e * TILE, TILE), pl.ds(b * TILE, TILE)]

    def drain(sem, count):
        pltpu.make_async_copy(spare.at[pl.ds(0, count)], spare.at[pl.ds(0, count)], sem).wait()

    mask_load = pltpu.make_async_copy(mask_any, mask, in_sem.at[0])
    t_loads = [pltpu.make_async_copy(
        t.at[:, pl.ds(i * TILE, TILE)], t_v.at[v * cols + i], in_sem.at[1]) for i in range(cols)]
    y_loads = [pltpu.make_async_copy(
        y.at[0, pl.ds(e * TILE, TILE)], y_v.at[e], in_sem.at[2]) for e in range(row_blocks)]
    x_loads = [pltpu.make_async_copy(
        block(p // col_blocks, p % col_blocks), x_v.at[p], in_sem.at[2]) for p in range(row_blocks * col_blocks)]
    lam_load = pltpu.make_async_copy(lam.at[c], lam_m, d_recv.at[5])
    mask_load.start()
    for load in t_loads + y_loads + x_loads:
        load.start()

    zero = jnp.zeros((TILE, TILE), bf16)
    for k in range(n):
        mine[k][CAP] = zero
        theirs[k][CAP] = zero

    pl.semaphore_wait(barrier, 1 + row + col)
    for k in (1, 2):
        @pl.when(last[k])
        def _():
            pl.semaphore_signal(ready.at[k - 1], inc=1, device_id=near[k], device_id_type=MESH)

    mask_load.wait()
    lead = top_row(mask, v, row_blocks, col_blocks)
    lead_columns = raw_columns(mask, v, lead, raw, col_blocks)
    drain(in_sem.at[1], cols)
    def t_part(k):
        return t_v.at[pl.ds(ids[k] * cols, cols)]

    t_copies = [None] + [remote(t_part(0), t_part(0), s_sem.at[1], t_recv.at[1], near[k]) for k in (1, 2)]
    t_relay = remote(t_part(1), t_part(1), s_sem.at[1], t_recv.at[0], to_y)
    t_swaps = [None] + [remote(t_part(k), t_part(k), s_sem.at[1], d_recv.at[k // 3], to_core) for k in (1, 2, 3)]

    for k in (1, 2):
        @pl.when((c == 1) & last[k])
        def _():
            t_copies[k].start()

    mask_swap = remote(mask_any, other, s_sem.at[2], d_recv.at[2], to_core)
    mask_swap.start()

    drain(in_sem.at[2], row_blocks + row_blocks * col_blocks)
    lam_load.start()
    for s in range(raw):
        raw_m[0][s] = x_v[lead * col_blocks + lead_columns[s]]
    raw_m[0][raw] = y_v[lead]

    spans = [(0, raw // 2), (raw // 2, raw + 1)]
    at = raw
    for size in [first // 2] * 2 + [late // 2 - 1, 1] * 2:
        spans.append((at, at + size))
        at += size
    low, high = (0, 2, 4, 5), (1, 3, 6, 7)
    groups = [(0, 0), (1, 1), (2, 2), (3, 3), (4, 5), (6, 7)]
    paths = [None, (0, 1, 2, 3, 4, 5), (1, 0, 3, 2, 5, 4)]

    def chunk(raws, gathered, k, q, r):
        start, stop = spans[q][0], spans[r][1]
        return (raws if q < 2 else gathered)[k].at[pl.ds(start, stop - start)]

    stages = [None, (0, 0, 0, 0, 2, 1), (0, 0, 0, 0, 1, 2)]
    last_stages = (0, 0, 1, 1, 2, 3, 2, 3)
    sizes = [raw + 1, first, late]

    def own_copy(k, g):
        q, r = groups[g]
        return remote(chunk(raw_m, mine, 0, q, r), chunk(raw_m, mine, k, q, r), s_sem.at[0], b_recv.at[stages[k][g]], near[k])

    def relay_copy(k, q):
        return remote(chunk(raw_m, mine, k, q, q), chunk(raw_m, mine, 3, q, q), s_sem.at[0],
                      b_recv.at[3 + last_stages[q]], near[3 - k])

    def swap(k, q, r):
        sem = 3 + k // 3 if q < 2 else 6 + k // 3
        return remote(chunk(raw_m, mine, k, q, r), chunk(raw_t, theirs, k, q, r), s_sem.at[0], d_recv.at[sem], to_core)

    own_swap = remote(mine[0].at[pl.ds(0, CAP)], theirs[0].at[pl.ds(0, CAP)], s_sem.at[0], d_recv.at[5], to_core)
    lam_swap = remote(lam.at[partner], lam_t, s_sem.at[0], d_recv.at[5], to_core)

    def raw_start(k):
        own_copy(k, paths[k][0]).start()

        @pl.when((c == 0) | (k == 1))
        def _():
            own_copy(k, paths[k][1]).start()

    for k in (1, 2):
        @pl.when(last[k])
        def _():
            raw_start(k)

    for k in (1, 2):
        @pl.when(jnp.logical_not(last[k]))
        def _():
            pl.semaphore_wait(ready.at[k - 1], 1)

            @pl.when(c == 1)
            def _():
                t_copies[k].start()

            raw_start(k)

    @pl.when(c == 0)
    def _():
        lam_swap.start()

    def dress(k):
        for i in range(cols):
            b = ids[k] * cols + i
            columns = t_v[b]
            for e in range(row_blocks):
                term = jnp.dot(y_v[e], columns, preferred_element_type=f32)
                dressed[e * col_blocks + b] = (x_v[e * col_blocks + b].astype(f32) - term).astype(bf16)

    slots = slots_of(mask, v, lead, raw, n - 1 - v, row_blocks, col_blocks, cols)
    order = []
    for s in range(raw, CAP):
        place = jnp.int32(0)
        for p, slot in enumerate(slots):
            place = jnp.where(slot == s, p, place)
        order.append(place)

    dress(0)
    @pl.when(c == 1)
    def _():
        drain(t_recv.at[1], 2 * cols)
        t_relay.start()
        own_copy(2, 0).start()
        t_swaps[1].start()
        t_swaps[2].start()

    @pl.when(c == 0)
    def _():
        drain(d_recv.at[0], 2 * cols)

    dress(1)
    dress(2)

    def pack(q):
        for s in range(*spans[q]):
            mine[0][s] = dressed[order[s - raw]]

    pack(2)
    pack(3)
    for i in (2, 3):
        for k in (1, 2):
            own_copy(k, paths[k][i]).start()
    @pl.when(c == 1)
    def _():
        t_relay.wait_recv()
        t_swaps[3].start()
        lam_swap.start()

    @pl.when(c == 0)
    def _():
        t_swaps[3].wait_recv()

    dress(3)
    for i in (4, 5):
        for q in groups[i]:
            pack(q)
    for i in (4, 5):
        for k in (1, 2):
            own_copy(k, paths[k][i]).start()
    for s in range(raw):
        mine[0][s] = dressed[lead * col_blocks + lead_columns[s]]
    own_swap.start()
    mask_swap.wait_recv()

    def mend(k, raws, gathered, live_of):
        best = top_row(live_of, ids[k], row_blocks, col_blocks)
        places = raw_columns(live_of, ids[k], best, raw, col_blocks)
        rows = raws[k][raw]
        for s in range(raw):
            term = jnp.dot(rows, t_v[places[s]], preferred_element_type=f32)
            gathered[k][s] = (raws[k][s].astype(f32) - term).astype(bf16)

    def places(live_of, k):
        j = ids[k]
        best = top_row(live_of, j, row_blocks, col_blocks)
        return slots_of(live_of, j, best, raw, n - 1 - j, row_blocks, col_blocks, cols)

    def tile(gathered, slots, e, b):
        rows = [jnp.concatenate([gathered[slots[p * col_blocks + q]] for q in (b, b + 1)], axis=1) for p in (e, e + 1)]
        return jnp.concatenate(rows, axis=0)

    def product(pairs, b):
        return sum(
            jnp.dot(rows[:, e * TILE:(e + 2) * TILE], tile(gathered, slots, e, b), preferred_element_type=f32)
            for rows, gathered, slots in pairs for e in range(0, row_blocks, 2))

    def both(k):
        mine_k = (lam_m[ids[k]], mine[k], places(mask, k))
        theirs_k = (lam_t[ids[k]], theirs[k], places(other, k))
        for b in range(0, col_blocks, 2):
            stage[k, :, b * TILE:(b + 2) * TILE] = product([mine_k, theirs_k], b).astype(bf16)

    def relay(level):
        for q in (0, 1, 2, 3, 4, 6, 5, 7):
            if min(last_stages[q], 2) == level:
                relay_copy(1 if q in low else 2, q).start()

    def arrive(level):
        relay(level)
        for k in (1, 2):
            swap(k, *((0, 1), (2, 3))[level]).start()

    drain(b_recv.at[0], 2 * (sizes[0] + sizes[1]))
    arrive(0)
    arrive(1)
    mend(1, raw_m, mine, mask)
    mend(2, raw_m, mine, mask)
    drain(d_recv.at[3], 2 * (raw + 1))
    mend(1, raw_t, theirs, other)
    mend(2, raw_t, theirs, other)
    drain(d_recv.at[5], CAP + 2 * lam_blocks)
    both(0)
    drain(b_recv.at[2], late)
    @pl.when(c == 0)
    def _():
        relay(2)

    swap(1, 4, 5).start()
    swap(2, 6, 7).start()
    drain(b_recv.at[1], late)
    swap(1, 6, 7).start()
    swap(2, 4, 5).start()
    here, there = places(mask, 3), places(other, 3)
    lam_last[...] = lam_t[ids[3]]
    drain(b_recv.at[3], raw + 1)
    swap(3, 0, 1).start()
    drain(d_recv.at[6], 2 * (CAP - raw))

    @pl.when(c == 1)
    def _():
        relay(2)

    both(1)
    drain(b_recv.at[4], first)
    swap(3, 2, 3).start()
    mend(3, raw_m, mine, mask)
    drain(d_recv.at[4], raw + 1)
    mend(3, raw_t, theirs, other)
    both(2)
    drain(b_recv.at[5], late - 2)
    for q in (4, 6):
        swap(3, q, q).start()
    drain(b_recv.at[6], 2)
    for q in (5, 7):
        swap(3, q, q).start()
    for b in range(0, col_blocks, 2):
        acc[:, b * TILE:(b + 2) * TILE] = product([(lam_m[ids[3]], mine[3], here)], b)
    drain(d_recv.at[7], CAP - raw)
    for b in range(0, col_blocks, 2):
        for e in range(0, row_blocks, 2):
            dense_t[e * TILE:(e + 2) * TILE, b * TILE:(b + 2) * TILE] = tile(theirs[3], there, e, b)

    @pl.when(c == 1)
    def _():
        drain(s_sem.at[1], 6 * cols)

    mask_swap.wait_send()
    drain(s_sem.at[0], 3 * (CAP + 1) + CAP + 3 * (CAP + 1) + lam_blocks)


def last_kernel(done, dense_t, lam_last, acc, out, stage, sem):
    v = lax.axis_index("vir")
    row, col = v // 2, v % 2
    ids = [v, row * 2 + (1 - col), (1 - row) * 2 + col, 3 - v]
    pieces, rows, width = stage.shape
    for k in range(done.shape[0]):
        pltpu.make_async_copy(done.at[k], out.at[0, ids[k]], sem.at[0]).start()
    for i in range(pieces):
        columns = slice(i * width, (i + 1) * width)
        stage[i] = (acc[:, columns] + jnp.dot(
            lam_last[...], dense_t[:, columns], preferred_element_type=jnp.float32)).astype(jnp.bfloat16)
        pltpu.make_async_copy(stage.at[i], out.at[0, ids[3], :, pl.ds(i * width, width)], sem.at[0]).start()
    pltpu.make_async_copy(out, out, sem.at[0]).wait()


def ring_kernel(n, lam, x, y, t, mask_any, out, lam_m, lam_t, x_v, y_v, t_v, dressed, dense_m, dense_t, acc, mask, other,
                in_sem, t_send, t_recv, b_send, b_recv, d_send, d_recv, l_send, l_recv, *bufs):
    mine, theirs = bufs[:n], bufs[n:]
    v, c = lax.axis_index("vir"), lax.axis_index("ka")
    dst, src = [(v + k) % n for k in range(n)], [(v + n - k) % n for k in range(n)]
    half, full = x_v.shape
    width = t_v.shape[2]
    row_blocks, col_blocks = half // TILE, full // TILE
    f32, bf16 = jnp.float32, jnp.bfloat16
    loads = [pltpu.make_async_copy(source, target, in_sem.at[i]) for i, (source, target) in enumerate(
        [(mask_any, mask), (t, t_v.at[v]), (y.at[0], y_v), (x.at[0], x_v), (lam.at[c], lam_m)])]
    for load in loads:
        load.start()
    to_core = {"ka": 1 - c}
    barrier = enter([{"vir": dst[k]} for k in range(1, n)] + [to_core])
    for load in loads:
        load.wait()
    pl.semaphore_wait(barrier, n)

    t_copies = [remote(t_v.at[v], t_v.at[v], t_send.at[k], t_recv.at[k], {"vir": dst[k]}) for k in range(1, n)]
    arrivals = [remote(t_v.at[v], t_v.at[src[k]], t_send.at[k], t_recv.at[k], {"vir": dst[k]}) for k in range(1, n)]
    for copy in t_copies:
        copy.start()
    mask_swap = remote(mask_any, other, l_send.at[0], l_recv.at[0], to_core)
    lam_swap = remote(lam.at[1 - c], lam_t, l_send.at[1], l_recv.at[1], to_core)
    mask_swap.start()
    lam_swap.start()

    zero = jnp.zeros((TILE, TILE), bf16)
    for k in range(n):
        mine[k][CAP] = zero
        theirs[k][CAP] = zero
    order = [jnp.int32(0)] * CAP
    count = jnp.int32(0)
    for p in range(row_blocks * col_blocks):
        live = mask[v, p // col_blocks, p % col_blocks]
        order = [jnp.where((live != 0) & (count == s), p, order[s]) for s in range(CAP)]
        count = count + live

    for copy in arrivals:
        copy.wait_recv()
    for b in range(col_blocks):
        if width >= TILE:
            owner, offset = b * TILE // width, b * TILE % width
            columns = t_v[owner][:, offset:offset + TILE]
        else:
            group = TILE // width
            columns = jnp.concatenate([t_v[b * group + i] for i in range(group)], axis=1)
        term = jnp.dot(y_v[...], columns, preferred_element_type=f32)
        value = (x_v[:, b * TILE:(b + 1) * TILE].astype(f32) - term).astype(bf16)
        for e in range(row_blocks):
            dressed[e * col_blocks + b] = value[e * TILE:(e + 1) * TILE]
    for s in range(CAP):
        mine[0][s] = dressed[order[s]]

    def live_part(ref):
        return ref.at[pl.ds(0, CAP)]

    copies = [None] + [
        remote(live_part(mine[0]), live_part(mine[k]), b_send.at[k], b_recv.at[k], {"vir": dst[k]}) for k in range(1, n)]
    swaps = [remote(live_part(mine[k]), live_part(theirs[k]), d_send.at[k], d_recv.at[k], to_core) for k in range(n)]
    for copy in copies[1:]:
        copy.start()

    def fill(dense, gathered, live_of, j):
        count = jnp.int32(0)
        for e in range(row_blocks):
            for b in range(col_blocks):
                live = live_of[j, e, b]
                dense[e * TILE:(e + 1) * TILE, b * TILE:(b + 1) * TILE] = gathered[jnp.where(live != 0, count, CAP)]
                count = count + live

    mask_swap.wait_recv()
    lam_swap.wait_recv()
    for k in range(n):
        if k:
            copies[k].wait_recv()
        swaps[k].start()
        fill(dense_m, mine[k], mask, src[k])
        acc[...] = jnp.dot(lam_m[src[k]], dense_m[...], preferred_element_type=f32)
        swaps[k].wait_recv()
        fill(dense_t, theirs[k], other, src[k])
        out[0, src[k]] = (acc[...] + jnp.dot(
            lam_t[src[k]], dense_t[...], preferred_element_type=f32)).astype(bf16)

    for copy in t_copies + copies[1:] + swaps + [mask_swap, lam_swap]:
        copy.wait_send()


def body(n, lambda_amps, screened_ints, half_ints, singles, block_mask):
    wide, pairs, rows, half = lambda_amps.shape
    full = screened_ints.shape[2]
    inner, width = singles.shape
    row_blocks, col_blocks = half // TILE, full // TILE
    blocks = row_blocks * col_blocks
    bf16, f32 = jnp.bfloat16, jnp.float32
    dma = pltpu.SemaphoreType.DMA
    tile = (TILE, TILE)
    anywhere, vmem = pl.BlockSpec(memory_space=pl.ANY), pl.BlockSpec(memory_space=pltpu.VMEM)
    lams = [pltpu.VMEM((pairs, rows, half), bf16)] * 2
    dense, total = pltpu.VMEM((half, full), bf16), pltpu.VMEM((rows, full), f32)
    masks = [pltpu.SMEM(block_mask.shape, jnp.int32)] * 2
    held = [pltpu.VMEM((CAP + 1,) + tile, bf16)] * (2 * n)
    args = (lambda_amps, screened_ints, half_ints, singles, block_mask)
    params = pltpu.CompilerParams(collective_id=0, has_side_effects=True, vmem_limit_bytes=56 * 1024 * 1024)
    if n != 4:
        return pl.pallas_call(
            functools.partial(ring_kernel, n),
            out_shape=pltpu.VMEM((1, pairs, rows, full), bf16),
            in_specs=[anywhere] * 5,
            out_specs=vmem,
            scratch_shapes=lams + [
                pltpu.VMEM((half, full), bf16), pltpu.VMEM((half, inner), bf16), pltpu.VMEM((n, inner, width), bf16),
                pltpu.VMEM((blocks,) + tile, bf16), dense, dense, total,
            ] + masks + [dma((5,)), dma((n,)), dma((n,)), dma((n,)), dma((n,)), dma((n,)), dma((n,)), dma((2,)), dma((2,))] + held,
            compiler_params=params,
        )(*args)
    raw = CAP // row_blocks
    held_over = (pltpu.VMEM((n - 1, rows, full), bf16), dense, pltpu.VMEM((rows, half), bf16), total)
    handed = pl.pallas_call(
        grid_kernel,
        out_shape=held_over,
        in_specs=[anywhere] * 5,
        out_specs=(vmem,) * 4,
        scratch_shapes=lams + [
            pltpu.VMEM((blocks,) + tile, bf16), pltpu.VMEM((row_blocks, TILE, inner), bf16),
            pltpu.VMEM((col_blocks, inner, TILE), bf16), pltpu.VMEM((blocks,) + tile, bf16),
        ] + masks + [
            pltpu.VMEM((7 * (CAP + 1) + pairs * rows * half // (TILE * TILE),) + tile, bf16),
            dma((3,)), dma((3,)), dma((2,)), dma((7,)), dma((8,)), pltpu.SemaphoreType.REGULAR((2,)),
        ] + held + [pltpu.VMEM((raw + 1,) + tile, bf16)] * (2 * n),
        compiler_params=params,
    )(*args)
    pieces = 2
    return pl.pallas_call(
        last_kernel,
        out_shape=jax.ShapeDtypeStruct((1, pairs, rows, full), bf16),
        in_specs=[vmem] * 4,
        out_specs=anywhere,
        scratch_shapes=[pltpu.VMEM((pieces, rows, full // pieces), bf16), dma((1,))],
        compiler_params=pltpu.CompilerParams(vmem_limit_bytes=8 * 1024 * 1024),
    )(*handed)


def solution(mesh):
    return jax.shard_map(
        functools.partial(body, mesh.shape["vir"]),
        mesh=mesh,
        in_specs=(
            P(None, "occ", "vir", "ka"),
            P(("occ", "vir"), "ka", None),
            P(("occ", "vir"), "ka", None),
            P(None, "vir"),
            P("occ", "ka", None),
        ),
        out_specs=P("ka", "occ", "vir", None),
        check_vma=False,
    )
```

```python
import functools

import jax
import jax.numpy as jnp
from jax import lax
from jax.experimental import pallas as pl
from jax.experimental.pallas import tpu as pltpu
from jax.sharding import PartitionSpec as P

TILE = 128
CAP = 16
MESH = pl.DeviceIdType.MESH


def remote(source, target, send, recv, where):
    return pltpu.make_async_remote_copy(
        src_ref=source, dst_ref=target, send_sem=send, recv_sem=recv, device_id=where, device_id_type=MESH)


def enter(places):
    barrier = pltpu.get_barrier_semaphore()
    for place in places:
        pl.semaphore_signal(barrier, inc=1, device_id=place, device_id_type=MESH)
    return barrier


def top_row(live_of, j, row_blocks, col_blocks):
    best, most = jnp.int32(0), jnp.int32(-1)
    for e in range(row_blocks):
        total = live_of[j, e, 0]
        for b in range(1, col_blocks):
            total = total + live_of[j, e, b]
        best = jnp.where(total > most, e, best)
        most = jnp.maximum(total, most)
    return best


def raw_columns(live_of, j, row, raw, col_blocks):
    found = [jnp.int32(0)] * raw
    rank = jnp.int32(0)
    for b in range(col_blocks):
        live = live_of[j, row, b]
        found = [jnp.where((live != 0) & (rank == s), b, found[s]) for s in range(raw)]
        rank = rank + live
    return found


def slots_of(live_of, j, row, raw, late, row_blocks, col_blocks, cols):
    early_next, late_next = jnp.int32(raw), jnp.int32(CAP - 1)
    is_late = [late == g for g in range(col_blocks // cols)]
    slots = []
    for e in range(row_blocks):
        room = jnp.where(row == e, raw, 0)
        rank = jnp.int32(0)
        for b in range(col_blocks):
            live = live_of[j, e, b]
            is_raw = rank < room
            behind = is_late[b // cols]
            slot = jnp.where(is_raw, rank, jnp.where(behind, late_next, early_next))
            slots.append(jnp.where(live != 0, slot, CAP))
            step = jnp.where(is_raw, 0, live)
            late_next = late_next - jnp.where(behind, step, 0)
            early_next = early_next + jnp.where(behind, 0, step)
            rank = rank + live
    return slots


def grid_kernel(lam, x, y, t, mask_any, stage, dense_t, lam_last, acc, lam_m, lam_t, x_v, y_v, t_v, dressed, mask, other,
                spare, in_sem, s_sem, t_recv, b_recv, d_recv, ready, *bufs):
    n = 4
    mine, theirs, raw_m, raw_t = bufs[:n], bufs[n:2 * n], bufs[2 * n:3 * n], bufs[3 * n:]
    v, c = lax.axis_index("vir"), lax.axis_index("ka")
    row, col = v // 2, v % 2
    ids = [v, row * 2 + (1 - col), (1 - row) * 2 + col, (1 - row) * 2 + (1 - col)]
    partner = 1 - c
    row_blocks, col_blocks = y_v.shape[0], t_v.shape[0]
    inner = t_v.shape[1]
    cols = col_blocks // n
    part = inner // 2
    raw = CAP // row_blocks
    late = row_blocks * cols
    first = CAP - raw - late
    lam_blocks = lam_m.shape[0] * lam_m.shape[1] * lam_m.shape[2] // (TILE * TILE)
    f32, bf16 = jnp.float32, jnp.bfloat16

    to_x, to_y, to_core = {"vir": ids[1]}, {"vir": ids[2]}, {"ka": partner}
    near = [None, to_x, to_y]
    last = [None, col == 1, row == 1]
    barrier = enter([to_core])
    for k in (1, 2):
        @pl.when(jnp.logical_not(last[k]))
        def _():
            pl.semaphore_signal(barrier, inc=1, device_id=near[k], device_id_type=MESH)

    def block(e, b):
        return x.at[0, pl.ds(e * TILE, TILE), pl.ds(b * TILE, TILE)]

    def drain(sem, count):
        pltpu.make_async_copy(spare.at[pl.ds(0, count)], spare.at[pl.ds(0, count)], sem).wait()

    mask_load = pltpu.make_async_copy(mask_any, mask, in_sem.at[0])
    t_loads = [pltpu.make_async_copy(
        t.at[:, pl.ds(i * TILE, TILE)], t_v.at[v * cols + i], in_sem.at[1]) for i in range(cols)]
    y_loads = [pltpu.make_async_copy(
        y.at[0, pl.ds(e * TILE, TILE)], y_v.at[e], in_sem.at[2]) for e in range(row_blocks)]
    x_loads = [pltpu.make_async_copy(
        block(p // col_blocks, p % col_blocks), x_v.at[p], in_sem.at[2]) for p in range(row_blocks * col_blocks)]
    lam_load = pltpu.make_async_copy(lam.at[c], lam_m, d_recv.at[5])
    mask_load.start()
    for load in t_loads + y_loads + x_loads:
        load.start()

    zero = jnp.zeros((TILE, TILE), bf16)
    for k in range(n):
        mine[k][CAP] = zero
        theirs[k][CAP] = zero

    pl.semaphore_wait(barrier, 1 + row + col)
    for k in (1, 2):
        @pl.when(last[k])
        def _():
            pl.semaphore_signal(ready.at[k - 1], inc=1, device_id=near[k], device_id_type=MESH)

    mask_load.wait()
    lead = top_row(mask, v, row_blocks, col_blocks)
    lead_columns = raw_columns(mask, v, lead, raw, col_blocks)
    drain(in_sem.at[1], cols)
    def t_part(k):
        return t_v.at[pl.ds(ids[k] * cols, cols)]

    t_copies = [None] + [remote(t_part(0), t_part(0), s_sem.at[1], t_recv.at[1], near[k]) for k in (1, 2)]
    t_relay = remote(t_part(1), t_part(1), s_sem.at[1], t_recv.at[0], to_y)
    t_swaps = [None] + [remote(t_part(k), t_part(k), s_sem.at[1], d_recv.at[k // 3], to_core) for k in (1, 2, 3)]

    for k in (1, 2):
        @pl.when((c == 1) & last[k])
        def _():
            t_copies[k].start()

    mask_swap = remote(mask_any, other, s_sem.at[2], d_recv.at[2], to_core)
    mask_swap.start()

    drain(in_sem.at[2], row_blocks + row_blocks * col_blocks)
    lam_load.start()
    for s in range(raw):
        raw_m[0][s] = x_v[lead * col_blocks + lead_columns[s]]
    raw_m[0][raw] = y_v[lead]

    spans = [(0, raw // 2), (raw // 2, raw + 1)]
    at = raw
    for size in [first // 2] * 2 + [late // 2 - 1, 1] * 2:
        spans.append((at, at + size))
        at += size
    low, high = (0, 2, 4, 5), (1, 3, 6, 7)
    groups = [(0, 0), (1, 1), (2, 2), (3, 3), (4, 5), (6, 7)]
    paths = [None, (0, 1, 2, 3, 4, 5), (1, 0, 3, 2, 5, 4)]

    def chunk(raws, gathered, k, q, r):
        start, stop = spans[q][0], spans[r][1]
        return (raws if q < 2 else gathered)[k].at[pl.ds(start, stop - start)]

    stages = [None, (0, 0, 1, 1, 2, 7), (0, 0, 1, 1, 7, 2)]
    last_stages = (0, 0, 1, 1, 2, 3, 2, 3)
    sizes = [raw + 1, first, late]

    def own_copy(k, g):
        q, r = groups[g]
        return remote(chunk(raw_m, mine, 0, q, r), chunk(raw_m, mine, k, q, r), s_sem.at[0], b_recv.at[stages[k][g]], near[k])

    def relay_copy(k, q):
        return remote(chunk(raw_m, mine, k, q, q), chunk(raw_m, mine, 3, q, q), s_sem.at[0],
                      b_recv.at[3 + last_stages[q]], near[3 - k])

    def swap(k, q, r):
        sem = 3 + k // 3 if q < 2 else 6 + k // 3
        return remote(chunk(raw_m, mine, k, q, r), chunk(raw_t, theirs, k, q, r), s_sem.at[0], d_recv.at[sem], to_core)

    own_swap = remote(mine[0].at[pl.ds(0, CAP)], theirs[0].at[pl.ds(0, CAP)], s_sem.at[0], d_recv.at[5], to_core)
    lam_swap = remote(lam.at[partner], lam_t, s_sem.at[0], d_recv.at[5], to_core)

    def raw_start(k):
        own_copy(k, paths[k][0]).start()

        @pl.when((c == 0) | (k == 1))
        def _():
            own_copy(k, paths[k][1]).start()

    for k in (1, 2):
        @pl.when(last[k])
        def _():
            raw_start(k)

    for k in (1, 2):
        @pl.when(jnp.logical_not(last[k]))
        def _():
            pl.semaphore_wait(ready.at[k - 1], 1)

            @pl.when(c == 1)
            def _():
                t_copies[k].start()

            raw_start(k)

    @pl.when(c == 0)
    def _():
        lam_swap.start()

    def dress(k):
        for i in range(cols):
            b = ids[k] * cols + i
            columns = t_v[b]
            for e in range(row_blocks):
                term = jnp.dot(y_v[e], columns, preferred_element_type=f32)
                dressed[e * col_blocks + b] = (x_v[e * col_blocks + b].astype(f32) - term).astype(bf16)

    slots = slots_of(mask, v, lead, raw, n - 1 - v, row_blocks, col_blocks, cols)
    order = []
    for s in range(raw, CAP):
        place = jnp.int32(0)
        for p, slot in enumerate(slots):
            place = jnp.where(slot == s, p, place)
        order.append(place)

    dress(0)
    @pl.when(c == 1)
    def _():
        drain(t_recv.at[1], 2 * cols)
        t_relay.start()
        own_copy(2, 0).start()
        t_swaps[1].start()
        t_swaps[2].start()

    @pl.when(c == 0)
    def _():
        drain(d_recv.at[0], 2 * cols)

    dress(1)
    dress(2)

    def pack(q):
        for s in range(*spans[q]):
            mine[0][s] = dressed[order[s - raw]]

    pack(2)
    pack(3)
    for i in (2, 3):
        for k in (1, 2):
            own_copy(k, paths[k][i]).start()
    @pl.when(c == 1)
    def _():
        t_relay.wait_recv()
        t_swaps[3].start()
        lam_swap.start()

    @pl.when(c == 0)
    def _():
        t_swaps[3].wait_recv()

    dress(3)
    for i in (4, 5):
        for q in groups[i]:
            pack(q)
    for i in (4, 5):
        for k in (1, 2):
            own_copy(k, paths[k][i]).start()
    for s in range(raw):
        mine[0][s] = dressed[lead * col_blocks + lead_columns[s]]
    own_swap.start()
    mask_swap.wait_recv()

    def mend(k, raws, gathered, live_of):
        best = top_row(live_of, ids[k], row_blocks, col_blocks)
        places = raw_columns(live_of, ids[k], best, raw, col_blocks)
        rows = raws[k][raw]
        for s in range(raw):
            term = jnp.dot(rows, t_v[places[s]], preferred_element_type=f32)
            gathered[k][s] = (raws[k][s].astype(f32) - term).astype(bf16)

    def places(live_of, k):
        j = ids[k]
        best = top_row(live_of, j, row_blocks, col_blocks)
        return slots_of(live_of, j, best, raw, n - 1 - j, row_blocks, col_blocks, cols)

    def tile(gathered, slots, e, b):
        rows = [jnp.concatenate([gathered[slots[p * col_blocks + q]] for q in (b, b + 1)], axis=1) for p in (e, e + 1)]
        return jnp.concatenate(rows, axis=0)

    def product(pairs, b):
        return sum(
            jnp.dot(rows[:, e * TILE:(e + 2) * TILE], tile(gathered, slots, e, b), preferred_element_type=f32)
            for rows, gathered, slots in pairs for e in range(0, row_blocks, 2))

    def both(k):
        mine_k = (lam_m[ids[k]], mine[k], places(mask, k))
        theirs_k = (lam_t[ids[k]], theirs[k], places(other, k))
        for b in range(0, col_blocks, 2):
            stage[k, :, b * TILE:(b + 2) * TILE] = product([mine_k, theirs_k], b).astype(bf16)

    def relay(level):
        for q in (0, 1, 2, 3, 4, 6, 5, 7):
            if min(last_stages[q], 2) == level:
                relay_copy(1 if q in low else 2, q).start()

    def arrive(level):
        drain(b_recv.at[level], 2 * sizes[level])
        relay(level)
        for k in (1, 2):
            swap(k, *((0, 1), (2, 3))[level]).start()

    arrive(0)
    arrive(1)
    mend(1, raw_m, mine, mask)
    mend(2, raw_m, mine, mask)
    drain(d_recv.at[3], 2 * (raw + 1))
    mend(1, raw_t, theirs, other)
    mend(2, raw_t, theirs, other)
    drain(d_recv.at[5], CAP + 2 * lam_blocks)
    both(0)
    drain(b_recv.at[2], late)
    @pl.when(c == 0)
    def _():
        relay(2)

    swap(1, 4, 5).start()
    swap(2, 6, 7).start()
    drain(b_recv.at[7], late)
    swap(1, 6, 7).start()
    swap(2, 4, 5).start()
    here, there = places(mask, 3), places(other, 3)
    lam_last[...] = lam_t[ids[3]]
    drain(b_recv.at[3], raw + 1)

    @pl.when(c == 1)
    def _():
        relay(2)

    swap(3, 0, 1).start()
    drain(d_recv.at[6], 2 * (CAP - raw))

    both(1)
    drain(b_recv.at[4], first)
    swap(3, 2, 3).start()
    mend(3, raw_m, mine, mask)
    drain(d_recv.at[4], raw + 1)
    mend(3, raw_t, theirs, other)
    both(2)
    drain(b_recv.at[5], late - 2)
    for q in (4, 6):
        swap(3, q, q).start()
    drain(b_recv.at[6], 2)
    for q in (5, 7):
        swap(3, q, q).start()
    for b in range(0, col_blocks, 2):
        acc[:, b * TILE:(b + 2) * TILE] = product([(lam_m[ids[3]], mine[3], here)], b)
    drain(d_recv.at[7], CAP - raw)
    for b in range(0, col_blocks, 2):
        for e in range(0, row_blocks, 2):
            dense_t[e * TILE:(e + 2) * TILE, b * TILE:(b + 2) * TILE] = tile(theirs[3], there, e, b)

    @pl.when(c == 1)
    def _():
        drain(s_sem.at[1], 6 * cols)

    mask_swap.wait_send()
    drain(s_sem.at[0], 3 * (CAP + 1) + CAP + 3 * (CAP + 1) + lam_blocks)


def last_kernel(done, dense_t, lam_last, acc, out, stage, sem):
    v = lax.axis_index("vir")
    row, col = v // 2, v % 2
    ids = [v, row * 2 + (1 - col), (1 - row) * 2 + col, 3 - v]
    pieces, rows, width = stage.shape
    for k in range(done.shape[0]):
        pltpu.make_async_copy(done.at[k], out.at[0, ids[k]], sem.at[0]).start()
    for i in range(pieces):
        columns = slice(i * width, (i + 1) * width)
        stage[i] = (acc[:, columns] + jnp.dot(
            lam_last[...], dense_t[:, columns], preferred_element_type=jnp.float32)).astype(jnp.bfloat16)
        pltpu.make_async_copy(stage.at[i], out.at[0, ids[3], :, pl.ds(i * width, width)], sem.at[0]).start()
    pltpu.make_async_copy(out, out, sem.at[0]).wait()


def ring_kernel(n, lam, x, y, t, mask_any, out, lam_m, lam_t, x_v, y_v, t_v, dressed, dense_m, dense_t, acc, mask, other,
                in_sem, t_send, t_recv, b_send, b_recv, d_send, d_recv, l_send, l_recv, *bufs):
    mine, theirs = bufs[:n], bufs[n:]
    v, c = lax.axis_index("vir"), lax.axis_index("ka")
    dst, src = [(v + k) % n for k in range(n)], [(v + n - k) % n for k in range(n)]
    half, full = x_v.shape
    width = t_v.shape[2]
    row_blocks, col_blocks = half // TILE, full // TILE
    f32, bf16 = jnp.float32, jnp.bfloat16
    loads = [pltpu.make_async_copy(source, target, in_sem.at[i]) for i, (source, target) in enumerate(
        [(mask_any, mask), (t, t_v.at[v]), (y.at[0], y_v), (x.at[0], x_v), (lam.at[c], lam_m)])]
    for load in loads:
        load.start()
    to_core = {"ka": 1 - c}
    barrier = enter([{"vir": dst[k]} for k in range(1, n)] + [to_core])
    for load in loads:
        load.wait()
    pl.semaphore_wait(barrier, n)

    t_copies = [remote(t_v.at[v], t_v.at[v], t_send.at[k], t_recv.at[k], {"vir": dst[k]}) for k in range(1, n)]
    arrivals = [remote(t_v.at[v], t_v.at[src[k]], t_send.at[k], t_recv.at[k], {"vir": dst[k]}) for k in range(1, n)]
    for copy in t_copies:
        copy.start()
    mask_swap = remote(mask_any, other, l_send.at[0], l_recv.at[0], to_core)
    lam_swap = remote(lam.at[1 - c], lam_t, l_send.at[1], l_recv.at[1], to_core)
    mask_swap.start()
    lam_swap.start()

    zero = jnp.zeros((TILE, TILE), bf16)
    for k in range(n):
        mine[k][CAP] = zero
        theirs[k][CAP] = zero
    order = [jnp.int32(0)] * CAP
    count = jnp.int32(0)
    for p in range(row_blocks * col_blocks):
        live = mask[v, p // col_blocks, p % col_blocks]
        order = [jnp.where((live != 0) & (count == s), p, order[s]) for s in range(CAP)]
        count = count + live

    for copy in arrivals:
        copy.wait_recv()
    for b in range(col_blocks):
        if width >= TILE:
            owner, offset = b * TILE // width, b * TILE % width
            columns = t_v[owner][:, offset:offset + TILE]
        else:
            group = TILE // width
            columns = jnp.concatenate([t_v[b * group + i] for i in range(group)], axis=1)
        term = jnp.dot(y_v[...], columns, preferred_element_type=f32)
        value = (x_v[:, b * TILE:(b + 1) * TILE].astype(f32) - term).astype(bf16)
        for e in range(row_blocks):
            dressed[e * col_blocks + b] = value[e * TILE:(e + 1) * TILE]
    for s in range(CAP):
        mine[0][s] = dressed[order[s]]

    def live_part(ref):
        return ref.at[pl.ds(0, CAP)]

    copies = [None] + [
        remote(live_part(mine[0]), live_part(mine[k]), b_send.at[k], b_recv.at[k], {"vir": dst[k]}) for k in range(1, n)]
    swaps = [remote(live_part(mine[k]), live_part(theirs[k]), d_send.at[k], d_recv.at[k], to_core) for k in range(n)]
    for copy in copies[1:]:
        copy.start()

    def fill(dense, gathered, live_of, j):
        count = jnp.int32(0)
        for e in range(row_blocks):
            for b in range(col_blocks):
                live = live_of[j, e, b]
                dense[e * TILE:(e + 1) * TILE, b * TILE:(b + 1) * TILE] = gathered[jnp.where(live != 0, count, CAP)]
                count = count + live

    mask_swap.wait_recv()
    lam_swap.wait_recv()
    for k in range(n):
        if k:
            copies[k].wait_recv()
        swaps[k].start()
        fill(dense_m, mine[k], mask, src[k])
        acc[...] = jnp.dot(lam_m[src[k]], dense_m[...], preferred_element_type=f32)
        swaps[k].wait_recv()
        fill(dense_t, theirs[k], other, src[k])
        out[0, src[k]] = (acc[...] + jnp.dot(
            lam_t[src[k]], dense_t[...], preferred_element_type=f32)).astype(bf16)

    for copy in t_copies + copies[1:] + swaps + [mask_swap, lam_swap]:
        copy.wait_send()


def body(n, lambda_amps, screened_ints, half_ints, singles, block_mask):
    wide, pairs, rows, half = lambda_amps.shape
    full = screened_ints.shape[2]
    inner, width = singles.shape
    row_blocks, col_blocks = half // TILE, full // TILE
    blocks = row_blocks * col_blocks
    bf16, f32 = jnp.bfloat16, jnp.float32
    dma = pltpu.SemaphoreType.DMA
    tile = (TILE, TILE)
    anywhere, vmem = pl.BlockSpec(memory_space=pl.ANY), pl.BlockSpec(memory_space=pltpu.VMEM)
    lams = [pltpu.VMEM((pairs, rows, half), bf16)] * 2
    dense, total = pltpu.VMEM((half, full), bf16), pltpu.VMEM((rows, full), f32)
    masks = [pltpu.SMEM(block_mask.shape, jnp.int32)] * 2
    held = [pltpu.VMEM((CAP + 1,) + tile, bf16)] * (2 * n)
    args = (lambda_amps, screened_ints, half_ints, singles, block_mask)
    params = pltpu.CompilerParams(collective_id=0, has_side_effects=True, vmem_limit_bytes=56 * 1024 * 1024)
    if n != 4:
        return pl.pallas_call(
            functools.partial(ring_kernel, n),
            out_shape=pltpu.VMEM((1, pairs, rows, full), bf16),
            in_specs=[anywhere] * 5,
            out_specs=vmem,
            scratch_shapes=lams + [
                pltpu.VMEM((half, full), bf16), pltpu.VMEM((half, inner), bf16), pltpu.VMEM((n, inner, width), bf16),
                pltpu.VMEM((blocks,) + tile, bf16), dense, dense, total,
            ] + masks + [dma((5,)), dma((n,)), dma((n,)), dma((n,)), dma((n,)), dma((n,)), dma((n,)), dma((2,)), dma((2,))] + held,
            compiler_params=params,
        )(*args)
    raw = CAP // row_blocks
    held_over = (pltpu.VMEM((n - 1, rows, full), bf16), dense, pltpu.VMEM((rows, half), bf16), total)
    handed = pl.pallas_call(
        grid_kernel,
        out_shape=held_over,
        in_specs=[anywhere] * 5,
        out_specs=(vmem,) * 4,
        scratch_shapes=lams + [
            pltpu.VMEM((blocks,) + tile, bf16), pltpu.VMEM((row_blocks, TILE, inner), bf16),
            pltpu.VMEM((col_blocks, inner, TILE), bf16), pltpu.VMEM((blocks,) + tile, bf16),
        ] + masks + [
            pltpu.VMEM((7 * (CAP + 1) + pairs * rows * half // (TILE * TILE),) + tile, bf16),
            dma((3,)), dma((3,)), dma((2,)), dma((8,)), dma((8,)), pltpu.SemaphoreType.REGULAR((2,)),
        ] + held + [pltpu.VMEM((raw + 1,) + tile, bf16)] * (2 * n),
        compiler_params=params,
    )(*args)
    pieces = 2
    return pl.pallas_call(
        last_kernel,
        out_shape=jax.ShapeDtypeStruct((1, pairs, rows, full), bf16),
        in_specs=[vmem] * 4,
        out_specs=anywhere,
        scratch_shapes=[pltpu.VMEM((pieces, rows, full // pieces), bf16), dma((1,))],
        compiler_params=pltpu.CompilerParams(vmem_limit_bytes=8 * 1024 * 1024),
    )(*handed)


def solution(mesh):
    return jax.shard_map(
        functools.partial(body, mesh.shape["vir"]),
        mesh=mesh,
        in_specs=(
            P(None, "occ", "vir", "ka"),
            P(("occ", "vir"), "ka", None),
            P(("occ", "vir"), "ka", None),
            P(None, "vir"),
            P("occ", "ka", None),
        ),
        out_specs=P("ka", "occ", "vir", None),
        check_vma=False,
    )
```
